32 devices in a mesh: row: 8 (over z, y), col: 4 (over x, core).
Axes of the slice: x: 2, y: 2, z: 4, core: 2. Of those that a mesh axis runs over, the one named last changes fastest.
Arguments:
- eigvec: float32 [32, 8, 128, 1024], P(None, 'row', None, 'col'), may hold values from -6 to 6
- reflectors: float32 [2, 32, 8, 256, 128], P(None, None, 'row', 'col'), may hold values from -6 to 6
- sweep_group: int32 [2, 32, 8], P(None, None, 'row'), may hold values from -1 to 254, as said below
Outputs:
- transformed: float32 [32, 8, 128, 1024], P(None, 'row', None, 'col')
The draws below stay inside these ranges and needn't reach their ends.
Inputs may be any that keep to these rules, and one draw needn't show every extreme that they name: `sweep_group`: -1 where no diamond sits at that diagonal and tile position (tile position l * R + r for entry [d, l, r]); otherwise the diamond's sweep group, at most its tile position. Within one diagonal no two diamonds sit at adjacent tile positions, and none sits at the last tile position 255.
All inputs are finite; a program needn't handle non-finite values.
Results may differ from the reference program's by a relative error of at most 0.0003.
Values sent between devices are 32-bit elements.
A program may use at most 128 MiB of HBM per device.

```python
import jax
import jax.numpy as jnp
from jax import lax

B = 128
DIAG = 2
NT = 256
TILES_DEV = 32
NC = 1024
N_ROW = 8


def draw_sweep_group(key, part):
    first_key = jax.random.fold_in(key, 11)
    second_key = jax.random.fold_in(key, 12)
    bits = jax.random.randint(first_key, (DIAG, NT), 0, 2).astype(jnp.int32)
    earlier = jnp.concatenate([jnp.zeros((DIAG, 1), jnp.int32), bits[:, :-1]], axis=1)
    positions = jnp.broadcast_to(jnp.arange(NT, dtype=jnp.int32)[None, :], (DIAG, NT))
    present = (bits == 1) & (earlier == 0) & (positions < NT - 1)
    groups = jax.random.randint(second_key, (DIAG, NT), 0, positions + 1).astype(jnp.int32)
    result = jnp.where(present, groups, -jnp.ones_like(groups))
    return result.reshape(DIAG, TILES_DEV, NT // TILES_DEV).astype(jnp.int32)


def level_of(key, dims, shards, least, largest):
    def one(dim, shards_of):
        steps = jax.random.uniform(jax.random.fold_in(jax.random.fold_in(key, 6), dim), (shards_of,), jnp.float32, least / len(shards), largest / len(shards))
        return jnp.repeat(jnp.exp(steps), dims[dim] // shards_of).reshape((-1,) + (1,) * (len(dims) - dim - 1))

    factor_of = one(*shards[0])
    for cut in shards[1:]:
        factor_of = factor_of * one(*cut)
    return factor_of


def gaussian(key, shape, deviation, reach, shards=(), kind=jnp.bfloat16):
    values = deviation * jax.random.normal(key, shape, jnp.float32)
    if shards:
        values = values * level_of(key, shape, shards, -0.22, 0.18)
    return jnp.clip(values, -reach, reach).astype(kind)


def setup_inputs(seed: int = 0) -> dict:
    streams_of = jax.random.split(jax.random.key(seed), 4)
    return {
        "eigvec": gaussian(streams_of[0], (TILES_DEV, N_ROW, B, NC), 1.0, 6.0, ((1, 8), (3, 4)), jnp.float32),
        "reflectors": gaussian(streams_of[1], (DIAG, TILES_DEV, N_ROW, 2 * B, B), 1.0, 6.0, ((2, 8), (3, 4)), jnp.float32),
        "sweep_group": draw_sweep_group(jax.random.fold_in(streams_of[3], 71), 0),
    }


highest_mode = lax.Precision.HIGHEST


def masked_vectors(panels):
    depth_rows = panels.shape[-2]
    band_width = panels.shape[-1]
    row_iota = lax.broadcasted_iota(jnp.int32, (depth_rows, band_width), 0)
    col_iota = lax.broadcasted_iota(jnp.int32, (depth_rows, band_width), 1)
    inside = (row_iota >= col_iota + 1) & (row_iota <= col_iota + band_width)
    leading = row_iota == col_iota + 1
    kept = jnp.where(inside, panels, jnp.zeros_like(panels))
    return jnp.where(leading, jnp.ones_like(panels), kept)


def inverse_factor(vectors):
    band_width = vectors.shape[-1]
    gram_matrix = jnp.einsum("...ji,...jk->...ik", vectors, vectors, precision=highest_mode)
    diagonal_part = jnp.diagonal(gram_matrix, axis1=-2, axis2=-1)
    strict_upper = jnp.triu(gram_matrix, 1)
    return strict_upper + jnp.eye(band_width, dtype=vectors.dtype) * (0.5 * diagonal_part[..., None, :])


def invert_upper(factor):
    band_width = factor.shape[-1]
    row_iota = lax.broadcasted_iota(jnp.int32, (band_width, band_width), 0)
    col_iota = lax.broadcasted_iota(jnp.int32, (band_width, band_width), 1)
    diagonal_part = jnp.diagonal(factor, axis1=-2, axis2=-1)
    eye_matrix = (row_iota == col_iota).astype(factor.dtype)
    inverse = eye_matrix * (1.0 / diagonal_part)[..., None, :]
    block = 1
    while block < band_width:
        coupling = ((row_iota // block) != (col_iota // block)) & ((row_iota // (2 * block)) == (col_iota // (2 * block)))
        upper_part = jnp.where(coupling, factor, jnp.zeros_like(factor))
        middle = jnp.einsum("...ij,...jk->...ik", upper_part, inverse, precision=highest_mode)
        inverse = inverse - jnp.einsum("...ij,...jk->...ik", inverse, middle, precision=highest_mode)
        block = block * 2
    return inverse


def reflect(stacked, vectors, factor):
    weights = jnp.einsum("...ji,...jc->...ic", vectors, stacked, precision=highest_mode)
    solved = jnp.einsum("...ik,...kc->...ic", invert_upper(factor), weights, precision=highest_mode)
    return stacked - jnp.einsum("...ji,...ic->...jc", vectors, solved, precision=highest_mode)


def apply_one(item):
    stacked, panels, flag = item
    vectors = masked_vectors(panels)
    factor = inverse_factor(vectors)
    updated = reflect(stacked, vectors, factor)
    return jnp.where(flag >= 0, updated, stacked)


def reference(eigvec, reflectors, sweep_group):
    tiles_dev = eigvec.shape[0]
    cycle_size = eigvec.shape[1]
    band = eigvec.shape[2]
    columns = eigvec.shape[3]
    total = tiles_dev * cycle_size
    diagonals = reflectors.shape[0]
    current = eigvec.reshape(total, band, columns)
    panels_all = reflectors.reshape(diagonals, total, 2 * band, band)
    flags_all = sweep_group.reshape(diagonals, total)
    for diagonal in range(diagonals):
        stacked = current.reshape(total // 2, 2 * band, columns)
        updated = lax.map(apply_one, (stacked, panels_all[diagonal, 0::2], flags_all[diagonal, 0::2]))
        current = updated.reshape(total, band, columns)
        inner = current[1:total - 1].reshape(total // 2 - 1, 2 * band, columns)
        updated = lax.map(apply_one, (inner, panels_all[diagonal, 1:total - 1:2], flags_all[diagonal, 1:total - 1:2]))
        current = jnp.concatenate([current[:1], updated.reshape(total - 2, band, columns), current[total - 1:]], axis=0)
    return current.reshape(tiles_dev, cycle_size, band, columns)
```

```python
import functools

import jax
import jax.numpy as jnp
from jax import lax
from jax.experimental import pallas as pl
from jax.experimental.pallas import tpu as pltpu
from jax.sharding import PartitionSpec as P


GROUP = 2
CHUNKS = 2
PROFILES = ((11, 9, 9, 11), (12, 10, 10, 12), (13, 11, 11, 13), (14, 12, 12, 14), (16, 14, 14, 16))
GROUPED = 4


def split(x):
    high = x.astype(jnp.bfloat16)
    return high, (x - high.astype(jnp.float32)).astype(jnp.bfloat16)


def dot(a, b):
    return jnp.dot(a, b, preferred_element_type=jnp.float32)


def dot3(a, b):
    return dot(a[1], b[0]) + dot(a[0], b[1]) + dot(a[0], b[0])


def bounds(slots):
    inner = [slots * i // CHUNKS // GROUP * GROUP for i in range(CHUNKS)]
    return inner + [slots]


def chunk_shapes(slots, tiles):
    edges = bounds(slots)
    return [
        jax.ShapeDtypeStruct((high - low,) + tiles.shape[1:], tiles.dtype)
        for low, high in zip(edges[:-1], edges[1:])
    ]


def slot_of(chunks, k):
    for chunk in chunks:
        if k < chunk.shape[0]:
            return chunk.at[k]
        k -= chunk.shape[0]


def gather_kernel(slots, own, behind, panels, tiles, picked, *rest):
    diagonals = panels.shape[0]
    sent, sems = rest[:-1], rest[-1]

    def panel_copy(d, k):
        return pltpu.make_async_copy(
            panels.at[d, own[d, k]], picked.at[d, k], sems.at[d * slots + k]
        )

    def tile_copy(k):
        return pltpu.make_async_copy(
            tiles.at[behind[0, k]], slot_of(sent, k), sems.at[diagonals * slots + k]
        )

    for k in range(slots):
        tile_copy(k).start()
    for d in range(diagonals):
        for k in range(slots):
            panel_copy(d, k).start()
    for k in range(slots):
        tile_copy(k).wait()
    for d in range(diagonals):
        for k in range(slots):
            panel_copy(d, k).wait()


def gather(slots, own, behind, panels, tiles):
    diagonals = panels.shape[0]
    any_spec = pl.BlockSpec(memory_space=pl.ANY)
    return pl.pallas_call(
        functools.partial(gather_kernel, slots),
        grid_spec=pltpu.PrefetchScalarGridSpec(
            num_scalar_prefetch=2,
            grid=(1,),
            in_specs=[any_spec, any_spec],
            out_specs=[pl.BlockSpec(memory_space=pltpu.VMEM)] * (1 + CHUNKS),
            scratch_shapes=[pltpu.SemaphoreType.DMA(((diagonals + 1) * slots,))],
        ),
        out_shape=[
            jax.ShapeDtypeStruct((diagonals, slots) + panels.shape[2:], panels.dtype),
        ] + chunk_shapes(slots, tiles),
        name="gather",
    )(own, behind, panels, tiles)


def scatter_kernel(slots, diagonal, more, behind, counts, tiles, *rest):
    returned, out, sent, sems = rest[:CHUNKS], rest[CHUNKS], rest[CHUNKS + 1:-1], rest[-1]

    def put(k):
        return pltpu.make_async_copy(
            slot_of(returned, k), out.at[behind[diagonal, k]], sems.at[k]
        )

    for k in range(slots):
        @pl.when(k < counts[1, diagonal])
        def _():
            put(k).start()
    for k in range(slots):
        @pl.when(k < counts[1, diagonal])
        def _():
            put(k).wait()
    if more:

        def take(k):
            return pltpu.make_async_copy(
                out.at[behind[diagonal + 1, k]], slot_of(sent, k), sems.at[slots + k]
            )

        for k in range(slots):
            take(k).start()
        for k in range(slots):
            take(k).wait()


def scatter(slots, diagonal, more, behind, counts, tiles, returned):
    any_spec = pl.BlockSpec(memory_space=pl.ANY)
    vmem_spec = pl.BlockSpec(memory_space=pltpu.VMEM)
    shapes = [jax.ShapeDtypeStruct(tiles.shape, tiles.dtype)]
    if more:
        shapes += chunk_shapes(slots, tiles)
    return pl.pallas_call(
        functools.partial(scatter_kernel, slots, diagonal, more),
        grid_spec=pltpu.PrefetchScalarGridSpec(
            num_scalar_prefetch=2,
            grid=(1,),
            in_specs=[any_spec] + [vmem_spec] * CHUNKS,
            out_specs=[any_spec] + [vmem_spec] * (len(shapes) - 1),
            scratch_shapes=[pltpu.SemaphoreType.DMA((2 * slots,))],
        ),
        out_shape=shapes,
        input_output_aliases={2: 0},
        name="scatter",
    )(behind, counts, tiles, *returned)


def factor_kernel(pieces_count, col_ref, *refs):
    pieces = refs[:pieces_count]
    vh_ref, vl_ref, yh_ref, yl_ref = refs[pieces_count:]
    me = col_ref[0]
    group = pieces[0].shape[1]
    band = pieces[0].shape[-1]
    depth = pieces_count * pieces[0].shape[2]
    row = lax.broadcasted_iota(jnp.int32, (depth, band), 0)
    col = lax.broadcasted_iota(jnp.int32, (depth, band), 1)
    inside = (row >= col + 1) & (row <= col + band)
    leading = row == col + 1
    r = lax.broadcasted_iota(jnp.int32, (band, band), 0)
    c = lax.broadcasted_iota(jnp.int32, (band, band), 1)
    slots = range(group)
    vs, ts, factors, inverses = [], [], [], []
    for g in slots:
        parts = [piece[0, g] for piece in pieces]
        stride = 1
        while stride < pieces_count:
            odd = (me // stride) % 2 == 1
            parts = [
                jnp.where(odd, parts[j ^ stride], parts[j]) for j in range(pieces_count)
            ]
            stride *= 2
        panel = jnp.concatenate(parts, axis=0)
        v = jnp.where(leading, 1.0, jnp.where(inside, panel, 0.0))
        vs.append(split(v))
        ts.append(split(v.T))
        vh_ref[g] = vs[g][0]
        vl_ref[g] = vs[g][1]
    for g in slots:
        gram = dot3(ts[g], vs[g])
        diagonal = jnp.sum(jnp.where(r == c, gram, 0.0), axis=0, keepdims=True)
        factors.append(gram)
        inverses.append(jnp.where(r == c, 2.0 / diagonal, 0.0))

    def level(n, inverses):
        coupling = ((r >> n) != (c >> n)) & ((r >> (n + 1)) == (c >> (n + 1))) & (r < c)
        inverse_parts = [split(inverse) for inverse in inverses]
        middles = [
            split(dot3(split(jnp.where(coupling, factors[g], 0.0)), inverse_parts[g]))
            for g in slots
        ]
        return tuple(inverses[g] - dot3(inverse_parts[g], middles[g]) for g in slots)

    inverses = lax.fori_loop(0, (band - 1).bit_length(), level, tuple(inverses))
    for g in slots:
        high, low = split(dot3(split(inverses[g]), ts[g]))
        yh_ref[g] = high
        yl_ref[g] = low


def factor(first, slots, diagonal, col, pieces):
    count = len(pieces)
    _, _, height, band = pieces[0].shape
    depth = count * height
    group = GROUP if slots % GROUP == 0 else 1
    start = first // group
    kind = jnp.bfloat16
    return pl.pallas_call(
        functools.partial(factor_kernel, count),
        grid_spec=pltpu.PrefetchScalarGridSpec(
            num_scalar_prefetch=1,
            grid=(slots // group,),
            in_specs=[
                pl.BlockSpec((1, group, height, band), lambda k, c: (diagonal, k + start, 0, 0))
            ] * count,
            out_specs=[pl.BlockSpec((group, depth, band), lambda k, c: (k, 0, 0))] * 2
            + [pl.BlockSpec((group, band, depth), lambda k, c: (k, 0, 0))] * 2,
        ),
        out_shape=[jax.ShapeDtypeStruct((slots, depth, band), kind)] * 2
        + [jax.ShapeDtypeStruct((slots, band, depth), kind)] * 2,
        name="factor",
    )(col, *pieces)


def apply_kernel(diagonal, first, own, counts, tile, below, vh, vl, yh, yl, tile_out, below_out):
    k = pl.program_id(0) + first
    band = tile.shape[1]
    upper, lower = tile[0], below[0]
    stacked = jnp.concatenate([upper, lower], axis=0)
    solved = dot3((yh[0], yl[0]), split(stacked))
    change = dot3((vh[0], vl[0]), split(solved))
    active = k < counts[0, diagonal]
    tile_out[0] = jnp.where(active, upper - change[:band], upper)
    below_out[0] = jnp.where(active, lower - change[band:], lower)


def apply(first, diagonal, own, counts, tiles, beneath, vh, vl, yh, yl):
    _, band, columns = tiles.shape
    depth = vh.shape[1]
    at_slot = lambda k, own, counts: (k, 0, 0)
    at_own = lambda k, own, counts: (own[diagonal, k + first], 0, 0)
    return pl.pallas_call(
        functools.partial(apply_kernel, diagonal, first),
        grid_spec=pltpu.PrefetchScalarGridSpec(
            num_scalar_prefetch=2,
            grid=(beneath.shape[0],),
            in_specs=[
                pl.BlockSpec((1, band, columns), at_own),
                pl.BlockSpec((1, band, columns), at_slot),
                pl.BlockSpec((1, depth, band), at_slot),
                pl.BlockSpec((1, depth, band), at_slot),
                pl.BlockSpec((1, band, depth), at_slot),
                pl.BlockSpec((1, band, depth), at_slot),
            ],
            out_specs=[
                pl.BlockSpec((1, band, columns), at_own),
                pl.BlockSpec((1, band, columns), at_slot),
            ],
        ),
        out_shape=[
            jax.ShapeDtypeStruct(tiles.shape, tiles.dtype),
            jax.ShapeDtypeStruct(beneath.shape, beneath.dtype),
        ],
        input_output_aliases={2: 0},
        name="apply",
    )(own, counts, tiles, beneath, vh, vl, yh, yl)


def lift(sent, to_above):
    beneath = []
    for chunk in sent:
        beneath.append(lax.ppermute(chunk, "row", to_above))
    return beneath


def steps(slots, own, behind, counts, tiles, panels):
    row_count = lax.axis_size("row")
    col_count = lax.axis_size("col")
    col = lax.axis_index("col").astype(jnp.int32)[None]
    diagonals = panels.shape[0]
    to_above = [(i, (i - 1) % row_count) for i in range(row_count)]
    to_below = [(i, (i + 1) % row_count) for i in range(row_count)]
    picked, *sent = gather(slots, own, behind, panels, tiles)
    beneath = lift(sent, to_above)
    pieces = {0: picked}
    stride = col_count // 2
    while stride >= 1:
        swap = [(i, i ^ stride) for i in range(col_count)]
        pieces.update(
            {q ^ stride: lax.ppermute(p, "col", swap) for q, p in pieces.items()}
        )
        stride //= 2
    pieces = [pieces[q] for q in range(col_count)]
    for diagonal in range(diagonals):
        returned = []
        for first, chunk in zip(bounds(slots), beneath):
            factors = factor(first, chunk.shape[0], diagonal, col, pieces)
            tiles, lower = apply(first, diagonal, own, counts, tiles, chunk, *factors)
            returned.append(lax.ppermute(lower, "row", to_below))
        more = diagonal + 1 < diagonals
        tiles, *sent = scatter(slots, diagonal, more, behind, counts, tiles, returned)
        if more:
            beneath = lift(sent, to_above)
    return tiles


def share_kernel(flags, out, held, send, recv):
    count = held.shape[0]
    me = lax.axis_index("row")
    barrier = pltpu.get_barrier_semaphore()
    mesh_id = pl.DeviceIdType.MESH
    others = [lax.rem(me + by, count) for by in range(1, count)]
    for other in others:
        pl.semaphore_signal(
            barrier, inc=1, device_id={"row": other}, device_id_type=mesh_id
        )
    pl.semaphore_wait(barrier, count - 1)
    copies = [
        pltpu.make_async_remote_copy(
            src_ref=flags,
            dst_ref=held.at[me],
            send_sem=send.at[i],
            recv_sem=recv.at[i],
            device_id={"row": other},
            device_id_type=mesh_id,
        )
        for i, other in enumerate(others)
    ]
    for copy in copies:
        copy.start()
    held[me] = flags[...]
    for copy in copies:
        copy.wait()
    out[...] = held[...]


def share(flags):
    count = lax.axis_size("row")
    diagonals, depth = flags.shape
    rows, lanes = -(-diagonals // 8) * 8, -(-depth // 128) * 128
    padded = jnp.pad(flags, ((0, rows - diagonals), (0, lanes - depth)))
    vmem_spec = pl.BlockSpec(memory_space=pltpu.VMEM)
    shape = (count, rows, lanes)
    gathered = pl.pallas_call(
        share_kernel,
        out_shape=jax.ShapeDtypeStruct(shape, flags.dtype),
        in_specs=[vmem_spec],
        out_specs=vmem_spec,
        scratch_shapes=[
            pltpu.VMEM(shape, flags.dtype),
            pltpu.SemaphoreType.DMA((count - 1,)),
            pltpu.SemaphoreType.DMA((count - 1,)),
        ],
        compiler_params=pltpu.CompilerParams(collective_id=0, has_side_effects=True),
        name="share",
    )(padded)
    return gathered[:, :diagonals, :depth]


def ordering(active):
    depth = active.shape[-1]
    here = jnp.arange(depth, dtype=jnp.int32)
    on = active.astype(jnp.int32)
    earlier = here[None, :] < here[:, None]
    before = jnp.sum(jnp.where(earlier, on[..., None, :], 0), axis=-1)
    total = jnp.sum(on, axis=-1)
    rank = jnp.where(active, before, total[..., None] + here - before)
    order = jnp.sum(
        jnp.where(rank[..., None, :] == here[:, None], here, 0), axis=-1
    ).astype(jnp.int32)
    return order, total.astype(jnp.int32)


def flipped(index, stride):
    return index + stride - 2 * stride * lax.rem(lax.div(index, stride), 2)


def invert_and_store(panels, first, count, vh_ref, vl_ref, yh_ref, yl_ref):
    depth, band = panels.shape[1:]
    row = lax.broadcasted_iota(jnp.int32, (depth, band), 0)
    col = lax.broadcasted_iota(jnp.int32, (depth, band), 1)
    inside = (row >= col + 1) & (row <= col + band)
    leading = row == col + 1
    r = lax.broadcasted_iota(jnp.int32, (band, band), 0)
    c = lax.broadcasted_iota(jnp.int32, (band, band), 1)
    slots = range(count)
    ts, factors, inverses = [], [], []
    for g in slots:
        v = jnp.where(leading, 1.0, jnp.where(inside, panels[first + g], 0.0))
        vs = split(v)
        ts.append(split(v.T))
        vh_ref[first + g] = vs[0]
        vl_ref[first + g] = vs[1]
        gram = dot3(ts[g], vs)
        diagonal = jnp.sum(jnp.where(r == c, gram, 0.0), axis=0, keepdims=True)
        factors.append(gram)
        inverses.append(jnp.where(r == c, 2.0 / diagonal, 0.0))

    def level(n, inverses):
        coupling = ((r >> n) != (c >> n)) & ((r >> (n + 1)) == (c >> (n + 1))) & (r < c)
        inverse_parts = [split(inverse) for inverse in inverses]
        middles = [
            split(dot3(split(jnp.where(coupling, factors[g], 0.0)), inverse_parts[g]))
            for g in slots
        ]
        return tuple(inverses[g] - dot3(inverse_parts[g], middles[g]) for g in slots)

    inverses = lax.fori_loop(0, (band - 1).bit_length(), level, tuple(inverses))
    for g in slots:
        high, low = split(dot3(split(inverses[g]), ts[g]))
        yh_ref[first + g] = high
        yl_ref[first + g] = low


def whole_kernel(
    profile, group, table, tiles_in, panels_in, out,
    tiles, pieces, panel, vh, vl, yh, yl, lift_out, lift_in, upper_new, lower_new, back_in,
    merged, in_sems, panel_sems, lift_sems, back_sems, out_sems,
):
    n0, b0, b1, n1 = profile
    slots, lifts, backs = (n0, n1), (n0, b1), (b0, n1)
    depth = tiles.shape[0]
    height = pieces.shape[2]
    rows = lax.axis_size("row")
    cols = lax.axis_size("col")
    me_row = lax.axis_index("row")
    me_col = lax.axis_index("col")
    above = lax.rem(me_row + rows - 1, rows)
    below = lax.rem(me_row + 1, rows)
    mesh_id = pl.DeviceIdType.MESH
    strides = []
    stride = cols // 2
    while stride >= 1:
        strides.append(stride)
        stride //= 2
    own = lambda d, k: table[d, k]
    behind = lambda d, k: table[2 + d, k]
    upper_slot = lambda d, j: table[4 + d, j]
    lower_slot = lambda d, j: table[6 + d, j]

    panels_copy = pltpu.make_async_copy(panels_in, pieces, in_sems.at[0])
    tiles_copy = pltpu.make_async_copy(tiles_in, tiles, in_sems.at[1])
    panels_copy.start()
    tiles_copy.start()

    barrier = pltpu.get_barrier_semaphore()
    peers = [{"row": above}, {"row": below}]
    peers += [{"col": flipped(me_col, s)} for s in strides]
    for peer in peers:
        pl.semaphore_signal(barrier, inc=1, device_id=peer, device_id_type=mesh_id)
    pl.semaphore_wait(barrier, len(peers))

    def exchange(d, g, stage):
        held = [me_col]
        for s in strides[:stage]:
            held += [flipped(h, s) for h in held]
        base = sum(2**i for i in range(stage))
        copies = []
        for i, h in enumerate(held):
            where = (pl.ds(g * group, group), pl.ds(pl.multiple_of(h * height, height), height))
            copies.append(
                pltpu.make_async_remote_copy(
                    src_ref=panel[d].at[where],
                    dst_ref=panel[d].at[where],
                    send_sem=panel_sems[d].at[0, g, base + i],
                    recv_sem=panel_sems[d].at[1, g, base + i],
                    device_id={"col": flipped(me_col, strides[stage])},
                    device_id_type=mesh_id,
                )
            )
        return copies

    def lift(d, k):
        return pltpu.make_async_remote_copy(
            src_ref=lift_out[d].at[k],
            dst_ref=lift_in[d].at[k],
            send_sem=lift_sems[d].at[0, k],
            recv_sem=lift_sems[d].at[1, k],
            device_id={"row": above},
            device_id_type=mesh_id,
        )

    def give_back(d, k):
        return pltpu.make_async_remote_copy(
            src_ref=lower_new[d].at[k],
            dst_ref=back_in[d].at[k],
            send_sem=back_sems[d].at[0, k],
            recv_sem=back_sems[d].at[1, k],
            device_id={"row": below},
            device_id_type=mesh_id,
        )

    def pick_panels(d):
        mine = pl.ds(pl.multiple_of(me_col * height, height), height)

        def one(g, _):
            for i in range(group):
                panel[d][g * group + i, mine] = pieces[d, own(d, g * group + i)]
            if strides:
                for copy in exchange(d, g, 0):
                    copy.start()
            return 0

        lax.fori_loop(0, panel[d].shape[0] // group, one, 0)

    def forward(d, g):
        for stage in range(1, len(strides)):
            for copy in exchange(d, g, stage - 1):
                copy.wait_recv()
            for copy in exchange(d, g, stage):
                copy.start()

    def factor(d):
        count = panel[d].shape[0] // group

        def one(g, _):
            if strides:
                for copy in exchange(d, g, len(strides) - 1):
                    copy.wait_recv()

            @pl.when(g + 1 < count)
            def _():
                forward(d, g + 1)

            invert_and_store(panel[d], g * group, group, vh[d], vl[d], yh[d], yl[d])
            return 0

        forward(d, 0)
        lax.fori_loop(0, count, one, 0)

    def after_first(j):
        u, l = upper_slot(0, j), lower_slot(0, j)
        kept = jnp.where(l >= 0, back_in[0][jnp.maximum(l, 0)], tiles[j])
        return jnp.where(u >= 0, upper_new[0][jnp.maximum(u, 0)], kept)

    def send_lifts(d, value):
        def one(k, _):
            lift_out[d][k] = value(behind(d, k))

            @pl.when(k > 0)
            def _():
                lift(d, k - 1).start()

            return 0

        lax.fori_loop(0, lifts[d], one, 0)
        lift(d, lifts[d] - 1).start()

    def reflect(d, upper_of, lower_of):
        def one(k, _):
            @pl.when(k < lifts[d])
            def _():
                lift(d, k).wait_recv()

            upper, lower = upper_of(k), lower_of(k)
            band = upper.shape[0]
            stacked = split(jnp.concatenate([upper, lower], axis=0))
            solved = split(dot3((yh[d][k], yl[d][k]), stacked))
            change = dot3((vh[d][k], vl[d][k]), solved)
            lower_new[d][k] = lower - change[band:]
            upper_new[d][k] = upper - change[:band]

            @pl.when(k < backs[d])
            def _():
                give_back(d, k).start()

            return 0

        lax.fori_loop(0, slots[d], one, 0)

    def receive(d):
        def one(k, _):
            give_back(d, k).wait_recv()
            return 0

        lax.fori_loop(0, backs[d], one, 0)

    panels_copy.wait()
    pick_panels(0)
    tiles_copy.wait()
    send_lifts(0, lambda j: tiles[j])
    pick_panels(1)
    factor(0)
    reflect(0, lambda k: tiles[own(0, k)], lambda k: lift_in[0][k])
    factor(1)
    receive(0)
    send_lifts(1, after_first)

    def second_lower(k):
        kept = upper_slot(0, own(1, k))
        return jnp.where(kept >= 0, lower_new[0][jnp.maximum(kept, 0)], lift_in[1][k])

    reflect(1, lambda k: after_first(own(1, k)), second_lower)

    def merge(j, _):
        u = upper_slot(1, j)
        merged[j] = jnp.where(u >= 0, upper_new[1][jnp.maximum(u, 0)], after_first(j))
        return 0

    lax.fori_loop(0, depth, merge, 0)
    receive(1)

    def write(j):
        return pltpu.make_async_copy(merged.at[j], out.at[j], out_sems.at[j])

    def finish(j, _):
        l = lower_slot(1, j)
        merged[j] = jnp.where(l >= 0, back_in[1][jnp.maximum(l, 0)], merged[j])

        @pl.when(j > 0)
        def _():
            write(j - 1).start()

        return 0

    lax.fori_loop(0, depth, finish, 0)
    write(depth - 1).start()

    def drain(j, _):
        write(j).wait()
        return 0

    for d in range(2):
        for g in range(panel[d].shape[0] // group):
            for stage in range(len(strides)):
                for copy in exchange(d, g, stage):
                    copy.wait_send()

        def sent(k, _):
            lift(d, k).wait_send()
            return 0

        def returned(k, _):
            give_back(d, k).wait_send()
            return 0

        lax.fori_loop(0, lifts[d], sent, 0)
        lax.fori_loop(0, backs[d], returned, 0)
    lax.fori_loop(0, depth, drain, 0)


def whole(profile, index, table, tiles, panels):
    depth, band, columns = tiles.shape
    _, _, height, _ = panels.shape
    cols = lax.axis_size("col")
    long = height * cols
    n0, b0, b1, n1 = profile
    group = GROUPED
    padded = [-(-n // group) * group for n in (n0, n1)]
    f32, bf16 = jnp.float32, jnp.bfloat16
    tile_slots = lambda counts: [pltpu.VMEM((n, band, columns), f32) for n in counts]
    dma = pltpu.SemaphoreType.DMA
    scratch = [
        pltpu.VMEM(tiles.shape, f32),
        pltpu.VMEM(panels.shape, f32),
        [pltpu.VMEM((n, long, band), f32) for n in padded],
        [pltpu.VMEM((n, long, band), bf16) for n in padded],
        [pltpu.VMEM((n, long, band), bf16) for n in padded],
        [pltpu.VMEM((n, band, long), bf16) for n in padded],
        [pltpu.VMEM((n, band, long), bf16) for n in padded],
        tile_slots((n0, b1)),
        tile_slots((n0, n1)),
        tile_slots((n0, n1)),
        tile_slots((n0, n1)),
        tile_slots((b0, n1)),
        pltpu.VMEM(tiles.shape, f32),
        dma((2,)),
        [dma((2, n // group, max(cols - 1, 1))) for n in padded],
        [dma((2, n)) for n in (n0, b1)],
        [dma((2, n)) for n in (b0, n1)],
        dma((depth,)),
    ]
    any_spec = pl.BlockSpec(memory_space=pl.ANY)
    return pl.pallas_call(
        functools.partial(whole_kernel, profile, group),
        in_specs=[pl.BlockSpec(memory_space=pltpu.SMEM), any_spec, any_spec],
        out_specs=any_spec,
        out_shape=jax.ShapeDtypeStruct(tiles.shape, tiles.dtype),
        scratch_shapes=scratch,
        compiler_params=pltpu.CompilerParams(
            collective_id=1 + index, has_side_effects=True, vmem_limit_bytes=58 * 2**20
        ),
    )(table, tiles, panels)


def tables(active, row_index):
    rows, _, depth = active.shape
    both = active[:, 0] & active[:, 1]
    single = active & ~both[:, None]
    counts = jnp.sum(active.astype(jnp.int32), axis=-1)
    singles = jnp.sum(single.astype(jnp.int32), axis=-1)
    most, most_single = jnp.max(counts, axis=0), jnp.max(singles, axis=0)
    pair = jnp.stack([row_index, (row_index + rows - 1) % rows])
    on, alone = active[pair], single[pair]
    again = both[pair]
    here = jnp.arange(depth, dtype=jnp.int32)
    earlier = here[None, :] < here[:, None]
    before = lambda x: jnp.sum((earlier & x[..., None, :]).astype(jnp.int32), axis=-1)
    total = jnp.sum(alone.astype(jnp.int32), axis=-1, keepdims=True)
    rank = jnp.where(alone, before(alone), total + before(again)[:, None])
    slot = jnp.where(on, rank, -1)
    order = jnp.sum(jnp.where(slot[..., None, :] == here[:, None], here, 0), axis=-1)
    first_row = row_index == 0
    behind = jnp.where(first_row, jnp.minimum(order[1] + 1, depth - 1), order[1])
    returned = jnp.where(jnp.stack([alone[1, 0], on[1, 1]]), slot[1], -1)
    shifted = jnp.concatenate([jnp.full((2, 1), -1, slot.dtype), returned[:, :-1]], axis=1)
    returned = jnp.where(first_row, shifted, returned)
    table = jnp.concatenate([order[0], behind, slot[0], returned]).astype(jnp.int32)
    return table, most, most_single


def local(eigvec, reflectors, sweep_group):
    row_index = lax.axis_index("row")
    row_count = lax.axis_size("row")
    depth = eigvec.shape[0]
    diagonals = sweep_group.shape[0]
    active = share(sweep_group[:, :, 0]) >= 0
    tiles, panels = eigvec[:, 0], reflectors[:, :, 0]

    def general(table, active, tiles, panels):
        mine = lax.dynamic_index_in_dim(active, row_index, 0, keepdims=False)
        above = lax.dynamic_index_in_dim(
            active, (row_index + row_count - 1) % row_count, 0, keepdims=False
        )
        order, counts = ordering(jnp.stack([mine, above]))
        own = order[0]
        behind = jnp.where(row_index == 0, (order[1] + 1) % depth, order[1])
        return steps(depth, own, behind, counts, tiles, panels)

    if diagonals != 2:
        return general(None, active, tiles, panels)[:, None]
    table, most, alone = tables(active, row_index)
    profiles = [p for p in PROFILES if max(p) <= depth]
    small = depth <= max(PROFILES[-1])
    if small and (depth,) * 4 not in profiles:
        profiles.append((depth,) * 4)
    needs = (most[0], alone[0], alone[1], most[1])
    choice, missed = jnp.int32(0), jnp.bool_(True)
    for profile in profiles[: len(profiles) - small]:
        fits = functools.reduce(jnp.logical_and, [n <= s for n, s in zip(needs, profile)])
        missed = missed & ~fits
        choice = choice + missed.astype(jnp.int32)

    def branch(index, profile):
        return lambda table, active, tiles, panels: whole(profile, index, table, tiles, panels)

    branches = [branch(i, p) for i, p in enumerate(profiles)]
    if not small:
        branches.append(general)
    args = (table, active, tiles, panels)
    out = lax.switch(choice, branches, *args) if len(branches) > 1 else branches[0](*args)
    return out[:, None]


def solution(mesh):
    return jax.shard_map(
        local,
        mesh=mesh,
        in_specs=(
            P(None, "row", None, "col"),
            P(None, None, "row", "col", None),
            P(None, None, "row"),
        ),
        out_specs=P(None, "row", None, "col"),
        check_vma=False,
    )
```

```python
import functools

import jax
import jax.numpy as jnp
from jax import lax
from jax.experimental import pallas as pl
from jax.experimental.pallas import tpu as pltpu
from jax.sharding import PartitionSpec as P


GROUP = 2
CHUNKS = 2
PROFILES = (
    (12, 4, 4, 12), (12, 5, 5, 12), (13, 5, 5, 13), (13, 5, 6, 14),
    (15, 6, 6, 15), (16, 7, 7, 16), (20, 12, 12, 20),
)
GROUPED = 4


def split(x):
    high = x.astype(jnp.bfloat16)
    return high, (x - high.astype(jnp.float32)).astype(jnp.bfloat16)


def dot(a, b):
    return jnp.dot(a, b, preferred_element_type=jnp.float32)


def dot3(a, b):
    return dot(a[1], b[0]) + dot(a[0], b[1]) + dot(a[0], b[0])


def bounds(slots):
    inner = [slots * i // CHUNKS // GROUP * GROUP for i in range(CHUNKS)]
    return inner + [slots]


def chunk_shapes(slots, tiles):
    edges = bounds(slots)
    return [
        jax.ShapeDtypeStruct((high - low,) + tiles.shape[1:], tiles.dtype)
        for low, high in zip(edges[:-1], edges[1:])
    ]


def slot_of(chunks, k):
    for chunk in chunks:
        if k < chunk.shape[0]:
            return chunk.at[k]
        k -= chunk.shape[0]


def gather_kernel(slots, own, behind, panels, tiles, picked, *rest):
    diagonals = panels.shape[0]
    sent, sems = rest[:-1], rest[-1]

    def panel_copy(d, k):
        return pltpu.make_async_copy(
            panels.at[d, own[d, k]], picked.at[d, k], sems.at[d * slots + k]
        )

    def tile_copy(k):
        return pltpu.make_async_copy(
            tiles.at[behind[0, k]], slot_of(sent, k), sems.at[diagonals * slots + k]
        )

    for k in range(slots):
        tile_copy(k).start()
    for d in range(diagonals):
        for k in range(slots):
            panel_copy(d, k).start()
    for k in range(slots):
        tile_copy(k).wait()
    for d in range(diagonals):
        for k in range(slots):
            panel_copy(d, k).wait()


def gather(slots, own, behind, panels, tiles):
    diagonals = panels.shape[0]
    any_spec = pl.BlockSpec(memory_space=pl.ANY)
    return pl.pallas_call(
        functools.partial(gather_kernel, slots),
        grid_spec=pltpu.PrefetchScalarGridSpec(
            num_scalar_prefetch=2,
            grid=(1,),
            in_specs=[any_spec, any_spec],
            out_specs=[pl.BlockSpec(memory_space=pltpu.VMEM)] * (1 + CHUNKS),
            scratch_shapes=[pltpu.SemaphoreType.DMA(((diagonals + 1) * slots,))],
        ),
        out_shape=[
            jax.ShapeDtypeStruct((diagonals, slots) + panels.shape[2:], panels.dtype),
        ] + chunk_shapes(slots, tiles),
        name="gather",
    )(own, behind, panels, tiles)


def scatter_kernel(slots, diagonal, more, behind, counts, tiles, *rest):
    returned, out, sent, sems = rest[:CHUNKS], rest[CHUNKS], rest[CHUNKS + 1:-1], rest[-1]

    def put(k):
        return pltpu.make_async_copy(
            slot_of(returned, k), out.at[behind[diagonal, k]], sems.at[k]
        )

    for k in range(slots):
        @pl.when(k < counts[1, diagonal])
        def _():
            put(k).start()
    for k in range(slots):
        @pl.when(k < counts[1, diagonal])
        def _():
            put(k).wait()
    if more:

        def take(k):
            return pltpu.make_async_copy(
                out.at[behind[diagonal + 1, k]], slot_of(sent, k), sems.at[slots + k]
            )

        for k in range(slots):
            take(k).start()
        for k in range(slots):
            take(k).wait()


def scatter(slots, diagonal, more, behind, counts, tiles, returned):
    any_spec = pl.BlockSpec(memory_space=pl.ANY)
    vmem_spec = pl.BlockSpec(memory_space=pltpu.VMEM)
    shapes = [jax.ShapeDtypeStruct(tiles.shape, tiles.dtype)]
    if more:
        shapes += chunk_shapes(slots, tiles)
    return pl.pallas_call(
        functools.partial(scatter_kernel, slots, diagonal, more),
        grid_spec=pltpu.PrefetchScalarGridSpec(
            num_scalar_prefetch=2,
            grid=(1,),
            in_specs=[any_spec] + [vmem_spec] * CHUNKS,
            out_specs=[any_spec] + [vmem_spec] * (len(shapes) - 1),
            scratch_shapes=[pltpu.SemaphoreType.DMA((2 * slots,))],
        ),
        out_shape=shapes,
        input_output_aliases={2: 0},
        name="scatter",
    )(behind, counts, tiles, *returned)


def factor_kernel(pieces_count, col_ref, *refs):
    pieces = refs[:pieces_count]
    vh_ref, vl_ref, yh_ref, yl_ref = refs[pieces_count:]
    me = col_ref[0]
    group = pieces[0].shape[1]
    band = pieces[0].shape[-1]
    depth = pieces_count * pieces[0].shape[2]
    row = lax.broadcasted_iota(jnp.int32, (depth, band), 0)
    col = lax.broadcasted_iota(jnp.int32, (depth, band), 1)
    inside = (row >= col + 1) & (row <= col + band)
    leading = row == col + 1
    r = lax.broadcasted_iota(jnp.int32, (band, band), 0)
    c = lax.broadcasted_iota(jnp.int32, (band, band), 1)
    slots = range(group)
    vs, ts, factors, inverses = [], [], [], []
    for g in slots:
        parts = [piece[0, g] for piece in pieces]
        stride = 1
        while stride < pieces_count:
            odd = (me // stride) % 2 == 1
            parts = [
                jnp.where(odd, parts[j ^ stride], parts[j]) for j in range(pieces_count)
            ]
            stride *= 2
        panel = jnp.concatenate(parts, axis=0)
        v = jnp.where(leading, 1.0, jnp.where(inside, panel, 0.0))
        vs.append(split(v))
        ts.append(split(v.T))
        vh_ref[g] = vs[g][0]
        vl_ref[g] = vs[g][1]
    for g in slots:
        gram = dot3(ts[g], vs[g])
        diagonal = jnp.sum(jnp.where(r == c, gram, 0.0), axis=0, keepdims=True)
        factors.append(gram)
        inverses.append(jnp.where(r == c, 2.0 / diagonal, 0.0))

    def level(n, inverses):
        coupling = ((r >> n) != (c >> n)) & ((r >> (n + 1)) == (c >> (n + 1))) & (r < c)
        inverse_parts = [split(inverse) for inverse in inverses]
        middles = [
            split(dot3(split(jnp.where(coupling, factors[g], 0.0)), inverse_parts[g]))
            for g in slots
        ]
        return tuple(inverses[g] - dot3(inverse_parts[g], middles[g]) for g in slots)

    inverses = lax.fori_loop(0, (band - 1).bit_length(), level, tuple(inverses))
    for g in slots:
        high, low = split(dot3(split(inverses[g]), ts[g]))
        yh_ref[g] = high
        yl_ref[g] = low


def factor(first, slots, diagonal, col, pieces):
    count = len(pieces)
    _, _, height, band = pieces[0].shape
    depth = count * height
    group = GROUP if slots % GROUP == 0 else 1
    start = first // group
    kind = jnp.bfloat16
    return pl.pallas_call(
        functools.partial(factor_kernel, count),
        grid_spec=pltpu.PrefetchScalarGridSpec(
            num_scalar_prefetch=1,
            grid=(slots // group,),
            in_specs=[
                pl.BlockSpec((1, group, height, band), lambda k, c: (diagonal, k + start, 0, 0))
            ] * count,
            out_specs=[pl.BlockSpec((group, depth, band), lambda k, c: (k, 0, 0))] * 2
            + [pl.BlockSpec((group, band, depth), lambda k, c: (k, 0, 0))] * 2,
        ),
        out_shape=[jax.ShapeDtypeStruct((slots, depth, band), kind)] * 2
        + [jax.ShapeDtypeStruct((slots, band, depth), kind)] * 2,
        name="factor",
    )(col, *pieces)


def apply_kernel(diagonal, first, own, counts, tile, below, vh, vl, yh, yl, tile_out, below_out):
    k = pl.program_id(0) + first
    band = tile.shape[1]
    upper, lower = tile[0], below[0]
    stacked = jnp.concatenate([upper, lower], axis=0)
    solved = dot3((yh[0], yl[0]), split(stacked))
    change = dot3((vh[0], vl[0]), split(solved))
    active = k < counts[0, diagonal]
    tile_out[0] = jnp.where(active, upper - change[:band], upper)
    below_out[0] = jnp.where(active, lower - change[band:], lower)


def apply(first, diagonal, own, counts, tiles, beneath, vh, vl, yh, yl):
    _, band, columns = tiles.shape
    depth = vh.shape[1]
    at_slot = lambda k, own, counts: (k, 0, 0)
    at_own = lambda k, own, counts: (own[diagonal, k + first], 0, 0)
    return pl.pallas_call(
        functools.partial(apply_kernel, diagonal, first),
        grid_spec=pltpu.PrefetchScalarGridSpec(
            num_scalar_prefetch=2,
            grid=(beneath.shape[0],),
            in_specs=[
                pl.BlockSpec((1, band, columns), at_own),
                pl.BlockSpec((1, band, columns), at_slot),
                pl.BlockSpec((1, depth, band), at_slot),
                pl.BlockSpec((1, depth, band), at_slot),
                pl.BlockSpec((1, band, depth), at_slot),
                pl.BlockSpec((1, band, depth), at_slot),
            ],
            out_specs=[
                pl.BlockSpec((1, band, columns), at_own),
                pl.BlockSpec((1, band, columns), at_slot),
            ],
        ),
        out_shape=[
            jax.ShapeDtypeStruct(tiles.shape, tiles.dtype),
            jax.ShapeDtypeStruct(beneath.shape, beneath.dtype),
        ],
        input_output_aliases={2: 0},
        name="apply",
    )(own, counts, tiles, beneath, vh, vl, yh, yl)


def lift(sent, to_above):
    beneath = []
    for chunk in sent:
        beneath.append(lax.ppermute(chunk, "row", to_above))
    return beneath


def steps(slots, own, behind, counts, tiles, panels):
    row_count = lax.axis_size("row")
    col_count = lax.axis_size("col")
    col = lax.axis_index("col").astype(jnp.int32)[None]
    diagonals = panels.shape[0]
    to_above = [(i, (i - 1) % row_count) for i in range(row_count)]
    to_below = [(i, (i + 1) % row_count) for i in range(row_count)]
    picked, *sent = gather(slots, own, behind, panels, tiles)
    beneath = lift(sent, to_above)
    pieces = {0: picked}
    stride = col_count // 2
    while stride >= 1:
        swap = [(i, i ^ stride) for i in range(col_count)]
        pieces.update(
            {q ^ stride: lax.ppermute(p, "col", swap) for q, p in pieces.items()}
        )
        stride //= 2
    pieces = [pieces[q] for q in range(col_count)]
    for diagonal in range(diagonals):
        returned = []
        for first, chunk in zip(bounds(slots), beneath):
            factors = factor(first, chunk.shape[0], diagonal, col, pieces)
            tiles, lower = apply(first, diagonal, own, counts, tiles, chunk, *factors)
            returned.append(lax.ppermute(lower, "row", to_below))
        more = diagonal + 1 < diagonals
        tiles, *sent = scatter(slots, diagonal, more, behind, counts, tiles, returned)
        if more:
            beneath = lift(sent, to_above)
    return tiles


def plan_kernel(profiles, flags, table, choice, everyone, mine, held, send, recv):
    count, _, lanes = held.shape
    diagonals, depth = flags.shape
    me = lax.axis_index("row")
    mine[...] = jnp.full(mine.shape, -1, mine.dtype)
    mine[0:diagonals, 0:depth] = flags[...]
    barrier = pltpu.get_barrier_semaphore()
    mesh_id = pl.DeviceIdType.MESH
    others = [lax.rem(me + by, count) for by in range(1, count)]
    for other in others:
        pl.semaphore_signal(
            barrier, inc=1, device_id={"row": other}, device_id_type=mesh_id
        )
    pl.semaphore_wait(barrier, count - 1)
    copies = [
        pltpu.make_async_remote_copy(
            src_ref=mine,
            dst_ref=held.at[me],
            send_sem=send.at[i],
            recv_sem=recv.at[i],
            device_id={"row": other},
            device_id_type=mesh_id,
        )
        for i, other in enumerate(others)
    ]
    for copy in copies:
        copy.start()
    held[me] = mine[...]
    for copy in copies:
        copy.wait()
    everyone[...] = held[...]

    f32 = jnp.float32
    row = lax.broadcasted_iota(jnp.int32, (count, lanes), 0)
    on = [jnp.where(held[:, d, :] >= 0, 1.0, 0.0) for d in range(2)]
    after = []
    for x in on:
        under = pltpu.roll(x, count - 1, axis=0)
        after.append(jnp.where(row == count - 1, pltpu.roll(under, lanes - 1, axis=1), under))
    again = on[0] * on[1]
    first, second = on[0] - again, on[1] - again
    kinds = [
        first * after[1],
        first - first * after[1],
        again,
        second - second * after[0],
        second * after[0],
    ]
    sums = [jnp.sum(x, axis=1, keepdims=True) for x in kinds]
    must, may, rep, ready, unready = sums
    chosen = [jnp.zeros((1, 1), f32) for _ in range(4)]
    index, missed = jnp.zeros((1, 1), f32), jnp.ones((1, 1), f32)
    for early, soon, late, last in profiles:
        bad = (must + may + rep > early) | (must > soon)
        bad |= rep + ready + unready + jnp.maximum(must + may - soon, 0.0) > last
        bad |= unready + jnp.maximum(ready - (early - must - may - rep), 0.0) > late
        still = missed * jnp.max(jnp.where(bad, 1.0, 0.0), axis=0, keepdims=True)
        for i, size in enumerate((early, soon, late, last)):
            chosen[i] = chosen[i] + (missed - still) * size
        index, missed = index + still, still
    choice[0] = index[0, 0].astype(jnp.int32)
    early, soon, late, last = chosen

    above = lax.rem(me + count - 1, count)
    picked = [
        jnp.sum(jnp.where(row == who, x, 0.0), axis=0, keepdims=True)
        for who in (me, above)
        for x in kinds
    ]
    none = jnp.zeros((1, lanes), f32)
    stacked = jnp.concatenate(picked + [none] * 6, axis=0)
    r = lax.broadcasted_iota(jnp.int32, (lanes, lanes), 0)
    c = lax.broadcasted_iota(jnp.int32, (lanes, lanes), 1)
    ahead = jnp.dot(
        stacked.astype(jnp.bfloat16),
        jnp.where(r < c, 1.0, 0.0).astype(jnp.bfloat16),
        preferred_element_type=f32,
    )
    totals = jnp.sum(stacked, axis=1, keepdims=True)

    def places(which):
        at = [stacked[5 * which + i : 5 * which + i + 1] > 0.5 for i in range(5)]
        rank = [ahead[5 * which + i : 5 * which + i + 1] for i in range(5)]
        must, may, rep, ready, unready = [
            totals[5 * which + i : 5 * which + i + 1] for i in range(5)
        ]
        slot0 = jnp.where(
            at[0],
            rank[0],
            jnp.where(at[1], must + rank[1], jnp.where(at[2], must + may + rank[2], -1.0)),
        )
        taken = must + may + rep
        spare = early - taken
        over = jnp.maximum(ready - spare, 0.0)
        tardy = over + unready
        prompt = rep + ready - over

        def placed(p):
            return jnp.where(p < last - late, p, p + tardy)

        fast = at[3] & (rank[3] < spare)
        lag = jnp.where(
            at[4], over + rank[4], jnp.where(at[3] & ~fast, rank[3] - spare, -1.0)
        )
        slot1 = jnp.where(
            at[2],
            placed(rank[2]),
            jnp.where(fast, placed(rep + rank[3]), jnp.where(lag >= 0, last - late + lag, -1.0)),
        )
        single = at[0] | at[1]
        held_back = single & (slot0 >= soon)
        kept = jnp.where(held_back, placed(prompt + slot0 - soon), -1.0)
        sooner = jnp.where(single & (slot0 < soon), slot0, -1.0)
        ahead_of = jnp.where(fast, taken + rank[3], -1.0)
        return at, slot0, slot1, kept, sooner, ahead_of, lag

    at, slot0, slot1, kept, _, ahead_of, _ = places(0)
    _, up0, up1, up_kept, up_sooner, up_ahead, up_lag = places(1)
    keys = [
        slot0,
        slot1,
        kept,
        jnp.maximum(up0, up_ahead),
        up_lag,
        jnp.where(at[2], slot0, -1.0),
        ahead_of,
        none,
    ]
    filler = jnp.zeros((lanes - len(keys), lanes), f32)
    turned = jnp.concatenate(keys + [filler], axis=0).T
    column = lambda i: turned[:, i : i + 1]
    tile = r.astype(f32)
    place = c.astype(f32)

    def turn(key, value, missing):
        hit = jnp.where(column(key) == place, value - missing, 0.0)
        return jnp.sum(hit, axis=0, keepdims=True) + missing

    top = me == 0

    def behind(key):
        found = turn(key, tile, 0.0)
        return jnp.where(top, jnp.minimum(found + 1.0, depth - 1.0), found)

    def below(x):
        return jnp.where(top, pltpu.roll(x, 1, axis=1), x)

    rows = [
        turn(0, tile, 0.0),
        turn(1, tile, 0.0),
        behind(3),
        behind(4),
        slot0,
        slot1,
        below(up_sooner),
        below(jnp.maximum(up1, up_kept)),
        turn(1, column(5), -1.0),
        turn(1, column(6), -1.0),
        turn(2, column(0), -1.0),
    ]
    rows += [none] * (table.shape[0] - len(rows))
    table[...] = jnp.concatenate(rows, axis=0).astype(jnp.int32)


def plan(profiles, flags):
    count = lax.axis_size("row")
    lanes = 128
    vmem_spec = pl.BlockSpec(memory_space=pltpu.VMEM)
    shape = (count, 8, lanes)
    kind = flags.dtype
    return pl.pallas_call(
        functools.partial(plan_kernel, profiles),
        out_shape=[
            jax.ShapeDtypeStruct((16, lanes), kind),
            jax.ShapeDtypeStruct((1,), kind),
            jax.ShapeDtypeStruct(shape, kind),
        ],
        in_specs=[vmem_spec],
        out_specs=[vmem_spec, pl.BlockSpec(memory_space=pltpu.SMEM), vmem_spec],
        scratch_shapes=[
            pltpu.VMEM(shape[1:], kind),
            pltpu.VMEM(shape, kind),
            pltpu.SemaphoreType.DMA((count - 1,)),
            pltpu.SemaphoreType.DMA((count - 1,)),
        ],
        compiler_params=pltpu.CompilerParams(collective_id=0, has_side_effects=True),
        name="plan",
    )(flags)


def fresh_kernel(x, out):
    out[...] = x[...]


def fresh(x):
    spec = pl.BlockSpec((1,) + x.shape[1:], lambda k: (k, 0, 0))
    return pl.pallas_call(
        fresh_kernel,
        grid=(x.shape[0],),
        in_specs=[spec],
        out_specs=spec,
        out_shape=jax.ShapeDtypeStruct(x.shape, x.dtype),
        name="fresh",
    )(x)


def ordering(active):
    depth = active.shape[-1]
    here = jnp.arange(depth, dtype=jnp.int32)
    on = active.astype(jnp.int32)
    earlier = here[None, :] < here[:, None]
    before = jnp.sum(jnp.where(earlier, on[..., None, :], 0), axis=-1)
    total = jnp.sum(on, axis=-1)
    rank = jnp.where(active, before, total[..., None] + here - before)
    order = jnp.sum(
        jnp.where(rank[..., None, :] == here[:, None], here, 0), axis=-1
    ).astype(jnp.int32)
    return order, total.astype(jnp.int32)


def flipped(index, stride):
    return index + stride - 2 * stride * lax.rem(lax.div(index, stride), 2)


def invert_and_store(panels, first, count, vh_ref, vl_ref, yh_ref, yl_ref):
    depth, band = panels.shape[1:]
    row = lax.broadcasted_iota(jnp.int32, (depth, band), 0)
    col = lax.broadcasted_iota(jnp.int32, (depth, band), 1)
    inside = (row >= col + 1) & (row <= col + band)
    leading = row == col + 1
    r = lax.broadcasted_iota(jnp.int32, (band, band), 0)
    c = lax.broadcasted_iota(jnp.int32, (band, band), 1)
    slots = range(count)
    ts, factors, inverses = [], [], []
    for g in slots:
        v = jnp.where(leading, 1.0, jnp.where(inside, panels[first + g], 0.0))
        vs = split(v)
        ts.append(split(v.T))
        vh_ref[first + g] = vs[0]
        vl_ref[first + g] = vs[1]
        gram = dot3(ts[g], vs)
        diagonal = jnp.sum(jnp.where(r == c, gram, 0.0), axis=0, keepdims=True)
        factors.append(gram)
        inverses.append(jnp.where(r == c, 2.0 / diagonal, 0.0))

    def level(n, inverses):
        coupling = ((r >> n) != (c >> n)) & ((r >> (n + 1)) == (c >> (n + 1))) & (r < c)
        inverse_parts = [split(inverse) for inverse in inverses]
        middles = [
            split(dot3(split(jnp.where(coupling, factors[g], 0.0)), inverse_parts[g]))
            for g in slots
        ]
        return tuple(inverses[g] - dot3(inverse_parts[g], middles[g]) for g in slots)

    inverses = lax.fori_loop(0, (band - 1).bit_length(), level, tuple(inverses))
    for g in slots:
        high, low = split(dot3(split(inverses[g]), ts[g]))
        yh_ref[first + g] = high
        yl_ref[first + g] = low


def whole_kernel(
    profile, group, table, tiles_in, panels_in, out,
    tiles, pieces, panel, vh, vl, yh, yl, lift_out, lift_in, upper_new, lower_new, back_in,
    merged, in_sems, panel_sems, lift_sems, back_sems, out_sems,
):
    early, soon, late, last = profile
    slots, lifts, backs = (early, last), (early, late), (soon, last)
    skip = (0, last - late)
    depth = tiles.shape[0]
    height = pieces.shape[2]
    rows = lax.axis_size("row")
    cols = lax.axis_size("col")
    me_row = lax.axis_index("row")
    me_col = lax.axis_index("col")
    above = lax.rem(me_row + rows - 1, rows)
    below = lax.rem(me_row + 1, rows)
    mesh_id = pl.DeviceIdType.MESH
    strides = []
    stride = cols // 2
    while stride >= 1:
        strides.append(stride)
        stride //= 2
    own = lambda d, k: table[d, k]
    behind = lambda d, k: table[2 + d, k]
    upper_slot = lambda d, j: table[4 + d, j]
    lower_slot = lambda d, j: table[6 + d, j]

    def either(source, index, other):
        return jnp.where(index >= 0, source[jnp.maximum(index, 0)], other)


    panels_copy = pltpu.make_async_copy(panels_in, pieces, in_sems.at[0])
    tiles_copy = pltpu.make_async_copy(tiles_in, tiles, in_sems.at[1])
    panels_copy.start()
    tiles_copy.start()

    barrier = pltpu.get_barrier_semaphore()
    peers = [{"row": above}, {"row": below}]
    peers += [{"col": flipped(me_col, s)} for s in strides]
    for peer in peers:
        pl.semaphore_signal(barrier, inc=1, device_id=peer, device_id_type=mesh_id)
    pl.semaphore_wait(barrier, len(peers))

    def exchange(d, g, stage):
        held = [me_col]
        for s in strides[:stage]:
            held += [flipped(h, s) for h in held]
        base = sum(2**i for i in range(stage))
        copies = []
        for i, h in enumerate(held):
            where = (pl.ds(g * group, group), pl.ds(pl.multiple_of(h * height, height), height))
            copies.append(
                pltpu.make_async_remote_copy(
                    src_ref=panel[d].at[where],
                    dst_ref=panel[d].at[where],
                    send_sem=panel_sems[d].at[0, g, base + i],
                    recv_sem=panel_sems[d].at[1, g, base + i],
                    device_id={"col": flipped(me_col, strides[stage])},
                    device_id_type=mesh_id,
                )
            )
        return copies

    def lift(d, k):
        return pltpu.make_async_remote_copy(
            src_ref=lift_out[d].at[k],
            dst_ref=lift_in[d].at[skip[d] + k],
            send_sem=lift_sems[d].at[0, k],
            recv_sem=lift_sems[d].at[1, k],
            device_id={"row": above},
            device_id_type=mesh_id,
        )

    def give_back(d, k):
        return pltpu.make_async_remote_copy(
            src_ref=lower_new[d].at[k],
            dst_ref=back_in[d].at[k],
            send_sem=back_sems[d].at[0, k],
            recv_sem=back_sems[d].at[1, k],
            device_id={"row": below},
            device_id_type=mesh_id,
        )

    def pick_panels(d):
        mine = pl.ds(pl.multiple_of(me_col * height, height), height)

        def one(g, _):
            for i in range(group):
                panel[d][g * group + i, mine] = pieces[d, own(d, g * group + i)]
            if strides:
                for copy in exchange(d, g, 0):
                    copy.start()
            return 0

        lax.fori_loop(0, panel[d].shape[0] // group, one, 0)

    def forward(d, g):
        for stage in range(1, len(strides)):
            for copy in exchange(d, g, stage - 1):
                copy.wait_recv()
            for copy in exchange(d, g, stage):
                copy.start()

    def factor(d):
        count = panel[d].shape[0] // group

        def one(g, _):
            if strides:
                for copy in exchange(d, g, len(strides) - 1):
                    copy.wait_recv()

            @pl.when(g + 1 < count)
            def _():
                forward(d, g + 1)

            invert_and_store(panel[d], g * group, group, vh[d], vl[d], yh[d], yl[d])
            return 0

        forward(d, 0)
        lax.fori_loop(0, count, one, 0)

    def after_first(j):
        kept = either(back_in[0], lower_slot(0, j), tiles[j])
        return either(upper_new[0], upper_slot(0, j), kept)

    def send_lifts(d, value):
        def one(k, _):
            lift_out[d][k] = value(behind(d, k))

            @pl.when(k > 0)
            def _():
                lift(d, k - 1).start()

            return 0

        lax.fori_loop(0, lifts[d], one, 0)
        lift(d, lifts[d] - 1).start()

    def reflect(d, upper_of, lower_of, sent_of):
        def one(k, _):
            @pl.when(k >= skip[d])
            def _():
                lift(d, k - skip[d]).wait_recv()

            upper, lower = upper_of(k), lower_of(k)
            band = upper.shape[0]
            stacked = split(jnp.concatenate([upper, lower], axis=0))
            solved = split(dot3((yh[d][k], yl[d][k]), stacked))
            change = dot3((vh[d][k], vl[d][k]), solved)
            lower_new[d][k] = sent_of(k, lower - change[band:])
            upper_new[d][k] = upper - change[:band]

            @pl.when(k < backs[d])
            def _():
                give_back(d, k).start()

            return 0

        lax.fori_loop(0, slots[d], one, 0)

    def receive(d):
        def one(k, _):
            give_back(d, k).wait_recv()
            return 0

        lax.fori_loop(0, backs[d], one, 0)

    panels_copy.wait()
    pick_panels(0)
    tiles_copy.wait()
    send_lifts(0, lambda j: tiles[j])
    pick_panels(1)
    factor(0)
    reflect(0, lambda k: tiles[own(0, k)], lambda k: lift_in[0][k], lambda k, lower: lower)
    factor(1)
    receive(0)
    send_lifts(1, after_first)

    def second_lower(k):
        arrived = either(lift_in[0], table[9, k], lift_in[1][k])
        return either(lower_new[0], table[8, k], arrived)

    reflect(
        1,
        lambda k: after_first(own(1, k)),
        second_lower,
        lambda k, lower: either(lower_new[0], table[10, k], lower),
    )

    def merge(j, _):
        merged[j] = either(upper_new[1], upper_slot(1, j), after_first(j))
        return 0

    lax.fori_loop(0, depth, merge, 0)
    receive(1)

    def write(j):
        return pltpu.make_async_copy(merged.at[j], out.at[j], out_sems.at[j])

    def finish(j, _):
        merged[j] = either(back_in[1], lower_slot(1, j), merged[j])

        @pl.when(j > 0)
        def _():
            write(j - 1).start()

        return 0

    lax.fori_loop(0, depth, finish, 0)
    write(depth - 1).start()

    def drain(j, _):
        write(j).wait()
        return 0

    for d in range(2):
        for g in range(panel[d].shape[0] // group):
            for stage in range(len(strides)):
                for copy in exchange(d, g, stage):
                    copy.wait_send()

        def sent(k, _):
            lift(d, k).wait_send()
            return 0

        def returned(k, _):
            give_back(d, k).wait_send()
            return 0

        lax.fori_loop(0, lifts[d], sent, 0)
        lax.fori_loop(0, backs[d], returned, 0)
    lax.fori_loop(0, depth, drain, 0)


def whole(profile, index, table, tiles, panels):
    depth, band, columns = tiles.shape
    _, _, height, _ = panels.shape
    cols = lax.axis_size("col")
    long = height * cols
    early, soon, late, last = profile
    group = GROUPED
    padded = [-(-n // group) * group for n in (early, last)]
    f32, bf16 = jnp.float32, jnp.bfloat16
    tile_slots = lambda counts: [pltpu.VMEM((n, band, columns), f32) for n in counts]
    dma = pltpu.SemaphoreType.DMA
    scratch = [
        pltpu.VMEM(tiles.shape, f32),
        pltpu.VMEM(panels.shape, f32),
        [pltpu.VMEM((n, long, band), f32) for n in padded],
        [pltpu.VMEM((n, long, band), bf16) for n in padded],
        [pltpu.VMEM((n, long, band), bf16) for n in padded],
        [pltpu.VMEM((n, band, long), bf16) for n in padded],
        [pltpu.VMEM((n, band, long), bf16) for n in padded],
        tile_slots((early, late)),
        tile_slots((early, last)),
        tile_slots((early, last)),
        tile_slots((early, last)),
        tile_slots((soon, last)),
        pltpu.VMEM(tiles.shape, f32),
        dma((2,)),
        [dma((2, n // group, max(cols - 1, 1))) for n in padded],
        [dma((2, n)) for n in (early, late)],
        [dma((2, n)) for n in (soon, last)],
        dma((depth,)),
    ]
    any_spec = pl.BlockSpec(memory_space=pl.ANY)
    return pl.pallas_call(
        functools.partial(whole_kernel, profile, group),
        in_specs=[pl.BlockSpec(memory_space=pltpu.SMEM), any_spec, any_spec],
        out_specs=any_spec,
        out_shape=jax.ShapeDtypeStruct(tiles.shape, tiles.dtype),
        scratch_shapes=scratch,
        compiler_params=pltpu.CompilerParams(
            collective_id=1 + index, has_side_effects=True, vmem_limit_bytes=58 * 2**20
        ),
    )(table, tiles, panels)


def local(eigvec, reflectors, sweep_group):
    row_index = lax.axis_index("row")
    row_count = lax.axis_size("row")
    depth = eigvec.shape[0]
    profiles = [p for p in PROFILES if max(p) <= depth]
    small = depth <= max(PROFILES[-1])
    if small and (depth,) * 4 not in profiles:
        profiles.append((depth,) * 4)
    table, choice, flags = plan(profiles, sweep_group[:, :, 0])

    def general(table, flags, tiles, panels):
        active = flags[:, : sweep_group.shape[0], :depth] >= 0
        mine = lax.dynamic_index_in_dim(active, row_index, 0, keepdims=False)
        above = lax.dynamic_index_in_dim(
            active, (row_index + row_count - 1) % row_count, 0, keepdims=False
        )
        order, counts = ordering(jnp.stack([mine, above]))
        own = order[0]
        behind = jnp.where(row_index == 0, (order[1] + 1) % depth, order[1])
        return steps(depth, own, behind, counts, fresh(tiles), panels)

    def branch(index, profile):
        return lambda table, flags, tiles, panels: whole(profile, index, table, tiles, panels)

    branches = [branch(i, p) for i, p in enumerate(profiles)]
    if not small:
        branches.append(general)
    args = (table, flags, eigvec[:, 0], reflectors[:, :, 0])
    out = lax.switch(choice[0], branches, *args) if len(branches) > 1 else branches[0](*args)
    return out[:, None]


def solution(mesh):
    return jax.shard_map(
        local,
        mesh=mesh,
        in_specs=(
            P(None, "row", None, "col"),
            P(None, None, "row", "col", None),
            P(None, None, "row"),
        ),
        out_specs=P(None, "row", None, "col"),
        check_vma=False,
    )
```

```python
import functools

import jax
import jax.numpy as jnp
from jax import lax
from jax.experimental import pallas as pl
from jax.experimental.pallas import tpu as pltpu
from jax.sharding import PartitionSpec as P


GROUP = 2
CHUNKS = 2
PROFILES = (
    (12, 4, 4, 12), (12, 5, 5, 12), (13, 5, 5, 13), (13, 5, 6, 14),
    (15, 6, 6, 15), (16, 7, 7, 16), (20, 12, 12, 20),
)
GROUPED = 4


def split(x):
    high = x.astype(jnp.bfloat16)
    return high, (x - high.astype(jnp.float32)).astype(jnp.bfloat16)


def dot(a, b):
    return jnp.dot(a, b, preferred_element_type=jnp.float32)


def dot3(a, b):
    return dot(a[1], b[0]) + dot(a[0], b[1]) + dot(a[0], b[0])


def bounds(slots):
    inner = [slots * i // CHUNKS // GROUP * GROUP for i in range(CHUNKS)]
    return inner + [slots]


def chunk_shapes(slots, tiles):
    edges = bounds(slots)
    return [
        jax.ShapeDtypeStruct((high - low,) + tiles.shape[1:], tiles.dtype)
        for low, high in zip(edges[:-1], edges[1:])
    ]


def slot_of(chunks, k):
    for chunk in chunks:
        if k < chunk.shape[0]:
            return chunk.at[k]
        k -= chunk.shape[0]


def gather_kernel(slots, own, behind, panels, tiles, picked, *rest):
    diagonals = panels.shape[0]
    sent, sems = rest[:-1], rest[-1]

    def panel_copy(d, k):
        return pltpu.make_async_copy(
            panels.at[d, own[d, k]], picked.at[d, k], sems.at[d * slots + k]
        )

    def tile_copy(k):
        return pltpu.make_async_copy(
            tiles.at[behind[0, k]], slot_of(sent, k), sems.at[diagonals * slots + k]
        )

    for k in range(slots):
        tile_copy(k).start()
    for d in range(diagonals):
        for k in range(slots):
            panel_copy(d, k).start()
    for k in range(slots):
        tile_copy(k).wait()
    for d in range(diagonals):
        for k in range(slots):
            panel_copy(d, k).wait()


def gather(slots, own, behind, panels, tiles):
    diagonals = panels.shape[0]
    any_spec = pl.BlockSpec(memory_space=pl.ANY)
    return pl.pallas_call(
        functools.partial(gather_kernel, slots),
        grid_spec=pltpu.PrefetchScalarGridSpec(
            num_scalar_prefetch=2,
            grid=(1,),
            in_specs=[any_spec, any_spec],
            out_specs=[pl.BlockSpec(memory_space=pltpu.VMEM)] * (1 + CHUNKS),
            scratch_shapes=[pltpu.SemaphoreType.DMA(((diagonals + 1) * slots,))],
        ),
        out_shape=[
            jax.ShapeDtypeStruct((diagonals, slots) + panels.shape[2:], panels.dtype),
        ] + chunk_shapes(slots, tiles),
        name="gather",
    )(own, behind, panels, tiles)


def scatter_kernel(slots, diagonal, more, behind, counts, tiles, *rest):
    returned, out, sent, sems = rest[:CHUNKS], rest[CHUNKS], rest[CHUNKS + 1:-1], rest[-1]

    def put(k):
        return pltpu.make_async_copy(
            slot_of(returned, k), out.at[behind[diagonal, k]], sems.at[k]
        )

    for k in range(slots):
        @pl.when(k < counts[1, diagonal])
        def _():
            put(k).start()
    for k in range(slots):
        @pl.when(k < counts[1, diagonal])
        def _():
            put(k).wait()
    if more:

        def take(k):
            return pltpu.make_async_copy(
                out.at[behind[diagonal + 1, k]], slot_of(sent, k), sems.at[slots + k]
            )

        for k in range(slots):
            take(k).start()
        for k in range(slots):
            take(k).wait()


def scatter(slots, diagonal, more, behind, counts, tiles, returned):
    any_spec = pl.BlockSpec(memory_space=pl.ANY)
    vmem_spec = pl.BlockSpec(memory_space=pltpu.VMEM)
    shapes = [jax.ShapeDtypeStruct(tiles.shape, tiles.dtype)]
    if more:
        shapes += chunk_shapes(slots, tiles)
    return pl.pallas_call(
        functools.partial(scatter_kernel, slots, diagonal, more),
        grid_spec=pltpu.PrefetchScalarGridSpec(
            num_scalar_prefetch=2,
            grid=(1,),
            in_specs=[any_spec] + [vmem_spec] * CHUNKS,
            out_specs=[any_spec] + [vmem_spec] * (len(shapes) - 1),
            scratch_shapes=[pltpu.SemaphoreType.DMA((2 * slots,))],
        ),
        out_shape=shapes,
        input_output_aliases={2: 0},
        name="scatter",
    )(behind, counts, tiles, *returned)


def factor_kernel(pieces_count, col_ref, *refs):
    pieces = refs[:pieces_count]
    vh_ref, vl_ref, yh_ref, yl_ref = refs[pieces_count:]
    me = col_ref[0]
    group = pieces[0].shape[1]
    band = pieces[0].shape[-1]
    depth = pieces_count * pieces[0].shape[2]
    row = lax.broadcasted_iota(jnp.int32, (depth, band), 0)
    col = lax.broadcasted_iota(jnp.int32, (depth, band), 1)
    inside = (row >= col + 1) & (row <= col + band)
    leading = row == col + 1
    r = lax.broadcasted_iota(jnp.int32, (band, band), 0)
    c = lax.broadcasted_iota(jnp.int32, (band, band), 1)
    slots = range(group)
    vs, ts, factors, inverses = [], [], [], []
    for g in slots:
        parts = [piece[0, g] for piece in pieces]
        stride = 1
        while stride < pieces_count:
            odd = (me // stride) % 2 == 1
            parts = [
                jnp.where(odd, parts[j ^ stride], parts[j]) for j in range(pieces_count)
            ]
            stride *= 2
        panel = jnp.concatenate(parts, axis=0)
        v = jnp.where(leading, 1.0, jnp.where(inside, panel, 0.0))
        vs.append(split(v))
        ts.append(split(v.T))
        vh_ref[g] = vs[g][0]
        vl_ref[g] = vs[g][1]
    for g in slots:
        gram = dot3(ts[g], vs[g])
        diagonal = jnp.sum(jnp.where(r == c, gram, 0.0), axis=0, keepdims=True)
        factors.append(gram)
        inverses.append(jnp.where(r == c, 2.0 / diagonal, 0.0))

    def level(n, inverses):
        coupling = ((r >> n) != (c >> n)) & ((r >> (n + 1)) == (c >> (n + 1))) & (r < c)
        inverse_parts = [split(inverse) for inverse in inverses]
        middles = [
            split(dot3(split(jnp.where(coupling, factors[g], 0.0)), inverse_parts[g]))
            for g in slots
        ]
        return tuple(inverses[g] - dot3(inverse_parts[g], middles[g]) for g in slots)

    inverses = lax.fori_loop(0, (band - 1).bit_length(), level, tuple(inverses))
    for g in slots:
        high, low = split(dot3(split(inverses[g]), ts[g]))
        yh_ref[g] = high
        yl_ref[g] = low


def factor(first, slots, diagonal, col, pieces):
    count = len(pieces)
    _, _, height, band = pieces[0].shape
    depth = count * height
    group = GROUP if slots % GROUP == 0 else 1
    start = first // group
    kind = jnp.bfloat16
    return pl.pallas_call(
        functools.partial(factor_kernel, count),
        grid_spec=pltpu.PrefetchScalarGridSpec(
            num_scalar_prefetch=1,
            grid=(slots // group,),
            in_specs=[
                pl.BlockSpec((1, group, height, band), lambda k, c: (diagonal, k + start, 0, 0))
            ] * count,
            out_specs=[pl.BlockSpec((group, depth, band), lambda k, c: (k, 0, 0))] * 2
            + [pl.BlockSpec((group, band, depth), lambda k, c: (k, 0, 0))] * 2,
        ),
        out_shape=[jax.ShapeDtypeStruct((slots, depth, band), kind)] * 2
        + [jax.ShapeDtypeStruct((slots, band, depth), kind)] * 2,
        name="factor",
    )(col, *pieces)


def apply_kernel(diagonal, first, own, counts, tile, below, vh, vl, yh, yl, tile_out, below_out):
    k = pl.program_id(0) + first
    band = tile.shape[1]
    upper, lower = tile[0], below[0]
    stacked = jnp.concatenate([upper, lower], axis=0)
    solved = dot3((yh[0], yl[0]), split(stacked))
    change = dot3((vh[0], vl[0]), split(solved))
    active = k < counts[0, diagonal]
    tile_out[0] = jnp.where(active, upper - change[:band], upper)
    below_out[0] = jnp.where(active, lower - change[band:], lower)


def apply(first, diagonal, own, counts, tiles, beneath, vh, vl, yh, yl):
    _, band, columns = tiles.shape
    depth = vh.shape[1]
    at_slot = lambda k, own, counts: (k, 0, 0)
    at_own = lambda k, own, counts: (own[diagonal, k + first], 0, 0)
    return pl.pallas_call(
        functools.partial(apply_kernel, diagonal, first),
        grid_spec=pltpu.PrefetchScalarGridSpec(
            num_scalar_prefetch=2,
            grid=(beneath.shape[0],),
            in_specs=[
                pl.BlockSpec((1, band, columns), at_own),
                pl.BlockSpec((1, band, columns), at_slot),
                pl.BlockSpec((1, depth, band), at_slot),
                pl.BlockSpec((1, depth, band), at_slot),
                pl.BlockSpec((1, band, depth), at_slot),
                pl.BlockSpec((1, band, depth), at_slot),
            ],
            out_specs=[
                pl.BlockSpec((1, band, columns), at_own),
                pl.BlockSpec((1, band, columns), at_slot),
            ],
        ),
        out_shape=[
            jax.ShapeDtypeStruct(tiles.shape, tiles.dtype),
            jax.ShapeDtypeStruct(beneath.shape, beneath.dtype),
        ],
        input_output_aliases={2: 0},
        name="apply",
    )(own, counts, tiles, beneath, vh, vl, yh, yl)


def lift(sent, to_above):
    beneath = []
    for chunk in sent:
        beneath.append(lax.ppermute(chunk, "row", to_above))
    return beneath


def steps(slots, own, behind, counts, tiles, panels):
    row_count = lax.axis_size("row")
    col_count = lax.axis_size("col")
    col = lax.axis_index("col").astype(jnp.int32)[None]
    diagonals = panels.shape[0]
    to_above = [(i, (i - 1) % row_count) for i in range(row_count)]
    to_below = [(i, (i + 1) % row_count) for i in range(row_count)]
    picked, *sent = gather(slots, own, behind, panels, tiles)
    beneath = lift(sent, to_above)
    pieces = {0: picked}
    stride = col_count // 2
    while stride >= 1:
        swap = [(i, i ^ stride) for i in range(col_count)]
        pieces.update(
            {q ^ stride: lax.ppermute(p, "col", swap) for q, p in pieces.items()}
        )
        stride //= 2
    pieces = [pieces[q] for q in range(col_count)]
    for diagonal in range(diagonals):
        returned = []
        for first, chunk in zip(bounds(slots), beneath):
            factors = factor(first, chunk.shape[0], diagonal, col, pieces)
            tiles, lower = apply(first, diagonal, own, counts, tiles, chunk, *factors)
            returned.append(lax.ppermute(lower, "row", to_below))
        more = diagonal + 1 < diagonals
        tiles, *sent = scatter(slots, diagonal, more, behind, counts, tiles, returned)
        if more:
            beneath = lift(sent, to_above)
    return tiles


def plan_kernel(profiles, flags, table, choice, everyone, mine, held, send, recv):
    count, _, lanes = held.shape
    diagonals, depth = flags.shape
    me = lax.axis_index("row")
    mine[...] = jnp.full(mine.shape, -1, mine.dtype)
    mine[0:diagonals, 0:depth] = flags[...]
    barrier = pltpu.get_barrier_semaphore()
    mesh_id = pl.DeviceIdType.MESH
    others = [lax.rem(me + by, count) for by in range(1, count)]
    for other in others:
        pl.semaphore_signal(
            barrier, inc=1, device_id={"row": other}, device_id_type=mesh_id
        )
    pl.semaphore_wait(barrier, count - 1)
    copies = [
        pltpu.make_async_remote_copy(
            src_ref=mine,
            dst_ref=held.at[me],
            send_sem=send.at[i],
            recv_sem=recv.at[i],
            device_id={"row": other},
            device_id_type=mesh_id,
        )
        for i, other in enumerate(others)
    ]
    for copy in copies:
        copy.start()
    held[me] = mine[...]
    for copy in copies:
        copy.wait()
    everyone[...] = held[...]

    f32 = jnp.float32
    row = lax.broadcasted_iota(jnp.int32, (count, lanes), 0)
    on = [jnp.where(held[:, d, :] >= 0, 1.0, 0.0) for d in range(2)]
    after = []
    for x in on:
        under = pltpu.roll(x, count - 1, axis=0)
        after.append(jnp.where(row == count - 1, pltpu.roll(under, lanes - 1, axis=1), under))
    again = on[0] * on[1]
    first, second = on[0] - again, on[1] - again
    kinds = [
        first * after[1],
        first - first * after[1],
        again,
        second - second * after[0],
        second * after[0],
    ]
    sums = [jnp.sum(x, axis=1, keepdims=True) for x in kinds]
    must, may, rep, ready, unready = sums
    chosen = [jnp.zeros((1, 1), f32) for _ in range(4)]
    index, missed = jnp.zeros((1, 1), f32), jnp.ones((1, 1), f32)
    for early, soon, late, last in profiles:
        bad = (must + may + rep > early) | (must > soon)
        bad |= rep + ready + unready + jnp.maximum(must + may - soon, 0.0) > last
        bad |= unready + jnp.maximum(ready - (early - must - may - rep), 0.0) > late
        still = missed * jnp.max(jnp.where(bad, 1.0, 0.0), axis=0, keepdims=True)
        for i, size in enumerate((early, soon, late, last)):
            chosen[i] = chosen[i] + (missed - still) * size
        index, missed = index + still, still
    choice[0] = index[0, 0].astype(jnp.int32)
    early, soon, late, last = chosen

    above = lax.rem(me + count - 1, count)
    picked = [
        jnp.sum(jnp.where(row == who, x, 0.0), axis=0, keepdims=True)
        for who in (me, above)
        for x in kinds
    ]
    none = jnp.zeros((1, lanes), f32)
    stacked = jnp.concatenate(picked + [none] * 6, axis=0)
    r = lax.broadcasted_iota(jnp.int32, (lanes, lanes), 0)
    c = lax.broadcasted_iota(jnp.int32, (lanes, lanes), 1)
    ahead = jnp.dot(
        stacked.astype(jnp.bfloat16),
        jnp.where(r < c, 1.0, 0.0).astype(jnp.bfloat16),
        preferred_element_type=f32,
    )
    totals = jnp.sum(stacked, axis=1, keepdims=True)

    def places(which):
        at = [stacked[5 * which + i : 5 * which + i + 1] > 0.5 for i in range(5)]
        rank = [ahead[5 * which + i : 5 * which + i + 1] for i in range(5)]
        must, may, rep, ready, unready = [
            totals[5 * which + i : 5 * which + i + 1] for i in range(5)
        ]
        slot0 = jnp.where(
            at[0],
            rank[0],
            jnp.where(at[1], must + rank[1], jnp.where(at[2], must + may + rank[2], -1.0)),
        )
        taken = must + may + rep
        spare = early - taken
        over = jnp.maximum(ready - spare, 0.0)
        tardy = over + unready
        prompt = rep + ready - over

        def placed(p):
            return jnp.where(p < last - late, p, p + tardy)

        fast = at[3] & (rank[3] < spare)
        lag = jnp.where(
            at[4], over + rank[4], jnp.where(at[3] & ~fast, rank[3] - spare, -1.0)
        )
        slot1 = jnp.where(
            at[2],
            placed(rank[2]),
            jnp.where(fast, placed(rep + rank[3]), jnp.where(lag >= 0, last - late + lag, -1.0)),
        )
        single = at[0] | at[1]
        held_back = single & (slot0 >= soon)
        kept = jnp.where(held_back, placed(prompt + slot0 - soon), -1.0)
        sooner = jnp.where(single & (slot0 < soon), slot0, -1.0)
        ahead_of = jnp.where(fast, taken + rank[3], -1.0)
        return at, slot0, slot1, kept, sooner, ahead_of, lag

    at, slot0, slot1, kept, _, ahead_of, _ = places(0)
    _, up0, up1, up_kept, up_sooner, up_ahead, up_lag = places(1)
    keys = [
        slot0,
        slot1,
        kept,
        jnp.maximum(up0, up_ahead),
        up_lag,
        jnp.where(at[2], slot0, -1.0),
        ahead_of,
        none,
    ]
    filler = jnp.zeros((lanes - len(keys), lanes), f32)
    turned = jnp.concatenate(keys + [filler], axis=0).T
    column = lambda i: turned[:, i : i + 1]
    tile = r.astype(f32)
    place = c.astype(f32)

    def turn(key, value, missing):
        hit = jnp.where(column(key) == place, value - missing, 0.0)
        return jnp.sum(hit, axis=0, keepdims=True) + missing

    top = me == 0

    def behind(key):
        found = turn(key, tile, 0.0)
        return jnp.where(top, jnp.minimum(found + 1.0, depth - 1.0), found)

    def below(x):
        return jnp.where(top, pltpu.roll(x, 1, axis=1), x)

    rows = [
        turn(0, tile, 0.0),
        turn(1, tile, 0.0),
        behind(3),
        behind(4),
        slot0,
        slot1,
        below(up_sooner),
        below(jnp.maximum(up1, up_kept)),
        turn(1, column(5), -1.0),
        turn(1, column(6), -1.0),
        turn(2, column(0), -1.0),
    ]
    rows += [none] * (table.shape[0] - len(rows))
    table[...] = jnp.concatenate(rows, axis=0).astype(jnp.int32)


def plan(profiles, flags):
    count = lax.axis_size("row")
    lanes = 128
    vmem_spec = pl.BlockSpec(memory_space=pltpu.VMEM)
    shape = (count, 8, lanes)
    kind = flags.dtype
    return pl.pallas_call(
        functools.partial(plan_kernel, profiles),
        out_shape=[
            jax.ShapeDtypeStruct((16, lanes), kind),
            jax.ShapeDtypeStruct((1,), kind),
            jax.ShapeDtypeStruct(shape, kind),
        ],
        in_specs=[vmem_spec],
        out_specs=[vmem_spec, pl.BlockSpec(memory_space=pltpu.SMEM), vmem_spec],
        scratch_shapes=[
            pltpu.VMEM(shape[1:], kind),
            pltpu.VMEM(shape, kind),
            pltpu.SemaphoreType.DMA((count - 1,)),
            pltpu.SemaphoreType.DMA((count - 1,)),
        ],
        compiler_params=pltpu.CompilerParams(collective_id=0, has_side_effects=True),
        name="plan",
    )(flags)


def fresh_kernel(x, out):
    out[...] = x[...]


def fresh(x):
    spec = pl.BlockSpec((1,) + x.shape[1:], lambda k: (k, 0, 0))
    return pl.pallas_call(
        fresh_kernel,
        grid=(x.shape[0],),
        in_specs=[spec],
        out_specs=spec,
        out_shape=jax.ShapeDtypeStruct(x.shape, x.dtype),
        name="fresh",
    )(x)


def ordering(active):
    depth = active.shape[-1]
    here = jnp.arange(depth, dtype=jnp.int32)
    on = active.astype(jnp.int32)
    earlier = here[None, :] < here[:, None]
    before = jnp.sum(jnp.where(earlier, on[..., None, :], 0), axis=-1)
    total = jnp.sum(on, axis=-1)
    rank = jnp.where(active, before, total[..., None] + here - before)
    order = jnp.sum(
        jnp.where(rank[..., None, :] == here[:, None], here, 0), axis=-1
    ).astype(jnp.int32)
    return order, total.astype(jnp.int32)


def flipped(index, stride):
    return index + stride - 2 * stride * lax.rem(lax.div(index, stride), 2)


def invert_and_store(panels, first, count, vh_ref, vl_ref, yh_ref, yl_ref):
    depth, band = panels.shape[1:]
    row = lax.broadcasted_iota(jnp.int32, (depth, band), 0)
    col = lax.broadcasted_iota(jnp.int32, (depth, band), 1)
    inside = (row >= col + 1) & (row <= col + band)
    leading = row == col + 1
    r = lax.broadcasted_iota(jnp.int32, (band, band), 0)
    c = lax.broadcasted_iota(jnp.int32, (band, band), 1)
    slots = range(count)
    ts, factors, inverses = [], [], []
    for g in slots:
        v = jnp.where(leading, 1.0, jnp.where(inside, panels[first + g], 0.0))
        vs = split(v)
        ts.append(split(v.T))
        vh_ref[first + g] = vs[0]
        vl_ref[first + g] = vs[1]
        gram = dot3(ts[g], vs)
        diagonal = jnp.sum(jnp.where(r == c, gram, 0.0), axis=0, keepdims=True)
        factors.append(gram)
        inverses.append(jnp.where(r == c, 2.0 / diagonal, 0.0))

    def level(n, inverses):
        coupling = ((r >> n) != (c >> n)) & ((r >> (n + 1)) == (c >> (n + 1))) & (r < c)
        inverse_parts = [split(inverse) for inverse in inverses]
        middles = [
            split(dot3(split(jnp.where(coupling, factors[g], 0.0)), inverse_parts[g]))
            for g in slots
        ]
        return tuple(inverses[g] - dot3(inverse_parts[g], middles[g]) for g in slots)

    inverses = lax.fori_loop(0, (band - 1).bit_length(), level, tuple(inverses))
    for g in slots:
        high, low = split(dot3(split(inverses[g]), ts[g]))
        yh_ref[first + g] = high
        yl_ref[first + g] = low


def whole_kernel(
    profile, group, table, tiles_in, panels_in, merged, last_back,
    tiles, pieces, panel, vh, vl, yh, yl, lift_out, lift_in, upper_new, lower_new, first_back,
    in_sems, panel_sems, lift_sems, back_sems,
):
    early, soon, late, last = profile
    slots, lifts, backs = (early, last), (early, late), (soon, last)
    skip = (0, last - late)
    back_in = (first_back, last_back)
    depth = tiles.shape[0]
    height = pieces.shape[2]
    rows = lax.axis_size("row")
    cols = lax.axis_size("col")
    me_row = lax.axis_index("row")
    me_col = lax.axis_index("col")
    above = lax.rem(me_row + rows - 1, rows)
    below = lax.rem(me_row + 1, rows)
    mesh_id = pl.DeviceIdType.MESH
    strides = []
    stride = cols // 2
    while stride >= 1:
        strides.append(stride)
        stride //= 2
    own = lambda d, k: table[d, k]
    behind = lambda d, k: table[2 + d, k]
    upper_slot = lambda d, j: table[4 + d, j]
    lower_slot = lambda d, j: table[6 + d, j]

    def either(source, index, other):
        return jnp.where(index >= 0, source[jnp.maximum(index, 0)], other)


    panels_copy = pltpu.make_async_copy(panels_in, pieces, in_sems.at[0])
    tiles_copy = pltpu.make_async_copy(tiles_in, tiles, in_sems.at[1])
    panels_copy.start()
    tiles_copy.start()

    barrier = pltpu.get_barrier_semaphore()
    peers = [{"row": above}, {"row": below}]
    peers += [{"col": flipped(me_col, s)} for s in strides]
    for peer in peers:
        pl.semaphore_signal(barrier, inc=1, device_id=peer, device_id_type=mesh_id)
    pl.semaphore_wait(barrier, len(peers))

    def exchange(d, g, stage):
        held = [me_col]
        for s in strides[:stage]:
            held += [flipped(h, s) for h in held]
        base = sum(2**i for i in range(stage))
        copies = []
        for i, h in enumerate(held):
            where = (pl.ds(g * group, group), pl.ds(pl.multiple_of(h * height, height), height))
            copies.append(
                pltpu.make_async_remote_copy(
                    src_ref=panel[d].at[where],
                    dst_ref=panel[d].at[where],
                    send_sem=panel_sems[d].at[0, g, base + i],
                    recv_sem=panel_sems[d].at[1, g, base + i],
                    device_id={"col": flipped(me_col, strides[stage])},
                    device_id_type=mesh_id,
                )
            )
        return copies

    def lift(d, k):
        return pltpu.make_async_remote_copy(
            src_ref=lift_out[d].at[k],
            dst_ref=lift_in[d].at[skip[d] + k],
            send_sem=lift_sems[d].at[0, k],
            recv_sem=lift_sems[d].at[1, k],
            device_id={"row": above},
            device_id_type=mesh_id,
        )

    def give_back(d, k):
        return pltpu.make_async_remote_copy(
            src_ref=lower_new[d].at[k],
            dst_ref=back_in[d].at[k],
            send_sem=back_sems[d].at[0, k],
            recv_sem=back_sems[d].at[1, k],
            device_id={"row": below},
            device_id_type=mesh_id,
        )

    def pick_panels(d):
        mine = pl.ds(pl.multiple_of(me_col * height, height), height)

        def one(g, _):
            for i in range(group):
                panel[d][g * group + i, mine] = pieces[d, own(d, g * group + i)]
            if strides:
                for copy in exchange(d, g, 0):
                    copy.start()
            return 0

        lax.fori_loop(0, panel[d].shape[0] // group, one, 0)

    def forward(d, g):
        for stage in range(1, len(strides)):
            for copy in exchange(d, g, stage - 1):
                copy.wait_recv()
            for copy in exchange(d, g, stage):
                copy.start()

    def factor(d):
        count = panel[d].shape[0] // group

        def one(g, _):
            if strides:
                for copy in exchange(d, g, len(strides) - 1):
                    copy.wait_recv()

            @pl.when(g + 1 < count)
            def _():
                forward(d, g + 1)

            invert_and_store(panel[d], g * group, group, vh[d], vl[d], yh[d], yl[d])
            return 0

        forward(d, 0)
        lax.fori_loop(0, count, one, 0)

    def after_first(j):
        kept = either(back_in[0], lower_slot(0, j), tiles[j])
        return either(upper_new[0], upper_slot(0, j), kept)

    def send_lifts(d, value):
        def one(k, _):
            lift_out[d][k] = value(behind(d, k))

            @pl.when(k > 0)
            def _():
                lift(d, k - 1).start()

            return 0

        lax.fori_loop(0, lifts[d], one, 0)
        lift(d, lifts[d] - 1).start()

    def reflect(d, upper_of, lower_of, sent_of):
        def one(k, _):
            @pl.when(k >= skip[d])
            def _():
                lift(d, k - skip[d]).wait_recv()

            upper, lower = upper_of(k), lower_of(k)
            band = upper.shape[0]
            stacked = split(jnp.concatenate([upper, lower], axis=0))
            solved = split(dot3((yh[d][k], yl[d][k]), stacked))
            change = dot3((vh[d][k], vl[d][k]), solved)
            lower_new[d][k] = sent_of(k, lower - change[band:])
            upper_new[d][k] = upper - change[:band]

            @pl.when(k < backs[d])
            def _():
                give_back(d, k).start()

            return 0

        lax.fori_loop(0, slots[d], one, 0)

    def receive(d):
        def one(k, _):
            give_back(d, k).wait_recv()
            return 0

        lax.fori_loop(0, backs[d], one, 0)

    panels_copy.wait()
    pick_panels(0)
    tiles_copy.wait()
    send_lifts(0, lambda j: tiles[j])
    pick_panels(1)
    factor(0)
    reflect(0, lambda k: tiles[own(0, k)], lambda k: lift_in[0][k], lambda k, lower: lower)
    send_lifts(1, lambda j: either(upper_new[0], upper_slot(0, j), tiles[j]))
    factor(1)
    receive(0)

    def second_lower(k):
        arrived = either(lift_in[0], table[9, k], lift_in[1][k])
        return either(lower_new[0], table[8, k], arrived)

    reflect(
        1,
        lambda k: after_first(own(1, k)),
        second_lower,
        lambda k, lower: either(lower_new[0], table[10, k], lower),
    )

    def merge(j, _):
        merged[j] = either(upper_new[1], upper_slot(1, j), after_first(j))
        return 0

    lax.fori_loop(0, depth, merge, 0)
    receive(1)
    for d in range(2):
        for g in range(panel[d].shape[0] // group):
            for stage in range(len(strides)):
                for copy in exchange(d, g, stage):
                    copy.wait_send()

        def sent(k, _):
            lift(d, k).wait_send()
            return 0

        def returned(k, _):
            give_back(d, k).wait_send()
            return 0

        lax.fori_loop(0, lifts[d], sent, 0)
        lax.fori_loop(0, backs[d], returned, 0)


def settle_kernel(table, merged, back, out, sems):
    depth = merged.shape[0]

    def one(j, _):
        slot = table[7, j]

        @pl.when(slot >= 0)
        def _():
            pltpu.make_async_copy(back.at[jnp.maximum(slot, 0)], out.at[j], sems.at[j]).start()

        @pl.when(slot < 0)
        def _():
            pltpu.make_async_copy(merged.at[j], out.at[j], sems.at[j]).start()

        return 0

    def drain(j, _):
        pltpu.make_async_copy(merged.at[j], out.at[j], sems.at[j]).wait()
        return 0

    lax.fori_loop(0, depth, one, 0)
    lax.fori_loop(0, depth, drain, 0)


def settle(table, merged, back):
    vmem_spec = pl.BlockSpec(memory_space=pltpu.VMEM)
    return pl.pallas_call(
        settle_kernel,
        in_specs=[pl.BlockSpec(memory_space=pltpu.SMEM), vmem_spec, vmem_spec],
        out_specs=pl.BlockSpec(memory_space=pl.ANY),
        out_shape=jax.ShapeDtypeStruct(merged.shape, merged.dtype),
        scratch_shapes=[pltpu.SemaphoreType.DMA((merged.shape[0],))],
        compiler_params=pltpu.CompilerParams(vmem_limit_bytes=8 * 2**20),
        name="settle",
    )(table, merged, back)


def whole(profile, index, table, tiles, panels):
    depth, band, columns = tiles.shape
    _, _, height, _ = panels.shape
    cols = lax.axis_size("col")
    long = height * cols
    early, soon, late, last = profile
    group = GROUPED
    padded = [-(-n // group) * group for n in (early, last)]
    f32, bf16 = jnp.float32, jnp.bfloat16
    tile_slots = lambda counts: [pltpu.VMEM((n, band, columns), f32) for n in counts]
    dma = pltpu.SemaphoreType.DMA
    scratch = [
        pltpu.VMEM(tiles.shape, f32),
        pltpu.VMEM(panels.shape, f32),
        [pltpu.VMEM((n, long, band), f32) for n in padded],
        [pltpu.VMEM((n, long, band), bf16) for n in padded],
        [pltpu.VMEM((n, long, band), bf16) for n in padded],
        [pltpu.VMEM((n, band, long), bf16) for n in padded],
        [pltpu.VMEM((n, band, long), bf16) for n in padded],
        tile_slots((early, late)),
        tile_slots((early, last)),
        tile_slots((early, last)),
        tile_slots((early, last)),
        pltpu.VMEM((soon, band, columns), f32),
        dma((2,)),
        [dma((2, n // group, max(cols - 1, 1))) for n in padded],
        [dma((2, n)) for n in (early, late)],
        [dma((2, n)) for n in (soon, last)],
    ]
    tile_bytes = band * columns * 4
    held = 2 * depth + soon + late + 3 * early + 4 * last
    factors = sum(padded) * long * band * 12
    limit = held * tile_bytes + panels.size * 4 + factors + 4 * 2**20
    any_spec = pl.BlockSpec(memory_space=pl.ANY)
    vmem_spec = pl.BlockSpec(memory_space=pltpu.VMEM)
    merged, back = pl.pallas_call(
        functools.partial(whole_kernel, profile, group),
        in_specs=[pl.BlockSpec(memory_space=pltpu.SMEM), any_spec, any_spec],
        out_specs=[vmem_spec] * 2,
        out_shape=[
            jax.ShapeDtypeStruct(tiles.shape, f32),
            jax.ShapeDtypeStruct((last, band, columns), f32),
        ],
        scratch_shapes=scratch,
        compiler_params=pltpu.CompilerParams(
            collective_id=1 + index, has_side_effects=True, vmem_limit_bytes=limit
        ),
    )(table, tiles, panels)
    return settle(table, merged, back)


def local(eigvec, reflectors, sweep_group):
    row_index = lax.axis_index("row")
    row_count = lax.axis_size("row")
    depth = eigvec.shape[0]
    profiles = [p for p in PROFILES if max(p) <= depth]
    small = depth <= max(PROFILES[-1])
    if small and (depth,) * 4 not in profiles:
        profiles.append((depth,) * 4)
    table, choice, flags = plan(profiles, sweep_group[:, :, 0])

    def general(table, flags, tiles, panels):
        active = flags[:, : sweep_group.shape[0], :depth] >= 0
        mine = lax.dynamic_index_in_dim(active, row_index, 0, keepdims=False)
        above = lax.dynamic_index_in_dim(
            active, (row_index + row_count - 1) % row_count, 0, keepdims=False
        )
        order, counts = ordering(jnp.stack([mine, above]))
        own = order[0]
        behind = jnp.where(row_index == 0, (order[1] + 1) % depth, order[1])
        return steps(depth, own, behind, counts, fresh(tiles), panels)

    def branch(index, profile):
        return lambda table, flags, tiles, panels: whole(profile, index, table, tiles, panels)

    branches = [branch(i, p) for i, p in enumerate(profiles)]
    if not small:
        branches.append(general)
    args = (table, flags, eigvec[:, 0], reflectors[:, :, 0])
    out = lax.switch(choice[0], branches, *args) if len(branches) > 1 else branches[0](*args)
    return out[:, None]


def solution(mesh):
    return jax.shard_map(
        local,
        mesh=mesh,
        in_specs=(
            P(None, "row", None, "col"),
            P(None, None, "row", "col", None),
            P(None, None, "row"),
        ),
        out_specs=P(None, "row", None, "col"),
        check_vma=False,
    )
```

```python
import functools

import jax
import jax.numpy as jnp
from jax import lax
from jax.experimental import pallas as pl
from jax.experimental.pallas import tpu as pltpu
from jax.sharding import PartitionSpec as P


GROUP = 2
CHUNKS = 2
PROFILES = (
    (12, 4, 4, 12), (12, 5, 5, 12), (13, 5, 5, 13), (13, 5, 6, 14),
    (15, 6, 6, 15), (16, 7, 7, 16), (20, 12, 12, 20),
)
GROUPED = 8


def split(x):
    high = x.astype(jnp.bfloat16)
    return high, (x - high.astype(jnp.float32)).astype(jnp.bfloat16)


def dot(a, b):
    return jnp.dot(a, b, preferred_element_type=jnp.float32)


def dot3(a, b):
    return dot(a[1], b[0]) + dot(a[0], b[1]) + dot(a[0], b[0])


def bounds(slots):
    inner = [slots * i // CHUNKS // GROUP * GROUP for i in range(CHUNKS)]
    return inner + [slots]


def chunk_shapes(slots, tiles):
    edges = bounds(slots)
    return [
        jax.ShapeDtypeStruct((high - low,) + tiles.shape[1:], tiles.dtype)
        for low, high in zip(edges[:-1], edges[1:])
    ]


def slot_of(chunks, k):
    for chunk in chunks:
        if k < chunk.shape[0]:
            return chunk.at[k]
        k -= chunk.shape[0]


def gather_kernel(slots, own, behind, panels, tiles, picked, *rest):
    diagonals = panels.shape[0]
    sent, sems = rest[:-1], rest[-1]

    def panel_copy(d, k):
        return pltpu.make_async_copy(
            panels.at[d, own[d, k]], picked.at[d, k], sems.at[d * slots + k]
        )

    def tile_copy(k):
        return pltpu.make_async_copy(
            tiles.at[behind[0, k]], slot_of(sent, k), sems.at[diagonals * slots + k]
        )

    for k in range(slots):
        tile_copy(k).start()
    for d in range(diagonals):
        for k in range(slots):
            panel_copy(d, k).start()
    for k in range(slots):
        tile_copy(k).wait()
    for d in range(diagonals):
        for k in range(slots):
            panel_copy(d, k).wait()


def gather(slots, own, behind, panels, tiles):
    diagonals = panels.shape[0]
    any_spec = pl.BlockSpec(memory_space=pl.ANY)
    return pl.pallas_call(
        functools.partial(gather_kernel, slots),
        grid_spec=pltpu.PrefetchScalarGridSpec(
            num_scalar_prefetch=2,
            grid=(1,),
            in_specs=[any_spec, any_spec],
            out_specs=[pl.BlockSpec(memory_space=pltpu.VMEM)] * (1 + CHUNKS),
            scratch_shapes=[pltpu.SemaphoreType.DMA(((diagonals + 1) * slots,))],
        ),
        out_shape=[
            jax.ShapeDtypeStruct((diagonals, slots) + panels.shape[2:], panels.dtype),
        ] + chunk_shapes(slots, tiles),
        name="gather",
    )(own, behind, panels, tiles)


def scatter_kernel(slots, diagonal, more, behind, counts, tiles, *rest):
    returned, out, sent, sems = rest[:CHUNKS], rest[CHUNKS], rest[CHUNKS + 1:-1], rest[-1]

    def put(k):
        return pltpu.make_async_copy(
            slot_of(returned, k), out.at[behind[diagonal, k]], sems.at[k]
        )

    for k in range(slots):
        @pl.when(k < counts[1, diagonal])
        def _():
            put(k).start()
    for k in range(slots):
        @pl.when(k < counts[1, diagonal])
        def _():
            put(k).wait()
    if more:

        def take(k):
            return pltpu.make_async_copy(
                out.at[behind[diagonal + 1, k]], slot_of(sent, k), sems.at[slots + k]
            )

        for k in range(slots):
            take(k).start()
        for k in range(slots):
            take(k).wait()


def scatter(slots, diagonal, more, behind, counts, tiles, returned):
    any_spec = pl.BlockSpec(memory_space=pl.ANY)
    vmem_spec = pl.BlockSpec(memory_space=pltpu.VMEM)
    shapes = [jax.ShapeDtypeStruct(tiles.shape, tiles.dtype)]
    if more:
        shapes += chunk_shapes(slots, tiles)
    return pl.pallas_call(
        functools.partial(scatter_kernel, slots, diagonal, more),
        grid_spec=pltpu.PrefetchScalarGridSpec(
            num_scalar_prefetch=2,
            grid=(1,),
            in_specs=[any_spec] + [vmem_spec] * CHUNKS,
            out_specs=[any_spec] + [vmem_spec] * (len(shapes) - 1),
            scratch_shapes=[pltpu.SemaphoreType.DMA((2 * slots,))],
        ),
        out_shape=shapes,
        input_output_aliases={2: 0},
        name="scatter",
    )(behind, counts, tiles, *returned)


def factor_kernel(pieces_count, col_ref, *refs):
    pieces = refs[:pieces_count]
    vh_ref, vl_ref, yh_ref, yl_ref = refs[pieces_count:]
    me = col_ref[0]
    group = pieces[0].shape[1]
    band = pieces[0].shape[-1]
    depth = pieces_count * pieces[0].shape[2]
    row = lax.broadcasted_iota(jnp.int32, (depth, band), 0)
    col = lax.broadcasted_iota(jnp.int32, (depth, band), 1)
    inside = (row >= col + 1) & (row <= col + band)
    leading = row == col + 1
    r = lax.broadcasted_iota(jnp.int32, (band, band), 0)
    c = lax.broadcasted_iota(jnp.int32, (band, band), 1)
    slots = range(group)
    vs, ts, factors, inverses = [], [], [], []
    for g in slots:
        parts = [piece[0, g] for piece in pieces]
        stride = 1
        while stride < pieces_count:
            odd = (me // stride) % 2 == 1
            parts = [
                jnp.where(odd, parts[j ^ stride], parts[j]) for j in range(pieces_count)
            ]
            stride *= 2
        panel = jnp.concatenate(parts, axis=0)
        v = jnp.where(leading, 1.0, jnp.where(inside, panel, 0.0))
        vs.append(split(v))
        ts.append(split(v.T))
        vh_ref[g] = vs[g][0]
        vl_ref[g] = vs[g][1]
    for g in slots:
        gram = dot3(ts[g], vs[g])
        diagonal = jnp.sum(jnp.where(r == c, gram, 0.0), axis=0, keepdims=True)
        factors.append(gram)
        inverses.append(jnp.where(r == c, 2.0 / diagonal, 0.0))

    def level(n, inverses):
        coupling = ((r >> n) != (c >> n)) & ((r >> (n + 1)) == (c >> (n + 1))) & (r < c)
        inverse_parts = [split(inverse) for inverse in inverses]
        middles = [
            split(dot3(split(jnp.where(coupling, factors[g], 0.0)), inverse_parts[g]))
            for g in slots
        ]
        return tuple(inverses[g] - dot3(inverse_parts[g], middles[g]) for g in slots)

    inverses = lax.fori_loop(0, (band - 1).bit_length(), level, tuple(inverses))
    for g in slots:
        high, low = split(dot3(split(inverses[g]), ts[g]))
        yh_ref[g] = high
        yl_ref[g] = low


def factor(first, slots, diagonal, col, pieces):
    count = len(pieces)
    _, _, height, band = pieces[0].shape
    depth = count * height
    group = GROUP if slots % GROUP == 0 else 1
    start = first // group
    kind = jnp.bfloat16
    return pl.pallas_call(
        functools.partial(factor_kernel, count),
        grid_spec=pltpu.PrefetchScalarGridSpec(
            num_scalar_prefetch=1,
            grid=(slots // group,),
            in_specs=[
                pl.BlockSpec((1, group, height, band), lambda k, c: (diagonal, k + start, 0, 0))
            ] * count,
            out_specs=[pl.BlockSpec((group, depth, band), lambda k, c: (k, 0, 0))] * 2
            + [pl.BlockSpec((group, band, depth), lambda k, c: (k, 0, 0))] * 2,
        ),
        out_shape=[jax.ShapeDtypeStruct((slots, depth, band), kind)] * 2
        + [jax.ShapeDtypeStruct((slots, band, depth), kind)] * 2,
        name="factor",
    )(col, *pieces)


def apply_kernel(diagonal, first, own, counts, tile, below, vh, vl, yh, yl, tile_out, below_out):
    k = pl.program_id(0) + first
    band = tile.shape[1]
    upper, lower = tile[0], below[0]
    stacked = jnp.concatenate([upper, lower], axis=0)
    solved = dot3((yh[0], yl[0]), split(stacked))
    change = dot3((vh[0], vl[0]), split(solved))
    active = k < counts[0, diagonal]
    tile_out[0] = jnp.where(active, upper - change[:band], upper)
    below_out[0] = jnp.where(active, lower - change[band:], lower)


def apply(first, diagonal, own, counts, tiles, beneath, vh, vl, yh, yl):
    _, band, columns = tiles.shape
    depth = vh.shape[1]
    at_slot = lambda k, own, counts: (k, 0, 0)
    at_own = lambda k, own, counts: (own[diagonal, k + first], 0, 0)
    return pl.pallas_call(
        functools.partial(apply_kernel, diagonal, first),
        grid_spec=pltpu.PrefetchScalarGridSpec(
            num_scalar_prefetch=2,
            grid=(beneath.shape[0],),
            in_specs=[
                pl.BlockSpec((1, band, columns), at_own),
                pl.BlockSpec((1, band, columns), at_slot),
                pl.BlockSpec((1, depth, band), at_slot),
                pl.BlockSpec((1, depth, band), at_slot),
                pl.BlockSpec((1, band, depth), at_slot),
                pl.BlockSpec((1, band, depth), at_slot),
            ],
            out_specs=[
                pl.BlockSpec((1, band, columns), at_own),
                pl.BlockSpec((1, band, columns), at_slot),
            ],
        ),
        out_shape=[
            jax.ShapeDtypeStruct(tiles.shape, tiles.dtype),
            jax.ShapeDtypeStruct(beneath.shape, beneath.dtype),
        ],
        input_output_aliases={2: 0},
        name="apply",
    )(own, counts, tiles, beneath, vh, vl, yh, yl)


def lift(sent, to_above):
    beneath = []
    for chunk in sent:
        beneath.append(lax.ppermute(chunk, "row", to_above))
    return beneath


def steps(slots, own, behind, counts, tiles, panels):
    row_count = lax.axis_size("row")
    col_count = lax.axis_size("col")
    col = lax.axis_index("col").astype(jnp.int32)[None]
    diagonals = panels.shape[0]
    to_above = [(i, (i - 1) % row_count) for i in range(row_count)]
    to_below = [(i, (i + 1) % row_count) for i in range(row_count)]
    picked, *sent = gather(slots, own, behind, panels, tiles)
    beneath = lift(sent, to_above)
    pieces = {0: picked}
    stride = col_count // 2
    while stride >= 1:
        swap = [(i, i ^ stride) for i in range(col_count)]
        pieces.update(
            {q ^ stride: lax.ppermute(p, "col", swap) for q, p in pieces.items()}
        )
        stride //= 2
    pieces = [pieces[q] for q in range(col_count)]
    for diagonal in range(diagonals):
        returned = []
        for first, chunk in zip(bounds(slots), beneath):
            factors = factor(first, chunk.shape[0], diagonal, col, pieces)
            tiles, lower = apply(first, diagonal, own, counts, tiles, chunk, *factors)
            returned.append(lax.ppermute(lower, "row", to_below))
        more = diagonal + 1 < diagonals
        tiles, *sent = scatter(slots, diagonal, more, behind, counts, tiles, returned)
        if more:
            beneath = lift(sent, to_above)
    return tiles


def plan_kernel(profiles, flags, table, choice, everyone, mine, held, send, recv):
    count, _, lanes = held.shape
    diagonals, depth = flags.shape
    me = lax.axis_index("row")
    mine[...] = jnp.full(mine.shape, -1, mine.dtype)
    mine[0:diagonals, 0:depth] = flags[...]
    barrier = pltpu.get_barrier_semaphore()
    mesh_id = pl.DeviceIdType.MESH
    others = [lax.rem(me + by, count) for by in range(1, count)]
    for other in others:
        pl.semaphore_signal(
            barrier, inc=1, device_id={"row": other}, device_id_type=mesh_id
        )
    pl.semaphore_wait(barrier, count - 1)
    copies = [
        pltpu.make_async_remote_copy(
            src_ref=mine,
            dst_ref=held.at[me],
            send_sem=send.at[i],
            recv_sem=recv.at[i],
            device_id={"row": other},
            device_id_type=mesh_id,
        )
        for i, other in enumerate(others)
    ]
    for copy in copies:
        copy.start()
    held[me] = mine[...]
    for copy in copies:
        copy.wait()
    everyone[...] = held[...]

    f32 = jnp.float32
    row = lax.broadcasted_iota(jnp.int32, (count, lanes), 0)
    on = [jnp.where(held[:, d, :] >= 0, 1.0, 0.0) for d in range(2)]
    after = []
    for x in on:
        under = pltpu.roll(x, count - 1, axis=0)
        after.append(jnp.where(row == count - 1, pltpu.roll(under, lanes - 1, axis=1), under))
    again = on[0] * on[1]
    first, second = on[0] - again, on[1] - again
    kinds = [
        first * after[1],
        first - first * after[1],
        again,
        second - second * after[0],
        second * after[0],
    ]
    sums = [jnp.sum(x, axis=1, keepdims=True) for x in kinds]
    must, may, rep, ready, unready = sums
    chosen = [jnp.zeros((1, 1), f32) for _ in range(4)]
    index, missed = jnp.zeros((1, 1), f32), jnp.ones((1, 1), f32)
    for early, soon, late, last in profiles:
        bad = (must + may + rep > early) | (must > soon)
        bad |= rep + ready + unready + jnp.maximum(must + may - soon, 0.0) > last
        bad |= unready + jnp.maximum(ready - (early - must - may - rep), 0.0) > late
        still = missed * jnp.max(jnp.where(bad, 1.0, 0.0), axis=0, keepdims=True)
        for i, size in enumerate((early, soon, late, last)):
            chosen[i] = chosen[i] + (missed - still) * size
        index, missed = index + still, still
    choice[0] = index[0, 0].astype(jnp.int32)
    early, soon, late, last = chosen

    above = lax.rem(me + count - 1, count)
    picked = [
        jnp.sum(jnp.where(row == who, x, 0.0), axis=0, keepdims=True)
        for who in (me, above)
        for x in kinds
    ]
    none = jnp.zeros((1, lanes), f32)
    stacked = jnp.concatenate(picked + [none] * 6, axis=0)
    r = lax.broadcasted_iota(jnp.int32, (lanes, lanes), 0)
    c = lax.broadcasted_iota(jnp.int32, (lanes, lanes), 1)
    ahead = jnp.dot(
        stacked.astype(jnp.bfloat16),
        jnp.where(r < c, 1.0, 0.0).astype(jnp.bfloat16),
        preferred_element_type=f32,
    )
    totals = jnp.sum(stacked, axis=1, keepdims=True)

    def places(which):
        at = [stacked[5 * which + i : 5 * which + i + 1] > 0.5 for i in range(5)]
        rank = [ahead[5 * which + i : 5 * which + i + 1] for i in range(5)]
        must, may, rep, ready, unready = [
            totals[5 * which + i : 5 * which + i + 1] for i in range(5)
        ]
        slot0 = jnp.where(
            at[0],
            rank[0],
            jnp.where(at[1], must + rank[1], jnp.where(at[2], must + may + rank[2], -1.0)),
        )
        taken = must + may + rep
        spare = early - taken
        over = jnp.maximum(ready - spare, 0.0)
        tardy = over + unready
        prompt = rep + ready - over

        def placed(p):
            return jnp.where(p < last - late, p, p + tardy)

        fast = at[3] & (rank[3] < spare)
        lag = jnp.where(
            at[4], over + rank[4], jnp.where(at[3] & ~fast, rank[3] - spare, -1.0)
        )
        slot1 = jnp.where(
            at[2],
            placed(rank[2]),
            jnp.where(fast, placed(rep + rank[3]), jnp.where(lag >= 0, last - late + lag, -1.0)),
        )
        single = at[0] | at[1]
        held_back = single & (slot0 >= soon)
        kept = jnp.where(held_back, placed(prompt + slot0 - soon), -1.0)
        sooner = jnp.where(single & (slot0 < soon), slot0, -1.0)
        ahead_of = jnp.where(fast, taken + rank[3], -1.0)
        return at, slot0, slot1, kept, sooner, ahead_of, lag

    at, slot0, slot1, kept, _, ahead_of, _ = places(0)
    _, up0, up1, up_kept, up_sooner, up_ahead, up_lag = places(1)
    keys = [
        slot0,
        slot1,
        kept,
        jnp.maximum(up0, up_ahead),
        up_lag,
        jnp.where(at[2], slot0, -1.0),
        ahead_of,
        none,
    ]
    filler = jnp.zeros((lanes - len(keys), lanes), f32)
    turned = jnp.concatenate(keys + [filler], axis=0).T
    column = lambda i: turned[:, i : i + 1]
    tile = r.astype(f32)
    place = c.astype(f32)

    def turn(key, value, missing):
        hit = jnp.where(column(key) == place, value - missing, 0.0)
        return jnp.sum(hit, axis=0, keepdims=True) + missing

    top = me == 0

    def behind(key):
        found = turn(key, tile, 0.0)
        return jnp.where(top, jnp.minimum(found + 1.0, depth - 1.0), found)

    def below(x):
        return jnp.where(top, pltpu.roll(x, 1, axis=1), x)

    rows = [
        turn(0, tile, 0.0),
        turn(1, tile, 0.0),
        behind(3),
        behind(4),
        slot0,
        slot1,
        below(up_sooner),
        below(jnp.maximum(up1, up_kept)),
        turn(1, column(5), -1.0),
        turn(1, column(6), -1.0),
        turn(2, column(0), -1.0),
    ]
    rows += [none] * (table.shape[0] - len(rows))
    table[...] = jnp.concatenate(rows, axis=0).astype(jnp.int32)


def plan(profiles, flags):
    count = lax.axis_size("row")
    lanes = 128
    vmem_spec = pl.BlockSpec(memory_space=pltpu.VMEM)
    shape = (count, 8, lanes)
    kind = flags.dtype
    return pl.pallas_call(
        functools.partial(plan_kernel, profiles),
        out_shape=[
            jax.ShapeDtypeStruct((16, lanes), kind),
            jax.ShapeDtypeStruct((1,), kind),
            jax.ShapeDtypeStruct(shape, kind),
        ],
        in_specs=[vmem_spec],
        out_specs=[vmem_spec, pl.BlockSpec(memory_space=pltpu.SMEM), vmem_spec],
        scratch_shapes=[
            pltpu.VMEM(shape[1:], kind),
            pltpu.VMEM(shape, kind),
            pltpu.SemaphoreType.DMA((count - 1,)),
            pltpu.SemaphoreType.DMA((count - 1,)),
        ],
        compiler_params=pltpu.CompilerParams(collective_id=0, has_side_effects=True),
        name="plan",
    )(flags)


def fresh_kernel(x, out):
    out[...] = x[...]


def fresh(x):
    spec = pl.BlockSpec((1,) + x.shape[1:], lambda k: (k, 0, 0))
    return pl.pallas_call(
        fresh_kernel,
        grid=(x.shape[0],),
        in_specs=[spec],
        out_specs=spec,
        out_shape=jax.ShapeDtypeStruct(x.shape, x.dtype),
        name="fresh",
    )(x)


def ordering(active):
    depth = active.shape[-1]
    here = jnp.arange(depth, dtype=jnp.int32)
    on = active.astype(jnp.int32)
    earlier = here[None, :] < here[:, None]
    before = jnp.sum(jnp.where(earlier, on[..., None, :], 0), axis=-1)
    total = jnp.sum(on, axis=-1)
    rank = jnp.where(active, before, total[..., None] + here - before)
    order = jnp.sum(
        jnp.where(rank[..., None, :] == here[:, None], here, 0), axis=-1
    ).astype(jnp.int32)
    return order, total.astype(jnp.int32)


def flipped(index, stride):
    return index + stride - 2 * stride * lax.rem(lax.div(index, stride), 2)


def wide(parts, axis):
    return jnp.concatenate(parts, axis=axis)


def square(a, b):
    size = b[0].shape[1]
    both = wide(b, 1)
    product = dot(wide(a, 1), wide([both, both], 0))
    return product[:, :size] + product[:, size:]


def invert_and_store(panels, first, count, vh_ref, vl_ref, yh_ref, yl_ref):
    depth, band = panels.shape[1:]
    row = lax.broadcasted_iota(jnp.int32, (depth, band), 0)
    col = lax.broadcasted_iota(jnp.int32, (depth, band), 1)
    inside = (row >= col + 1) & (row <= col + band)
    leading = row == col + 1
    r = lax.broadcasted_iota(jnp.int32, (band, band), 0)
    c = lax.broadcasted_iota(jnp.int32, (band, band), 1)
    slots = range(count)
    ts, factors, inverses = [], [], []
    for g in slots:
        v = jnp.where(leading, 1.0, jnp.where(inside, panels[first + g], 0.0))
        vs = split(v)
        ts.append(split(v.T))
        vh_ref[first + g] = vs[0]
        vl_ref[first + g] = vs[1]
        product = dot(wide(ts[g], 0), wide(vs, 1))
        gram = product[:band, :band] + (product[:band, band:] + product[band:, :band])
        diagonal = jnp.sum(jnp.where(r == c, gram, 0.0), axis=0, keepdims=True)
        factors.append(jnp.where(r < c, gram, 0.0))
        inverses.append(jnp.where(r == c, 2.0 / diagonal, 0.0))

    def level(n, inverses):
        coupling = ((r >> n) != (c >> n)) & ((r >> (n + 1)) == (c >> (n + 1)))
        inverse_parts = [split(inverse) for inverse in inverses]
        middles = [
            split(square(split(jnp.where(coupling, factors[g], 0.0)), inverse_parts[g]))
            for g in slots
        ]
        return tuple(inverses[g] - square(inverse_parts[g], middles[g]) for g in slots)

    inverses = lax.fori_loop(0, (band - 1).bit_length(), level, tuple(inverses))
    for g in slots:
        parts = split(inverses[g])
        high, low = ts[g]
        product = dot(wide(parts, 1), wide([high, high], 0)) + dot(parts[0], low)
        yh_ref[first + g], yl_ref[first + g] = split(product)


def whole_kernel(
    profile, group, table, tiles_in, panels_in, merged, last_back,
    tiles, pieces, panel, vh, vl, yh, yl, lift_out, lift_in, upper_new, lower_new, first_back,
    in_sems, panel_sems, lift_sems, back_sems,
):
    early, soon, late, last = profile
    slots, lifts, backs = (early, last), (early, late), (soon, last)
    skip = (0, last - late)
    back_in = (first_back, last_back)
    depth = tiles.shape[0]
    height = pieces.shape[2]
    rows = lax.axis_size("row")
    cols = lax.axis_size("col")
    me_row = lax.axis_index("row")
    me_col = lax.axis_index("col")
    above = lax.rem(me_row + rows - 1, rows)
    below = lax.rem(me_row + 1, rows)
    mesh_id = pl.DeviceIdType.MESH
    strides = []
    stride = cols // 2
    while stride >= 1:
        strides.append(stride)
        stride //= 2
    own = lambda d, k: table[d, k]
    behind = lambda d, k: table[2 + d, k]
    upper_slot = lambda d, j: table[4 + d, j]
    lower_slot = lambda d, j: table[6 + d, j]

    def either(source, index, other):
        return jnp.where(index >= 0, source[jnp.maximum(index, 0)], other)


    panels_copy = pltpu.make_async_copy(panels_in, pieces, in_sems.at[0])
    tiles_copy = pltpu.make_async_copy(tiles_in, tiles, in_sems.at[1])
    panels_copy.start()
    tiles_copy.start()

    barrier = pltpu.get_barrier_semaphore()
    peers = [{"row": above}, {"row": below}]
    peers += [{"col": flipped(me_col, s)} for s in strides]
    for peer in peers:
        pl.semaphore_signal(barrier, inc=1, device_id=peer, device_id_type=mesh_id)
    pl.semaphore_wait(barrier, len(peers))

    def exchange(d, g, stage):
        held = [me_col]
        for s in strides[:stage]:
            held += [flipped(h, s) for h in held]
        base = sum(2**i for i in range(stage))
        copies = []
        for i, h in enumerate(held):
            where = (pl.ds(g * group, group), pl.ds(pl.multiple_of(h * height, height), height))
            copies.append(
                pltpu.make_async_remote_copy(
                    src_ref=panel[d].at[where],
                    dst_ref=panel[d].at[where],
                    send_sem=panel_sems[d].at[0, g, base + i],
                    recv_sem=panel_sems[d].at[1, g, base + i],
                    device_id={"col": flipped(me_col, strides[stage])},
                    device_id_type=mesh_id,
                )
            )
        return copies

    def lift(d, k):
        return pltpu.make_async_remote_copy(
            src_ref=lift_out[d].at[k],
            dst_ref=lift_in[d].at[skip[d] + k],
            send_sem=lift_sems[d].at[0, k],
            recv_sem=lift_sems[d].at[1, k],
            device_id={"row": above},
            device_id_type=mesh_id,
        )

    def give_back(d, k):
        return pltpu.make_async_remote_copy(
            src_ref=lower_new[d].at[k],
            dst_ref=back_in[d].at[k],
            send_sem=back_sems[d].at[0, k],
            recv_sem=back_sems[d].at[1, k],
            device_id={"row": below},
            device_id_type=mesh_id,
        )

    def pick_panels(d):
        mine = pl.ds(pl.multiple_of(me_col * height, height), height)

        def one(g, _):
            for i in range(group):
                panel[d][g * group + i, mine] = pieces[d, own(d, g * group + i)]
            if strides:
                for copy in exchange(d, g, 0):
                    copy.start()
            return 0

        lax.fori_loop(0, panel[d].shape[0] // group, one, 0)

    def forward(d, g):
        for stage in range(1, len(strides)):
            for copy in exchange(d, g, stage - 1):
                copy.wait_recv()
            for copy in exchange(d, g, stage):
                copy.start()

    def factor(d):
        count = panel[d].shape[0] // group

        def one(g, _):
            if strides:
                for copy in exchange(d, g, len(strides) - 1):
                    copy.wait_recv()

            @pl.when(g + 1 < count)
            def _():
                forward(d, g + 1)

            invert_and_store(panel[d], g * group, group, vh[d], vl[d], yh[d], yl[d])
            return 0

        forward(d, 0)
        lax.fori_loop(0, count, one, 0)

    def after_first(j):
        kept = either(back_in[0], lower_slot(0, j), tiles[j])
        return either(upper_new[0], upper_slot(0, j), kept)

    def send_lifts(d, value):
        def one(k, _):
            lift_out[d][k] = value(behind(d, k))

            @pl.when(k > 0)
            def _():
                lift(d, k - 1).start()

            return 0

        lax.fori_loop(0, lifts[d], one, 0)
        lift(d, lifts[d] - 1).start()

    def reflect(d, upper_of, lower_of, sent_of):
        def one(k, _):
            @pl.when(k >= skip[d])
            def _():
                lift(d, k - skip[d]).wait_recv()

            upper, lower = upper_of(k), lower_of(k)
            band = upper.shape[0]
            stacked = split(jnp.concatenate([upper, lower], axis=0))
            solved = split(dot3((yh[d][k], yl[d][k]), stacked))
            change = dot3((vh[d][k], vl[d][k]), solved)
            lower_new[d][k] = sent_of(k, lower - change[band:])
            upper_new[d][k] = upper - change[:band]

            @pl.when(k < backs[d])
            def _():
                give_back(d, k).start()

            return 0

        lax.fori_loop(0, slots[d], one, 0)

    def receive(d):
        def one(k, _):
            give_back(d, k).wait_recv()
            return 0

        lax.fori_loop(0, backs[d], one, 0)

    panels_copy.wait()
    pick_panels(0)
    tiles_copy.wait()
    send_lifts(0, lambda j: tiles[j])
    pick_panels(1)
    factor(0)
    reflect(0, lambda k: tiles[own(0, k)], lambda k: lift_in[0][k], lambda k, lower: lower)
    send_lifts(1, lambda j: either(upper_new[0], upper_slot(0, j), tiles[j]))
    factor(1)
    receive(0)

    def second_lower(k):
        arrived = either(lift_in[0], table[9, k], lift_in[1][k])
        return either(lower_new[0], table[8, k], arrived)

    reflect(
        1,
        lambda k: after_first(own(1, k)),
        second_lower,
        lambda k, lower: either(lower_new[0], table[10, k], lower),
    )

    def merge(j, _):
        merged[j] = either(upper_new[1], upper_slot(1, j), after_first(j))
        return 0

    lax.fori_loop(0, depth, merge, 0)
    receive(1)
    for d in range(2):
        for g in range(panel[d].shape[0] // group):
            for stage in range(len(strides)):
                for copy in exchange(d, g, stage):
                    copy.wait_send()

        def sent(k, _):
            lift(d, k).wait_send()
            return 0

        def returned(k, _):
            give_back(d, k).wait_send()
            return 0

        lax.fori_loop(0, lifts[d], sent, 0)
        lax.fori_loop(0, backs[d], returned, 0)


def settle_kernel(table, merged, back, out, sems):
    depth = merged.shape[0]

    def one(j, _):
        slot = table[7, j]

        @pl.when(slot >= 0)
        def _():
            pltpu.make_async_copy(back.at[jnp.maximum(slot, 0)], out.at[j], sems.at[j]).start()

        @pl.when(slot < 0)
        def _():
            pltpu.make_async_copy(merged.at[j], out.at[j], sems.at[j]).start()

        return 0

    def drain(j, _):
        pltpu.make_async_copy(merged.at[j], out.at[j], sems.at[j]).wait()
        return 0

    lax.fori_loop(0, depth, one, 0)
    lax.fori_loop(0, depth, drain, 0)


def settle(table, merged, back):
    vmem_spec = pl.BlockSpec(memory_space=pltpu.VMEM)
    return pl.pallas_call(
        settle_kernel,
        in_specs=[pl.BlockSpec(memory_space=pltpu.SMEM), vmem_spec, vmem_spec],
        out_specs=pl.BlockSpec(memory_space=pl.ANY),
        out_shape=jax.ShapeDtypeStruct(merged.shape, merged.dtype),
        scratch_shapes=[pltpu.SemaphoreType.DMA((merged.shape[0],))],
        compiler_params=pltpu.CompilerParams(vmem_limit_bytes=8 * 2**20),
        name="settle",
    )(table, merged, back)


def whole(profile, index, table, tiles, panels):
    depth, band, columns = tiles.shape
    _, _, height, _ = panels.shape
    cols = lax.axis_size("col")
    long = height * cols
    early, soon, late, last = profile
    group = GROUPED
    padded = [-(-n // group) * group for n in (early, last)]
    f32, bf16 = jnp.float32, jnp.bfloat16
    tile_slots = lambda counts: [pltpu.VMEM((n, band, columns), f32) for n in counts]
    dma = pltpu.SemaphoreType.DMA
    scratch = [
        pltpu.VMEM(tiles.shape, f32),
        pltpu.VMEM(panels.shape, f32),
        [pltpu.VMEM((n, long, band), f32) for n in padded],
        [pltpu.VMEM((n, long, band), bf16) for n in padded],
        [pltpu.VMEM((n, long, band), bf16) for n in padded],
        [pltpu.VMEM((n, band, long), bf16) for n in padded],
        [pltpu.VMEM((n, band, long), bf16) for n in padded],
        tile_slots((early, late)),
        tile_slots((early, last)),
        tile_slots((early, last)),
        tile_slots((early, last)),
        pltpu.VMEM((soon, band, columns), f32),
        dma((2,)),
        [dma((2, n // group, max(cols - 1, 1))) for n in padded],
        [dma((2, n)) for n in (early, late)],
        [dma((2, n)) for n in (soon, last)],
    ]
    tile_bytes = band * columns * 4
    held = 2 * depth + soon + late + 3 * early + 4 * last
    factors = sum(padded) * long * band * 12
    limit = held * tile_bytes + panels.size * 4 + factors + 12 * 2**20
    any_spec = pl.BlockSpec(memory_space=pl.ANY)
    vmem_spec = pl.BlockSpec(memory_space=pltpu.VMEM)
    merged, back = pl.pallas_call(
        functools.partial(whole_kernel, profile, group),
        in_specs=[pl.BlockSpec(memory_space=pltpu.SMEM), any_spec, any_spec],
        out_specs=[vmem_spec] * 2,
        out_shape=[
            jax.ShapeDtypeStruct(tiles.shape, f32),
            jax.ShapeDtypeStruct((last, band, columns), f32),
        ],
        scratch_shapes=scratch,
        compiler_params=pltpu.CompilerParams(
            collective_id=1 + index, has_side_effects=True, vmem_limit_bytes=limit
        ),
    )(table, tiles, panels)
    return settle(table, merged, back)


def local(eigvec, reflectors, sweep_group):
    row_index = lax.axis_index("row")
    row_count = lax.axis_size("row")
    depth = eigvec.shape[0]
    profiles = [p for p in PROFILES if max(p) <= depth]
    small = depth <= max(PROFILES[-1])
    if small and (depth,) * 4 not in profiles:
        profiles.append((depth,) * 4)
    table, choice, flags = plan(profiles, sweep_group[:, :, 0])

    def general(table, flags, tiles, panels):
        active = flags[:, : sweep_group.shape[0], :depth] >= 0
        mine = lax.dynamic_index_in_dim(active, row_index, 0, keepdims=False)
        above = lax.dynamic_index_in_dim(
            active, (row_index + row_count - 1) % row_count, 0, keepdims=False
        )
        order, counts = ordering(jnp.stack([mine, above]))
        own = order[0]
        behind = jnp.where(row_index == 0, (order[1] + 1) % depth, order[1])
        return steps(depth, own, behind, counts, fresh(tiles), panels)

    def branch(index, profile):
        return lambda table, flags, tiles, panels: whole(profile, index, table, tiles, panels)

    branches = [branch(i, p) for i, p in enumerate(profiles)]
    if not small:
        branches.append(general)
    args = (table, flags, eigvec[:, 0], reflectors[:, :, 0])
    out = lax.switch(choice[0], branches, *args) if len(branches) > 1 else branches[0](*args)
    return out[:, None]


def solution(mesh):
    return jax.shard_map(
        local,
        mesh=mesh,
        in_specs=(
            P(None, "row", None, "col"),
            P(None, None, "row", "col", None),
            P(None, None, "row"),
        ),
        out_specs=P(None, "row", None, "col"),
        check_vma=False,
    )
```

```python
import functools

import jax
import jax.numpy as jnp
from jax import lax
from jax.experimental import pallas as pl
from jax.experimental.pallas import tpu as pltpu
from jax.sharding import PartitionSpec as P

GROUP = 1
CHUNKS = 1
PROFILES = (
    (12, 4, 4, 12), (12, 5, 5, 12), (13, 5, 5, 13), (13, 5, 6, 14), (14, 6, 5, 13), (13, 5, 7, 15),
    (15, 7, 5, 13), (15, 7, 6, 14), (16, 5, 6, 17), (15, 7, 8, 15), (17, 8, 7, 16), (20, 12, 12, 20),
)
GROUPED = 8
SPARE = 10 * 2**20


def split(x):
    high = x.astype(jnp.bfloat16)
    return high, (x - high.astype(jnp.float32)).astype(jnp.bfloat16)


def dot(a, b):
    return jnp.dot(a, b, preferred_element_type=jnp.float32)


def dot3(a, b):
    return dot(a[1], b[0]) + dot(a[0], b[1]) + dot(a[0], b[0])


def bounds(slots):
    inner = [slots * i // CHUNKS // GROUP * GROUP for i in range(CHUNKS)]
    return inner + [slots]


def chunk_shapes(slots, tiles):
    edges = bounds(slots)
    return [
        jax.ShapeDtypeStruct((high - low,) + tiles.shape[1:], tiles.dtype)
        for low, high in zip(edges[:-1], edges[1:])
    ]


def slot_of(chunks, k):
    for chunk in chunks:
        if k < chunk.shape[0]:
            return chunk.at[k]
        k -= chunk.shape[0]


def gather_kernel(slots, own, behind, panels, tiles, picked, *rest):
    diagonals = panels.shape[0]
    sent, sems = rest[:-1], rest[-1]

    def panel_copy(d, k):
        return pltpu.make_async_copy(
            panels.at[d, own[d, k]], picked.at[d, k], sems.at[d * slots + k]
        )

    def tile_copy(k):
        return pltpu.make_async_copy(
            tiles.at[behind[0, k]], slot_of(sent, k), sems.at[diagonals * slots + k]
        )

    for k in range(slots):
        tile_copy(k).start()
    for d in range(diagonals):
        for k in range(slots):
            panel_copy(d, k).start()
    for k in range(slots):
        tile_copy(k).wait()
    for d in range(diagonals):
        for k in range(slots):
            panel_copy(d, k).wait()


def gather(slots, own, behind, panels, tiles):
    diagonals = panels.shape[0]
    any_spec = pl.BlockSpec(memory_space=pl.ANY)
    return pl.pallas_call(
        functools.partial(gather_kernel, slots),
        grid_spec=pltpu.PrefetchScalarGridSpec(
            num_scalar_prefetch=2,
            grid=(1,),
            in_specs=[any_spec, any_spec],
            out_specs=[pl.BlockSpec(memory_space=pltpu.VMEM)] * (1 + CHUNKS),
            scratch_shapes=[pltpu.SemaphoreType.DMA(((diagonals + 1) * slots,))],
        ),
        out_shape=[
            jax.ShapeDtypeStruct((diagonals, slots) + panels.shape[2:], panels.dtype),
        ] + chunk_shapes(slots, tiles),
        name="gather",
    )(own, behind, panels, tiles)


def scatter_kernel(slots, diagonal, more, behind, counts, tiles, *rest):
    returned, out, sent, sems = rest[:CHUNKS], rest[CHUNKS], rest[CHUNKS + 1:-1], rest[-1]

    def put(k):
        return pltpu.make_async_copy(
            slot_of(returned, k), out.at[behind[diagonal, k]], sems.at[k]
        )

    for k in range(slots):
        @pl.when(k < counts[1, diagonal])
        def _():
            put(k).start()
    for k in range(slots):
        @pl.when(k < counts[1, diagonal])
        def _():
            put(k).wait()
    if more:

        def take(k):
            return pltpu.make_async_copy(
                out.at[behind[diagonal + 1, k]], slot_of(sent, k), sems.at[slots + k]
            )

        for k in range(slots):
            take(k).start()
        for k in range(slots):
            take(k).wait()


def scatter(slots, diagonal, more, behind, counts, tiles, returned):
    any_spec = pl.BlockSpec(memory_space=pl.ANY)
    vmem_spec = pl.BlockSpec(memory_space=pltpu.VMEM)
    shapes = [jax.ShapeDtypeStruct(tiles.shape, tiles.dtype)]
    if more:
        shapes += chunk_shapes(slots, tiles)
    return pl.pallas_call(
        functools.partial(scatter_kernel, slots, diagonal, more),
        grid_spec=pltpu.PrefetchScalarGridSpec(
            num_scalar_prefetch=2,
            grid=(1,),
            in_specs=[any_spec] + [vmem_spec] * CHUNKS,
            out_specs=[any_spec] + [vmem_spec] * (len(shapes) - 1),
            scratch_shapes=[pltpu.SemaphoreType.DMA((2 * slots,))],
        ),
        out_shape=shapes,
        input_output_aliases={2: 0},
        name="scatter",
    )(behind, counts, tiles, *returned)


def factor_kernel(pieces_count, col_ref, *refs):
    pieces = refs[:pieces_count]
    vh_ref, vl_ref, yh_ref, yl_ref = refs[pieces_count:]
    me = col_ref[0]
    group = pieces[0].shape[1]
    band = pieces[0].shape[-1]
    depth = pieces_count * pieces[0].shape[2]
    row = lax.broadcasted_iota(jnp.int32, (depth, band), 0)
    col = lax.broadcasted_iota(jnp.int32, (depth, band), 1)
    inside = (row >= col + 1) & (row <= col + band)
    leading = row == col + 1
    r = lax.broadcasted_iota(jnp.int32, (band, band), 0)
    c = lax.broadcasted_iota(jnp.int32, (band, band), 1)
    slots = range(group)
    vs, ts, factors, inverses = [], [], [], []
    for g in slots:
        parts = [piece[0, g] for piece in pieces]
        stride = 1
        while stride < pieces_count:
            odd = (me // stride) % 2 == 1
            parts = [
                jnp.where(odd, parts[j ^ stride], parts[j]) for j in range(pieces_count)
            ]
            stride *= 2
        panel = jnp.concatenate(parts, axis=0)
        v = jnp.where(leading, 1.0, jnp.where(inside, panel, 0.0))
        vs.append(split(v))
        ts.append(split(v.T))
        vh_ref[g] = vs[g][0]
        vl_ref[g] = vs[g][1]
    for g in slots:
        gram = dot3(ts[g], vs[g])
        diagonal = jnp.sum(jnp.where(r == c, gram, 0.0), axis=0, keepdims=True)
        factors.append(gram)
        inverses.append(jnp.where(r == c, 2.0 / diagonal, 0.0))

    def level(n, inverses):
        coupling = ((r >> n) != (c >> n)) & ((r >> (n + 1)) == (c >> (n + 1))) & (r < c)
        inverse_parts = [split(inverse) for inverse in inverses]
        middles = [
            split(dot3(split(jnp.where(coupling, factors[g], 0.0)), inverse_parts[g]))
            for g in slots
        ]
        return tuple(inverses[g] - dot3(inverse_parts[g], middles[g]) for g in slots)

    inverses = lax.fori_loop(0, (band - 1).bit_length(), level, tuple(inverses))
    for g in slots:
        high, low = split(dot3(split(inverses[g]), ts[g]))
        yh_ref[g] = high
        yl_ref[g] = low


def factor(first, slots, diagonal, col, pieces):
    count = len(pieces)
    _, _, height, band = pieces[0].shape
    depth = count * height
    group = GROUP if slots % GROUP == 0 else 1
    start = first // group
    kind = jnp.bfloat16
    return pl.pallas_call(
        functools.partial(factor_kernel, count),
        grid_spec=pltpu.PrefetchScalarGridSpec(
            num_scalar_prefetch=1,
            grid=(slots // group,),
            in_specs=[
                pl.BlockSpec((1, group, height, band), lambda k, c: (diagonal, k + start, 0, 0))
            ] * count,
            out_specs=[pl.BlockSpec((group, depth, band), lambda k, c: (k, 0, 0))] * 2
            + [pl.BlockSpec((group, band, depth), lambda k, c: (k, 0, 0))] * 2,
        ),
        out_shape=[jax.ShapeDtypeStruct((slots, depth, band), kind)] * 2
        + [jax.ShapeDtypeStruct((slots, band, depth), kind)] * 2,
        name="factor",
    )(col, *pieces)


def apply_kernel(diagonal, first, own, counts, tile, below, vh, vl, yh, yl, tile_out, below_out):
    k = pl.program_id(0) + first
    band = tile.shape[1]
    upper, lower = tile[0], below[0]
    stacked = jnp.concatenate([upper, lower], axis=0)
    solved = dot3((yh[0], yl[0]), split(stacked))
    change = dot3((vh[0], vl[0]), split(solved))
    active = k < counts[0, diagonal]
    tile_out[0] = jnp.where(active, upper - change[:band], upper)
    below_out[0] = jnp.where(active, lower - change[band:], lower)


def apply(first, diagonal, own, counts, tiles, beneath, vh, vl, yh, yl):
    _, band, columns = tiles.shape
    depth = vh.shape[1]
    at_slot = lambda k, own, counts: (k, 0, 0)
    at_own = lambda k, own, counts: (own[diagonal, k + first], 0, 0)
    return pl.pallas_call(
        functools.partial(apply_kernel, diagonal, first),
        grid_spec=pltpu.PrefetchScalarGridSpec(
            num_scalar_prefetch=2,
            grid=(beneath.shape[0],),
            in_specs=[
                pl.BlockSpec((1, band, columns), at_own),
                pl.BlockSpec((1, band, columns), at_slot),
                pl.BlockSpec((1, depth, band), at_slot),
                pl.BlockSpec((1, depth, band), at_slot),
                pl.BlockSpec((1, band, depth), at_slot),
                pl.BlockSpec((1, band, depth), at_slot),
            ],
            out_specs=[
                pl.BlockSpec((1, band, columns), at_own),
                pl.BlockSpec((1, band, columns), at_slot),
            ],
        ),
        out_shape=[
            jax.ShapeDtypeStruct(tiles.shape, tiles.dtype),
            jax.ShapeDtypeStruct(beneath.shape, beneath.dtype),
        ],
        input_output_aliases={2: 0},
        name="apply",
    )(own, counts, tiles, beneath, vh, vl, yh, yl)


def lift(sent, to_above):
    beneath = []
    for chunk in sent:
        beneath.append(lax.ppermute(chunk, "row", to_above))
    return beneath


def steps(slots, own, behind, counts, tiles, panels):
    row_count = lax.axis_size("row")
    col_count = lax.axis_size("col")
    col = lax.axis_index("col").astype(jnp.int32)[None]
    diagonals = panels.shape[0]
    to_above = [(i, (i - 1) % row_count) for i in range(row_count)]
    to_below = [(i, (i + 1) % row_count) for i in range(row_count)]
    picked, *sent = gather(slots, own, behind, panels, tiles)
    beneath = lift(sent, to_above)
    pieces = {0: picked}
    stride = col_count // 2
    while stride >= 1:
        swap = [(i, i ^ stride) for i in range(col_count)]
        pieces.update(
            {q ^ stride: lax.ppermute(p, "col", swap) for q, p in pieces.items()}
        )
        stride //= 2
    pieces = [pieces[q] for q in range(col_count)]
    for diagonal in range(diagonals):
        returned = []
        for first, chunk in zip(bounds(slots), beneath):
            factors = factor(first, chunk.shape[0], diagonal, col, pieces)
            tiles, lower = apply(first, diagonal, own, counts, tiles, chunk, *factors)
            returned.append(lax.ppermute(lower, "row", to_below))
        more = diagonal + 1 < diagonals
        tiles, *sent = scatter(slots, diagonal, more, behind, counts, tiles, returned)
        if more:
            beneath = lift(sent, to_above)
    return tiles


def plan_kernel(profiles, flags, table, choice, everyone, mine, held, send, recv):
    count, _, lanes = held.shape
    diagonals, depth = flags.shape
    me = lax.axis_index("row")
    mine[...] = jnp.full(mine.shape, -1, mine.dtype)
    mine[0:diagonals, 0:depth] = flags[...]
    barrier = pltpu.get_barrier_semaphore()
    mesh_id = pl.DeviceIdType.MESH
    others = [lax.rem(me + by, count) for by in range(1, count)]
    for other in others:
        pl.semaphore_signal(
            barrier, inc=1, device_id={"row": other}, device_id_type=mesh_id
        )
    pl.semaphore_wait(barrier, count - 1)
    copies = [
        pltpu.make_async_remote_copy(
            src_ref=mine,
            dst_ref=held.at[me],
            send_sem=send.at[i],
            recv_sem=recv.at[i],
            device_id={"row": other},
            device_id_type=mesh_id,
        )
        for i, other in enumerate(others)
    ]
    for copy in copies:
        copy.start()
    held[me] = mine[...]
    for copy in copies:
        copy.wait()
    everyone[...] = held[...]

    f32 = jnp.float32
    row = lax.broadcasted_iota(jnp.int32, (count, lanes), 0)
    on = [jnp.where(held[:, d, :] >= 0, 1.0, 0.0) for d in range(2)]
    after = []
    for x in on:
        under = pltpu.roll(x, count - 1, axis=0)
        after.append(jnp.where(row == count - 1, pltpu.roll(under, lanes - 1, axis=1), under))
    again = on[0] * on[1]
    first, second = on[0] - again, on[1] - again
    kinds = [
        first * after[1],
        first - first * after[1],
        again,
        second - second * after[0],
        second * after[0],
    ]
    sums = [jnp.sum(x, axis=1, keepdims=True) for x in kinds]
    must, may, rep, ready, unready = sums
    chosen = [jnp.zeros((1, 1), f32) for _ in range(4)]
    index, missed = jnp.zeros((1, 1), f32), jnp.ones((1, 1), f32)
    for early, soon, late, last in profiles:
        bad = (must + may + rep > early) | (must > soon)
        bad |= rep + ready + unready + jnp.maximum(must + may - soon, 0.0) > last
        bad |= unready + jnp.maximum(ready - (early - must - may - rep), 0.0) > late
        still = missed * jnp.max(jnp.where(bad, 1.0, 0.0), axis=0, keepdims=True)
        for i, size in enumerate((early, soon, late, last)):
            chosen[i] = chosen[i] + (missed - still) * size
        index, missed = index + still, still
    choice[0] = index[0, 0].astype(jnp.int32)
    early, soon, late, last = chosen

    above = lax.rem(me + count - 1, count)
    picked = [
        jnp.sum(jnp.where(row == who, x, 0.0), axis=0, keepdims=True)
        for who in (me, above)
        for x in kinds
    ]
    none = jnp.zeros((1, lanes), f32)
    stacked = jnp.concatenate(picked + [none] * 6, axis=0)
    r = lax.broadcasted_iota(jnp.int32, (lanes, lanes), 0)
    c = lax.broadcasted_iota(jnp.int32, (lanes, lanes), 1)
    ahead = jnp.dot(
        stacked.astype(jnp.bfloat16),
        jnp.where(r < c, 1.0, 0.0).astype(jnp.bfloat16),
        preferred_element_type=f32,
    )
    totals = jnp.sum(stacked, axis=1, keepdims=True)

    def places(which):
        at = [stacked[5 * which + i : 5 * which + i + 1] > 0.5 for i in range(5)]
        rank = [ahead[5 * which + i : 5 * which + i + 1] for i in range(5)]
        must, may, rep, ready, unready = [
            totals[5 * which + i : 5 * which + i + 1] for i in range(5)
        ]
        slot0 = jnp.where(
            at[0],
            rank[0],
            jnp.where(at[1], must + rank[1], jnp.where(at[2], must + may + rank[2], -1.0)),
        )
        taken = must + may + rep
        spare = early - taken
        over = jnp.maximum(ready - spare, 0.0)
        tardy = over + unready
        prompt = rep + ready - over

        def placed(p):
            return jnp.where(p < last - late, p, p + tardy)

        fast = at[3] & (rank[3] < spare)
        lag = jnp.where(
            at[4], over + rank[4], jnp.where(at[3] & ~fast, rank[3] - spare, -1.0)
        )
        slot1 = jnp.where(
            at[2],
            placed(rank[2]),
            jnp.where(fast, placed(rep + rank[3]), jnp.where(lag >= 0, last - late + lag, -1.0)),
        )
        single = at[0] | at[1]
        held_back = single & (slot0 >= soon)
        kept = jnp.where(held_back, placed(prompt + slot0 - soon), -1.0)
        sooner = jnp.where(single & (slot0 < soon), slot0, -1.0)
        ahead_of = jnp.where(fast, taken + rank[3], -1.0)
        return at, slot0, slot1, kept, sooner, ahead_of, lag

    top = me == 0

    def below(x):
        return jnp.where(top, pltpu.roll(x, 1, axis=1), x)

    at, slot0, slot1, kept, _, ahead_of, _ = places(0)
    _, up0, up1, up_kept, up_sooner, up_ahead, up_lag = places(1)
    keys = [
        slot0,
        slot1,
        kept,
        jnp.maximum(up0, up_ahead),
        up_lag,
        jnp.where(at[2], slot0, -1.0),
        ahead_of,
        below(up_sooner),
    ]
    filler = jnp.zeros((lanes - len(keys), lanes), f32)
    turned = jnp.concatenate(keys + [filler], axis=0).T
    column = lambda i: turned[:, i : i + 1]
    tile = r.astype(f32)
    place = c.astype(f32)

    def turn(key, value, missing):
        hit = jnp.where(column(key) == place, value - missing, 0.0)
        return jnp.sum(hit, axis=0, keepdims=True) + missing


    def behind(key):
        found = turn(key, tile, 0.0)
        return jnp.where(top, jnp.minimum(found + 1.0, depth - 1.0), found)

    owned = [turn(0, tile, 0.0), turn(1, tile, 0.0)]
    rows = [
        owned[0],
        owned[1],
        behind(3),
        behind(4),
        slot0,
        jnp.where(slot1 >= 0, slot1 + early, -1.0),
        below(up_sooner),
        below(jnp.maximum(up1, up_kept)),
        turn(1, column(5), -1.0),
        turn(1, column(7), -1.0),
        turn(1, column(6), -1.0),
        owned[0],
        owned[1],
        turn(2, column(0), -1.0),
    ]
    rows += [none] * (table.shape[0] - len(rows))
    table[...] = jnp.concatenate(rows, axis=0).astype(jnp.int32)


def plan(profiles, flags):
    count = lax.axis_size("row")
    lanes = 128
    vmem_spec = pl.BlockSpec(memory_space=pltpu.VMEM)
    shape = (count, 8, lanes)
    kind = flags.dtype
    return pl.pallas_call(
        functools.partial(plan_kernel, profiles),
        out_shape=[
            jax.ShapeDtypeStruct((16, lanes), kind),
            jax.ShapeDtypeStruct((1,), kind),
            jax.ShapeDtypeStruct(shape, kind),
        ],
        in_specs=[vmem_spec],
        out_specs=[vmem_spec, pl.BlockSpec(memory_space=pltpu.SMEM), vmem_spec],
        scratch_shapes=[
            pltpu.VMEM(shape[1:], kind),
            pltpu.VMEM(shape, kind),
            pltpu.SemaphoreType.DMA((count - 1,)),
            pltpu.SemaphoreType.DMA((count - 1,)),
        ],
        compiler_params=pltpu.CompilerParams(collective_id=0, has_side_effects=True),
        name="plan",
    )(flags)


def fresh_kernel(x, out):
    out[...] = x[...]


def fresh(x):
    spec = pl.BlockSpec((1,) + x.shape[1:], lambda k: (k, 0, 0))
    return pl.pallas_call(
        fresh_kernel,
        grid=(x.shape[0],),
        in_specs=[spec],
        out_specs=spec,
        out_shape=jax.ShapeDtypeStruct(x.shape, x.dtype),
        name="fresh",
    )(x)


def ordering(active):
    depth = active.shape[-1]
    here = jnp.arange(depth, dtype=jnp.int32)
    on = active.astype(jnp.int32)
    earlier = here[None, :] < here[:, None]
    before = jnp.sum(jnp.where(earlier, on[..., None, :], 0), axis=-1)
    total = jnp.sum(on, axis=-1)
    rank = jnp.where(active, before, total[..., None] + here - before)
    order = jnp.sum(
        jnp.where(rank[..., None, :] == here[:, None], here, 0), axis=-1
    ).astype(jnp.int32)
    return order, total.astype(jnp.int32)


def flipped(index, stride):
    return index + stride - 2 * stride * lax.rem(lax.div(index, stride), 2)


def wide(parts, axis):
    return jnp.concatenate(parts, axis=axis)


def square(a, b):
    size = b[0].shape[1]
    both = wide(b, 1)
    product = dot(wide(a, 1), wide([both, both], 0))
    return product[:, :size] + product[:, size:]


def invert_and_store(panels, first, count, vh_ref, vl_ref, yh_ref, yl_ref):
    depth, band = panels.shape[1:]
    row = lax.broadcasted_iota(jnp.int32, (depth, band), 0)
    col = lax.broadcasted_iota(jnp.int32, (depth, band), 1)
    inside = (row >= col + 1) & (row <= col + band)
    leading = row == col + 1
    r = lax.broadcasted_iota(jnp.int32, (band, band), 0)
    c = lax.broadcasted_iota(jnp.int32, (band, band), 1)
    slots = range(count)
    ts, factors, inverses = [], [], []
    for g in slots:
        v = jnp.where(leading, 1.0, jnp.where(inside, panels[first + g], 0.0))
        vs = split(v)
        ts.append(split(v.T))
        vh_ref[first + g] = vs[0]
        vl_ref[first + g] = vs[1]
        product = dot(wide(ts[g], 0), wide(vs, 1))
        gram = product[:band, :band] + (product[:band, band:] + product[band:, :band])
        diagonal = jnp.sum(jnp.where(r == c, gram, 0.0), axis=0, keepdims=True)
        factors.append(jnp.where(r < c, gram, 0.0))
        inverses.append(jnp.where(r == c, 2.0 / diagonal, 0.0))

    def level(n, inverses):
        coupling = ((r >> n) != (c >> n)) & ((r >> (n + 1)) == (c >> (n + 1)))
        inverse_parts = [split(inverse) for inverse in inverses]
        middles = [
            split(square(split(jnp.where(coupling, factors[g], 0.0)), inverse_parts[g]))
            for g in slots
        ]
        return tuple(inverses[g] - square(inverse_parts[g], middles[g]) for g in slots)

    inverses = lax.fori_loop(0, (band - 1).bit_length(), level, tuple(inverses))
    for g in slots:
        parts = split(inverses[g])
        high, low = ts[g]
        product = dot(wide(parts, 1), wide([high, high], 0)) + dot(parts[0], low)
        yh_ref[first + g], yl_ref[first + g] = split(product)


def whole_kernel(
    profile, group, table, tiles_in, panels_in, merged, last_back,
    tiles, pieces, panel, vh, vl, yh, yl, lift_out, lift_in, upper_new, lower_new, first_back,
    upper_now, lower_now, in_sems, panel_sems, lift_sems, back_sems,
):
    early, soon, late, last = profile
    slots, lifts, backs = (early, last), (early, late), (soon, last)
    skip = (0, last - late)
    groups = [-(-n // group) for n in slots]
    depth = tiles.shape[0]
    height = pieces.shape[2]
    rows = lax.axis_size("row")
    cols = lax.axis_size("col")
    me_row = lax.axis_index("row")
    me_col = lax.axis_index("col")
    above = lax.rem(me_row + rows - 1, rows)
    below = lax.rem(me_row + 1, rows)
    mesh_id = pl.DeviceIdType.MESH
    strides = []
    stride = cols // 2
    while stride >= 1:
        strides.append(stride)
        stride //= 2

    def by(d, pair):
        return pair[0] + d * (pair[1] - pair[0])

    def either(source, index, other):
        return jnp.where(index >= 0, source[jnp.maximum(index, 0)], other)

    panels_copy = pltpu.make_async_copy(panels_in, pieces, in_sems.at[0])
    tiles_copy = pltpu.make_async_copy(tiles_in, tiles, in_sems.at[1])
    panels_copy.start()
    tiles_copy.start()

    barrier = pltpu.get_barrier_semaphore()
    peers = [{"row": above}, {"row": below}]
    peers += [{"col": flipped(me_col, s)} for s in strides]
    for peer in peers:
        pl.semaphore_signal(barrier, inc=1, device_id=peer, device_id_type=mesh_id)
    pl.semaphore_wait(barrier, len(peers))

    def exchange(g, stage):
        held = [me_col]
        for s in strides[:stage]:
            held += [flipped(h, s) for h in held]
        base = sum(2**i for i in range(stage))
        copies = []
        for i, h in enumerate(held):
            where = (pl.ds(g * group, group), pl.ds(pl.multiple_of(h * height, height), height))
            copies.append(
                pltpu.make_async_remote_copy(
                    src_ref=panel.at[where],
                    dst_ref=panel.at[where],
                    send_sem=panel_sems.at[0, g, base + i],
                    recv_sem=panel_sems.at[1, g, base + i],
                    device_id={"col": flipped(me_col, strides[stage])},
                    device_id_type=mesh_id,
                )
            )
        return copies

    def lift(d, k):
        return pltpu.make_async_remote_copy(
            src_ref=lift_out.at[d * early + k],
            dst_ref=lift_in[d].at[skip[d] + k],
            send_sem=lift_sems.at[0, d * early + k],
            recv_sem=lift_sems.at[1, d * early + k],
            device_id={"row": above},
            device_id_type=mesh_id,
        )

    def give_back(d, k):
        return pltpu.make_async_remote_copy(
            src_ref=lower_new.at[d * early + k],
            dst_ref=(first_back, last_back)[d].at[k],
            send_sem=back_sems.at[0, d * soon + k],
            recv_sem=back_sems.at[1, d * soon + k],
            device_id={"row": below},
            device_id_type=mesh_id,
        )

    def repeat(count, body):
        def one(k, _):
            body(k)
            return 0

        lax.fori_loop(0, count, one, 0)

    mine = pl.ds(pl.multiple_of(me_col * height, height), height)

    def pick_panels(d):
        def one(g):
            for i in range(group):
                at = g * group + i
                panel[d * groups[0] * group + at, mine] = pieces[d, table[11 + d, at]]
            if strides:
                for copy in exchange(d * groups[0] + g, 0):
                    copy.start()

        repeat(groups[d], one)

    def forward(g):
        for stage in range(1, len(strides)):
            for copy in exchange(g, stage - 1):
                copy.wait_recv()
            for copy in exchange(g, stage):
                copy.start()

    def factor(d):
        count = by(d, groups)

        def one(at):
            g = d * groups[0] + at
            if strides:
                for copy in exchange(g, len(strides) - 1):
                    copy.wait_recv()

            @pl.when(at + 1 < count)
            def _():
                forward(g + 1)

            invert_and_store(panel, g * group, group, vh, vl, yh, yl)

        forward(d * groups[0])
        repeat(count, one)

    def send_lifts(d, value):
        def one(k):
            lift_out[d * early + k] = value(table[2 + d, k])

            @pl.when(k > 0)
            def _():
                lift(d, k - 1).start()

        repeat(lifts[d], one)
        lift(d, lifts[d] - 1).start()

    def reflect(d):
        def one(k):
            slot = d * early + k
            at = d * groups[0] * group + k

            @pl.when(d == 0)
            def _():
                lift(0, k).wait_recv()
                upper_now[...] = tiles[table[0, k]]
                lower_now[...] = lift_in[0][k]

            @pl.when(d == 1)
            def _():
                @pl.when(k >= skip[1])
                def _():
                    lift(1, k - skip[1]).wait_recv()

                kept = either(first_back, table[9, k], tiles[table[1, k]])
                again = table[8, k]
                upper_now[...] = either(upper_new, again, kept)
                arrived = either(lift_in[0], table[10, k], lift_in[1][k])
                lower_now[...] = either(lower_new, again, arrived)

            upper, lower = upper_now[...], lower_now[...]
            band = upper.shape[0]
            stacked = split(jnp.concatenate([upper, lower], axis=0))
            solved = split(dot3((yh[at], yl[at]), stacked))
            change = dot3((vh[at], vl[at]), solved)
            lower_now[...] = lower - change[band:]
            upper_new[slot] = upper - change[:band]

            @pl.when(d == 0)
            def _():
                lower_new[slot] = lower_now[...]

                @pl.when(k < soon)
                def _():
                    give_back(0, k).start()

            @pl.when(d == 1)
            def _():
                lower_new[slot] = either(lower_new, table[13, k], lower_now[...])
                give_back(1, k).start()

        repeat(by(d, slots), one)

    def receive(d):
        repeat(backs[d], lambda k: give_back(d, k).wait_recv())

    panels_copy.wait()
    pick_panels(0)
    tiles_copy.wait()
    send_lifts(0, lambda j: tiles[j])
    pick_panels(1)

    def diagonal(d):
        factor(d)

        @pl.when(d == 1)
        def _():
            receive(0)

        reflect(d)

        @pl.when(d == 0)
        def _():
            send_lifts(1, lambda j: either(upper_new, table[4, j], tiles[j]))

    repeat(2, diagonal)

    def merge(j):
        kept = either(first_back, table[6, j], tiles[j])
        merged[j] = either(upper_new, table[5, j], either(upper_new, table[4, j], kept))

    repeat(depth, merge)
    receive(1)

    def drain(g):
        for stage in range(len(strides)):
            for copy in exchange(g, stage):
                copy.wait_send()

    repeat(sum(groups), drain)
    for d in range(2):
        repeat(lifts[d], lambda k, d=d: lift(d, k).wait_send())
        repeat(backs[d], lambda k, d=d: give_back(d, k).wait_send())


def settle_kernel(table, merged, back, out, sems):
    depth = merged.shape[0]

    def one(j, _):
        slot = table[7, j]

        @pl.when(slot >= 0)
        def _():
            pltpu.make_async_copy(back.at[jnp.maximum(slot, 0)], out.at[j], sems.at[j]).start()

        @pl.when(slot < 0)
        def _():
            pltpu.make_async_copy(merged.at[j], out.at[j], sems.at[j]).start()

        return 0

    def drain(j, _):
        pltpu.make_async_copy(merged.at[j], out.at[j], sems.at[j]).wait()
        return 0

    lax.fori_loop(0, depth, one, 0)
    lax.fori_loop(0, depth, drain, 0)


def settle(table, merged, back):
    vmem_spec = pl.BlockSpec(memory_space=pltpu.VMEM)
    return pl.pallas_call(
        settle_kernel,
        in_specs=[pl.BlockSpec(memory_space=pltpu.SMEM), vmem_spec, vmem_spec],
        out_specs=pl.BlockSpec(memory_space=pl.ANY),
        out_shape=jax.ShapeDtypeStruct(merged.shape, merged.dtype),
        scratch_shapes=[pltpu.SemaphoreType.DMA((merged.shape[0],))],
        compiler_params=pltpu.CompilerParams(vmem_limit_bytes=8 * 2**20),
        name="settle",
    )(table, merged, back)


def whole(profile, index, table, tiles, panels):
    depth, band, columns = tiles.shape
    _, _, height, _ = panels.shape
    cols = lax.axis_size("col")
    long = height * cols
    early, soon, late, last = profile
    group = GROUPED
    groups = [-(-n // group) for n in (early, last)]
    padded = sum(groups) * group
    f32, bf16 = jnp.float32, jnp.bfloat16
    tile_slots = lambda n: pltpu.VMEM((n, band, columns), f32)
    dma = pltpu.SemaphoreType.DMA
    scratch = [
        pltpu.VMEM(tiles.shape, f32),
        pltpu.VMEM(panels.shape, f32),
        pltpu.VMEM((padded, long, band), f32),
        pltpu.VMEM((padded, long, band), bf16),
        pltpu.VMEM((padded, long, band), bf16),
        pltpu.VMEM((padded, band, long), bf16),
        pltpu.VMEM((padded, band, long), bf16),
        tile_slots(early + late),
        [tile_slots(early), tile_slots(last)],
        tile_slots(early + last),
        tile_slots(early + last),
        tile_slots(soon),
        pltpu.VMEM((band, columns), f32),
        pltpu.VMEM((band, columns), f32),
        dma((2,)),
        dma((2, sum(groups), max(cols - 1, 1))),
        dma((2, early + late)),
        dma((2, soon + last)),
    ]
    tile_bytes = band * columns * 4
    held = 2 * depth + soon + late + 4 * early + 4 * last
    limit = held * tile_bytes + panels.size * 4 + padded * long * band * 12 + SPARE
    any_spec = pl.BlockSpec(memory_space=pl.ANY)
    vmem_spec = pl.BlockSpec(memory_space=pltpu.VMEM)
    merged, back = pl.pallas_call(
        functools.partial(whole_kernel, profile, group),
        in_specs=[pl.BlockSpec(memory_space=pltpu.SMEM), any_spec, any_spec],
        out_specs=[vmem_spec] * 2,
        out_shape=[
            jax.ShapeDtypeStruct(tiles.shape, f32),
            jax.ShapeDtypeStruct((last, band, columns), f32),
        ],
        scratch_shapes=scratch,
        compiler_params=pltpu.CompilerParams(
            collective_id=1 + index, has_side_effects=True, vmem_limit_bytes=limit
        ),
    )(table, tiles, panels)
    return settle(table, merged, back)


def local(eigvec, reflectors, sweep_group):
    row_index = lax.axis_index("row")
    row_count = lax.axis_size("row")
    depth = eigvec.shape[0]
    profiles = [p for p in PROFILES if max(p) <= depth]
    small = depth <= max(PROFILES[-1])
    if small and (depth,) * 4 not in profiles:
        profiles.append((depth,) * 4)
    table, choice, flags = plan(profiles, sweep_group[:, :, 0])

    def general(table, flags, tiles, panels):
        active = flags[:, : sweep_group.shape[0], :depth] >= 0
        mine = lax.dynamic_index_in_dim(active, row_index, 0, keepdims=False)
        above = lax.dynamic_index_in_dim(
            active, (row_index + row_count - 1) % row_count, 0, keepdims=False
        )
        order, counts = ordering(jnp.stack([mine, above]))
        own = order[0]
        behind = jnp.where(row_index == 0, (order[1] + 1) % depth, order[1])
        return steps(depth, own, behind, counts, fresh(tiles), panels)

    def branch(index, profile):
        return lambda table, flags, tiles, panels: whole(profile, index, table, tiles, panels)

    branches = [branch(i, p) for i, p in enumerate(profiles)]
    if not small:
        branches.append(general)
    args = (table, flags, eigvec[:, 0], reflectors[:, :, 0])
    out = lax.switch(choice[0], branches, *args) if len(branches) > 1 else branches[0](*args)
    return out[:, None]


def solution(mesh):
    return jax.shard_map(
        local,
        mesh=mesh,
        in_specs=(
            P(None, "row", None, "col"),
            P(None, None, "row", "col", None),
            P(None, None, "row"),
        ),
        out_specs=P(None, "row", None, "col"),
        check_vma=False,
    )
```

```python
import functools

import jax
import jax.numpy as jnp
from jax import lax
from jax.experimental import pallas as pl
from jax.experimental.pallas import tpu as pltpu
from jax.sharding import PartitionSpec as P

GROUP = 1
CHUNKS = 1
PROFILES = (
    (12, 4, 4, 12), (12, 5, 5, 12), (13, 5, 5, 13), (13, 5, 6, 14), (14, 6, 5, 13), (13, 5, 7, 15),
    (15, 7, 5, 13), (15, 7, 6, 14), (16, 5, 6, 17), (15, 7, 8, 15), (17, 8, 7, 16), (20, 12, 12, 20),
)
GROUPED = 8
SPARE = 10 * 2**20


def split(x):
    high = x.astype(jnp.bfloat16)
    return high, (x - high.astype(jnp.float32)).astype(jnp.bfloat16)


def dot(a, b):
    return jnp.dot(a, b, preferred_element_type=jnp.float32)


def dot3(a, b):
    return dot(a[1], b[0]) + dot(a[0], b[1]) + dot(a[0], b[0])


def bounds(slots):
    inner = [slots * i // CHUNKS // GROUP * GROUP for i in range(CHUNKS)]
    return inner + [slots]


def chunk_shapes(slots, tiles):
    edges = bounds(slots)
    return [
        jax.ShapeDtypeStruct((high - low,) + tiles.shape[1:], tiles.dtype)
        for low, high in zip(edges[:-1], edges[1:])
    ]


def slot_of(chunks, k):
    for chunk in chunks:
        if k < chunk.shape[0]:
            return chunk.at[k]
        k -= chunk.shape[0]


def gather_kernel(slots, own, behind, panels, tiles, picked, *rest):
    diagonals = panels.shape[0]
    sent, sems = rest[:-1], rest[-1]

    def panel_copy(d, k):
        return pltpu.make_async_copy(
            panels.at[d, own[d, k]], picked.at[d, k], sems.at[d * slots + k]
        )

    def tile_copy(k):
        return pltpu.make_async_copy(
            tiles.at[behind[0, k]], slot_of(sent, k), sems.at[diagonals * slots + k]
        )

    for k in range(slots):
        tile_copy(k).start()
    for d in range(diagonals):
        for k in range(slots):
            panel_copy(d, k).start()
    for k in range(slots):
        tile_copy(k).wait()
    for d in range(diagonals):
        for k in range(slots):
            panel_copy(d, k).wait()


def gather(slots, own, behind, panels, tiles):
    diagonals = panels.shape[0]
    any_spec = pl.BlockSpec(memory_space=pl.ANY)
    return pl.pallas_call(
        functools.partial(gather_kernel, slots),
        grid_spec=pltpu.PrefetchScalarGridSpec(
            num_scalar_prefetch=2,
            grid=(1,),
            in_specs=[any_spec, any_spec],
            out_specs=[pl.BlockSpec(memory_space=pltpu.VMEM)] * (1 + CHUNKS),
            scratch_shapes=[pltpu.SemaphoreType.DMA(((diagonals + 1) * slots,))],
        ),
        out_shape=[
            jax.ShapeDtypeStruct((diagonals, slots) + panels.shape[2:], panels.dtype),
        ] + chunk_shapes(slots, tiles),
        name="gather",
    )(own, behind, panels, tiles)


def scatter_kernel(slots, diagonal, more, behind, counts, tiles, *rest):
    returned, out, sent, sems = rest[:CHUNKS], rest[CHUNKS], rest[CHUNKS + 1:-1], rest[-1]

    def put(k):
        return pltpu.make_async_copy(
            slot_of(returned, k), out.at[behind[diagonal, k]], sems.at[k]
        )

    for k in range(slots):
        @pl.when(k < counts[1, diagonal])
        def _():
            put(k).start()
    for k in range(slots):
        @pl.when(k < counts[1, diagonal])
        def _():
            put(k).wait()
    if more:

        def take(k):
            return pltpu.make_async_copy(
                out.at[behind[diagonal + 1, k]], slot_of(sent, k), sems.at[slots + k]
            )

        for k in range(slots):
            take(k).start()
        for k in range(slots):
            take(k).wait()


def scatter(slots, diagonal, more, behind, counts, tiles, returned):
    any_spec = pl.BlockSpec(memory_space=pl.ANY)
    vmem_spec = pl.BlockSpec(memory_space=pltpu.VMEM)
    shapes = [jax.ShapeDtypeStruct(tiles.shape, tiles.dtype)]
    if more:
        shapes += chunk_shapes(slots, tiles)
    return pl.pallas_call(
        functools.partial(scatter_kernel, slots, diagonal, more),
        grid_spec=pltpu.PrefetchScalarGridSpec(
            num_scalar_prefetch=2,
            grid=(1,),
            in_specs=[any_spec] + [vmem_spec] * CHUNKS,
            out_specs=[any_spec] + [vmem_spec] * (len(shapes) - 1),
            scratch_shapes=[pltpu.SemaphoreType.DMA((2 * slots,))],
        ),
        out_shape=shapes,
        input_output_aliases={2: 0},
        name="scatter",
    )(behind, counts, tiles, *returned)


def factor_kernel(pieces_count, col_ref, *refs):
    pieces = refs[:pieces_count]
    vh_ref, vl_ref, yh_ref, yl_ref = refs[pieces_count:]
    me = col_ref[0]
    group = pieces[0].shape[1]
    band = pieces[0].shape[-1]
    depth = pieces_count * pieces[0].shape[2]
    row = lax.broadcasted_iota(jnp.int32, (depth, band), 0)
    col = lax.broadcasted_iota(jnp.int32, (depth, band), 1)
    inside = (row >= col + 1) & (row <= col + band)
    leading = row == col + 1
    r = lax.broadcasted_iota(jnp.int32, (band, band), 0)
    c = lax.broadcasted_iota(jnp.int32, (band, band), 1)
    slots = range(group)
    vs, ts, factors, inverses = [], [], [], []
    for g in slots:
        parts = [piece[0, g] for piece in pieces]
        stride = 1
        while stride < pieces_count:
            odd = (me // stride) % 2 == 1
            parts = [
                jnp.where(odd, parts[j ^ stride], parts[j]) for j in range(pieces_count)
            ]
            stride *= 2
        panel = jnp.concatenate(parts, axis=0)
        v = jnp.where(leading, 1.0, jnp.where(inside, panel, 0.0))
        vs.append(split(v))
        ts.append(split(v.T))
        vh_ref[g] = vs[g][0]
        vl_ref[g] = vs[g][1]
    for g in slots:
        gram = dot3(ts[g], vs[g])
        diagonal = jnp.sum(jnp.where(r == c, gram, 0.0), axis=0, keepdims=True)
        factors.append(gram)
        inverses.append(jnp.where(r == c, 2.0 / diagonal, 0.0))

    def level(n, inverses):
        coupling = ((r >> n) != (c >> n)) & ((r >> (n + 1)) == (c >> (n + 1))) & (r < c)
        inverse_parts = [split(inverse) for inverse in inverses]
        middles = [
            split(dot3(split(jnp.where(coupling, factors[g], 0.0)), inverse_parts[g]))
            for g in slots
        ]
        return tuple(inverses[g] - dot3(inverse_parts[g], middles[g]) for g in slots)

    inverses = lax.fori_loop(0, (band - 1).bit_length(), level, tuple(inverses))
    for g in slots:
        high, low = split(dot3(split(inverses[g]), ts[g]))
        yh_ref[g] = high
        yl_ref[g] = low


def factor(first, slots, diagonal, col, pieces):
    count = len(pieces)
    _, _, height, band = pieces[0].shape
    depth = count * height
    group = GROUP if slots % GROUP == 0 else 1
    start = first // group
    kind = jnp.bfloat16
    return pl.pallas_call(
        functools.partial(factor_kernel, count),
        grid_spec=pltpu.PrefetchScalarGridSpec(
            num_scalar_prefetch=1,
            grid=(slots // group,),
            in_specs=[
                pl.BlockSpec((1, group, height, band), lambda k, c: (diagonal, k + start, 0, 0))
            ] * count,
            out_specs=[pl.BlockSpec((group, depth, band), lambda k, c: (k, 0, 0))] * 2
            + [pl.BlockSpec((group, band, depth), lambda k, c: (k, 0, 0))] * 2,
        ),
        out_shape=[jax.ShapeDtypeStruct((slots, depth, band), kind)] * 2
        + [jax.ShapeDtypeStruct((slots, band, depth), kind)] * 2,
        name="factor",
    )(col, *pieces)


def apply_kernel(diagonal, first, own, counts, tile, below, vh, vl, yh, yl, tile_out, below_out):
    k = pl.program_id(0) + first
    band = tile.shape[1]
    upper, lower = tile[0], below[0]
    stacked = jnp.concatenate([upper, lower], axis=0)
    solved = dot3((yh[0], yl[0]), split(stacked))
    change = dot3((vh[0], vl[0]), split(solved))
    active = k < counts[0, diagonal]
    tile_out[0] = jnp.where(active, upper - change[:band], upper)
    below_out[0] = jnp.where(active, lower - change[band:], lower)


def apply(first, diagonal, own, counts, tiles, beneath, vh, vl, yh, yl):
    _, band, columns = tiles.shape
    depth = vh.shape[1]
    at_slot = lambda k, own, counts: (k, 0, 0)
    at_own = lambda k, own, counts: (own[diagonal, k + first], 0, 0)
    return pl.pallas_call(
        functools.partial(apply_kernel, diagonal, first),
        grid_spec=pltpu.PrefetchScalarGridSpec(
            num_scalar_prefetch=2,
            grid=(beneath.shape[0],),
            in_specs=[
                pl.BlockSpec((1, band, columns), at_own),
                pl.BlockSpec((1, band, columns), at_slot),
                pl.BlockSpec((1, depth, band), at_slot),
                pl.BlockSpec((1, depth, band), at_slot),
                pl.BlockSpec((1, band, depth), at_slot),
                pl.BlockSpec((1, band, depth), at_slot),
            ],
            out_specs=[
                pl.BlockSpec((1, band, columns), at_own),
                pl.BlockSpec((1, band, columns), at_slot),
            ],
        ),
        out_shape=[
            jax.ShapeDtypeStruct(tiles.shape, tiles.dtype),
            jax.ShapeDtypeStruct(beneath.shape, beneath.dtype),
        ],
        input_output_aliases={2: 0},
        name="apply",
    )(own, counts, tiles, beneath, vh, vl, yh, yl)


def lift(sent, to_above):
    beneath = []
    for chunk in sent:
        beneath.append(lax.ppermute(chunk, "row", to_above))
    return beneath


def steps(slots, own, behind, counts, tiles, panels):
    row_count = lax.axis_size("row")
    col_count = lax.axis_size("col")
    col = lax.axis_index("col").astype(jnp.int32)[None]
    diagonals = panels.shape[0]
    to_above = [(i, (i - 1) % row_count) for i in range(row_count)]
    to_below = [(i, (i + 1) % row_count) for i in range(row_count)]
    picked, *sent = gather(slots, own, behind, panels, tiles)
    beneath = lift(sent, to_above)
    pieces = {0: picked}
    stride = col_count // 2
    while stride >= 1:
        swap = [(i, i ^ stride) for i in range(col_count)]
        pieces.update(
            {q ^ stride: lax.ppermute(p, "col", swap) for q, p in pieces.items()}
        )
        stride //= 2
    pieces = [pieces[q] for q in range(col_count)]
    for diagonal in range(diagonals):
        returned = []
        for first, chunk in zip(bounds(slots), beneath):
            factors = factor(first, chunk.shape[0], diagonal, col, pieces)
            tiles, lower = apply(first, diagonal, own, counts, tiles, chunk, *factors)
            returned.append(lax.ppermute(lower, "row", to_below))
        more = diagonal + 1 < diagonals
        tiles, *sent = scatter(slots, diagonal, more, behind, counts, tiles, returned)
        if more:
            beneath = lift(sent, to_above)
    return tiles


def plan_kernel(profiles, flags, table, choice, everyone, mine, held, send, recv):
    count, lanes = held.shape
    half = lanes // 2
    depth = flags.shape[1]
    me = lax.axis_index("row")
    mine[...] = jnp.full(mine.shape, -1, mine.dtype)
    for d in range(2):
        mine[0:1, d * half : d * half + depth] = flags[d : d + 1]
    barrier = pltpu.get_barrier_semaphore()
    mesh_id = pl.DeviceIdType.MESH
    others = [lax.rem(me + by, count) for by in range(1, count)]
    for other in others:
        pl.semaphore_signal(
            barrier, inc=1, device_id={"row": other}, device_id_type=mesh_id
        )
    pl.semaphore_wait(barrier, count - 1)
    here = pl.ds(me, 1)
    copies = [
        pltpu.make_async_remote_copy(
            src_ref=mine.at[pl.ds(0, 1)],
            dst_ref=held.at[here],
            send_sem=send.at[i],
            recv_sem=recv.at[i],
            device_id={"row": other},
            device_id_type=mesh_id,
        )
        for i, other in enumerate(others)
    ]
    for copy in copies:
        copy.start()
    held[here] = mine[0:1]
    for copy in copies:
        copy.wait()
    packed = held[...]
    everyone[...] = packed

    f32 = jnp.float32
    row = lax.broadcasted_iota(jnp.int32, (count, lanes), 0)
    lane = lax.broadcasted_iota(jnp.int32, (count, lanes), 1)
    set_lanes = jnp.where(packed >= 0, 1.0, 0.0)
    on = [
        jnp.where(lane < half, x, 0.0)
        for x in (set_lanes, pltpu.roll(set_lanes, half, axis=1))
    ]
    after = []
    for x in on:
        under = pltpu.roll(x, count - 1, axis=0)
        after.append(jnp.where(row == count - 1, pltpu.roll(under, lanes - 1, axis=1), under))
    again = on[0] * on[1]
    first, second = on[0] - again, on[1] - again
    kinds = [
        first * after[1],
        first - first * after[1],
        again,
        second - second * after[0],
        second * after[0],
    ]
    sums = [jnp.sum(x, axis=1, keepdims=True) for x in kinds]
    must, may, rep, ready, unready = sums
    chosen = [jnp.zeros((1, 1), f32) for _ in range(4)]
    index, missed = jnp.zeros((1, 1), f32), jnp.ones((1, 1), f32)
    for early, soon, late, last in profiles:
        bad = (must + may + rep > early) | (must > soon)
        bad |= rep + ready + unready + jnp.maximum(must + may - soon, 0.0) > last
        bad |= unready + jnp.maximum(ready - (early - must - may - rep), 0.0) > late
        still = missed * jnp.max(jnp.where(bad, 1.0, 0.0), axis=0, keepdims=True)
        for i, size in enumerate((early, soon, late, last)):
            chosen[i] = chosen[i] + (missed - still) * size
        index, missed = index + still, still
    choice[0] = index[0, 0].astype(jnp.int32)
    early, soon, late, last = chosen

    above = lax.rem(me + count - 1, count)
    picked = [
        jnp.sum(jnp.where(row == who, x, 0.0), axis=0, keepdims=True)
        for who in (me, above)
        for x in kinds
    ]
    none = jnp.zeros((1, lanes), f32)
    stacked = jnp.concatenate(picked + [none] * 6, axis=0)
    r = lax.broadcasted_iota(jnp.int32, (lanes, lanes), 0)
    c = lax.broadcasted_iota(jnp.int32, (lanes, lanes), 1)
    ahead = jnp.dot(
        stacked.astype(jnp.bfloat16),
        jnp.where(r < c, 1.0, 0.0).astype(jnp.bfloat16),
        preferred_element_type=f32,
    )
    totals = jnp.sum(stacked, axis=1, keepdims=True)

    def places(which):
        at = [stacked[5 * which + i : 5 * which + i + 1] > 0.5 for i in range(5)]
        rank = [ahead[5 * which + i : 5 * which + i + 1] for i in range(5)]
        must, may, rep, ready, unready = [
            totals[5 * which + i : 5 * which + i + 1] for i in range(5)
        ]
        slot0 = jnp.where(
            at[0],
            rank[0],
            jnp.where(at[1], must + rank[1], jnp.where(at[2], must + may + rank[2], -1.0)),
        )
        taken = must + may + rep
        spare = early - taken
        over = jnp.maximum(ready - spare, 0.0)
        tardy = over + unready
        prompt = rep + ready - over

        def placed(p):
            return jnp.where(p < last - late, p, p + tardy)

        fast = at[3] & (rank[3] < spare)
        lag = jnp.where(
            at[4], over + rank[4], jnp.where(at[3] & ~fast, rank[3] - spare, -1.0)
        )
        slot1 = jnp.where(
            at[2],
            placed(rank[2]),
            jnp.where(fast, placed(rep + rank[3]), jnp.where(lag >= 0, last - late + lag, -1.0)),
        )
        single = at[0] | at[1]
        held_back = single & (slot0 >= soon)
        kept = jnp.where(held_back, placed(prompt + slot0 - soon), -1.0)
        sooner = jnp.where(single & (slot0 < soon), slot0, -1.0)
        ahead_of = jnp.where(fast, taken + rank[3], -1.0)
        return at, slot0, slot1, kept, sooner, ahead_of, lag

    top = me == 0

    def below(x):
        return jnp.where(top, pltpu.roll(x, 1, axis=1), x)

    at, slot0, slot1, kept, _, ahead_of, _ = places(0)
    _, up0, up1, up_kept, up_sooner, up_ahead, up_lag = places(1)
    keys = [
        slot0,
        slot1,
        kept,
        jnp.maximum(up0, up_ahead),
        up_lag,
        jnp.where(at[2], slot0, -1.0),
        ahead_of,
        below(up_sooner),
    ]
    filler = jnp.zeros((lanes - len(keys), lanes), f32)
    turned = jnp.concatenate(keys + [filler], axis=0).T
    column = lambda i: turned[:, i : i + 1]
    tile = r.astype(f32)
    place = c.astype(f32)

    def turn(key, value, missing):
        hit = jnp.where(column(key) == place, value - missing, 0.0)
        return jnp.sum(hit, axis=0, keepdims=True) + missing


    def behind(key):
        found = turn(key, tile, 0.0)
        return jnp.where(top, jnp.minimum(found + 1.0, depth - 1.0), found)

    owned = [turn(0, tile, 0.0), turn(1, tile, 0.0)]
    rows = [
        owned[0],
        owned[1],
        behind(3),
        behind(4),
        slot0,
        jnp.where(slot1 >= 0, slot1 + early, -1.0),
        below(up_sooner),
        below(jnp.maximum(up1, up_kept)),
        turn(1, column(5), -1.0),
        turn(1, column(7), -1.0),
        turn(1, column(6), -1.0),
        owned[0],
        owned[1],
        turn(2, column(0), -1.0),
    ]
    rows += [none] * (table.shape[0] - len(rows))
    table[...] = jnp.concatenate(rows, axis=0).astype(jnp.int32)


def plan(profiles, flags):
    count = lax.axis_size("row")
    lanes = 128
    vmem_spec = pl.BlockSpec(memory_space=pltpu.VMEM)
    shape = (count, lanes)
    kind = flags.dtype
    return pl.pallas_call(
        functools.partial(plan_kernel, profiles),
        out_shape=[
            jax.ShapeDtypeStruct((16, lanes), kind),
            jax.ShapeDtypeStruct((1,), kind),
            jax.ShapeDtypeStruct(shape, kind),
        ],
        in_specs=[vmem_spec],
        out_specs=[vmem_spec, pl.BlockSpec(memory_space=pltpu.SMEM), vmem_spec],
        scratch_shapes=[
            pltpu.VMEM((8, lanes), kind),
            pltpu.VMEM(shape, kind),
            pltpu.SemaphoreType.DMA((count - 1,)),
            pltpu.SemaphoreType.DMA((count - 1,)),
        ],
        compiler_params=pltpu.CompilerParams(collective_id=0, has_side_effects=True),
        name="plan",
    )(flags)


def fresh_kernel(x, out):
    out[...] = x[...]


def fresh(x):
    spec = pl.BlockSpec((1,) + x.shape[1:], lambda k: (k, 0, 0))
    return pl.pallas_call(
        fresh_kernel,
        grid=(x.shape[0],),
        in_specs=[spec],
        out_specs=spec,
        out_shape=jax.ShapeDtypeStruct(x.shape, x.dtype),
        name="fresh",
    )(x)


def ordering(active):
    depth = active.shape[-1]
    here = jnp.arange(depth, dtype=jnp.int32)
    on = active.astype(jnp.int32)
    earlier = here[None, :] < here[:, None]
    before = jnp.sum(jnp.where(earlier, on[..., None, :], 0), axis=-1)
    total = jnp.sum(on, axis=-1)
    rank = jnp.where(active, before, total[..., None] + here - before)
    order = jnp.sum(
        jnp.where(rank[..., None, :] == here[:, None], here, 0), axis=-1
    ).astype(jnp.int32)
    return order, total.astype(jnp.int32)


def flipped(index, stride):
    return index + stride - 2 * stride * lax.rem(lax.div(index, stride), 2)


def wide(parts, axis):
    return jnp.concatenate(parts, axis=axis)


def square(a, b):
    size = b[0].shape[1]
    both = wide(b, 1)
    product = dot(wide(a, 1), wide([both, both], 0))
    return product[:, :size] + product[:, size:]


def invert_and_store(panels, first, count, vh_ref, vl_ref, yh_ref, yl_ref):
    depth, band = panels.shape[1:]
    row = lax.broadcasted_iota(jnp.int32, (depth, band), 0)
    col = lax.broadcasted_iota(jnp.int32, (depth, band), 1)
    inside = (row >= col + 1) & (row <= col + band)
    leading = row == col + 1
    r = lax.broadcasted_iota(jnp.int32, (band, band), 0)
    c = lax.broadcasted_iota(jnp.int32, (band, band), 1)
    slots = range(count)
    ts, factors, inverses = [], [], []
    for g in slots:
        v = jnp.where(leading, 1.0, jnp.where(inside, panels[first + g], 0.0))
        vs = split(v)
        ts.append(split(v.T))
        vh_ref[first + g] = vs[0]
        vl_ref[first + g] = vs[1]
        product = dot(wide(ts[g], 0), wide(vs, 1))
        gram = product[:band, :band] + (product[:band, band:] + product[band:, :band])
        diagonal = jnp.sum(jnp.where(r == c, gram, 0.0), axis=0, keepdims=True)
        factors.append(jnp.where(r < c, gram, 0.0))
        inverses.append(jnp.where(r == c, 2.0 / diagonal, 0.0))

    def level(n, inverses):
        coupling = ((r >> n) != (c >> n)) & ((r >> (n + 1)) == (c >> (n + 1)))
        inverse_parts = [split(inverse) for inverse in inverses]
        middles = [
            split(square(split(jnp.where(coupling, factors[g], 0.0)), inverse_parts[g]))
            for g in slots
        ]
        return tuple(inverses[g] - square(inverse_parts[g], middles[g]) for g in slots)

    inverses = lax.fori_loop(0, (band - 1).bit_length(), level, tuple(inverses))
    for g in slots:
        parts = split(inverses[g])
        high, low = ts[g]
        product = dot(wide(parts, 1), wide([high, high], 0)) + dot(parts[0], low)
        yh_ref[first + g], yl_ref[first + g] = split(product)


def whole_kernel(
    profile, group, table, tiles_in, panels_in, merged, last_back,
    tiles, pieces, panel, vh, vl, yh, yl, lift_out, lift_in, upper_new, lower_new, first_back,
    upper_now, lower_now, in_sems, panel_sems, lift_sems, back_sems,
):
    early, soon, late, last = profile
    slots, lifts, backs = (early, last), (early, late), (soon, last)
    skip = (0, last - late)
    groups = [-(-n // group) for n in slots]
    depth = tiles.shape[0]
    height = pieces.shape[2]
    rows = lax.axis_size("row")
    cols = lax.axis_size("col")
    me_row = lax.axis_index("row")
    me_col = lax.axis_index("col")
    above = lax.rem(me_row + rows - 1, rows)
    below = lax.rem(me_row + 1, rows)
    mesh_id = pl.DeviceIdType.MESH
    strides = []
    stride = cols // 2
    while stride >= 1:
        strides.append(stride)
        stride //= 2

    def by(d, pair):
        return pair[0] + d * (pair[1] - pair[0])

    def either(source, index, other):
        return jnp.where(index >= 0, source[jnp.maximum(index, 0)], other)

    panels_copy = pltpu.make_async_copy(panels_in, pieces, in_sems.at[0])
    tiles_copy = pltpu.make_async_copy(tiles_in, tiles, in_sems.at[1])
    panels_copy.start()
    tiles_copy.start()

    barrier = pltpu.get_barrier_semaphore()
    peers = [{"row": above}, {"row": below}]
    peers += [{"col": flipped(me_col, s)} for s in strides]
    for peer in peers:
        pl.semaphore_signal(barrier, inc=1, device_id=peer, device_id_type=mesh_id)
    pl.semaphore_wait(barrier, len(peers))

    def exchange(g, stage):
        held = [me_col]
        for s in strides[:stage]:
            held += [flipped(h, s) for h in held]
        base = sum(2**i for i in range(stage))
        copies = []
        for i, h in enumerate(held):
            where = (pl.ds(g * group, group), pl.ds(pl.multiple_of(h * height, height), height))
            copies.append(
                pltpu.make_async_remote_copy(
                    src_ref=panel.at[where],
                    dst_ref=panel.at[where],
                    send_sem=panel_sems.at[0, g, base + i],
                    recv_sem=panel_sems.at[1, g, base + i],
                    device_id={"col": flipped(me_col, strides[stage])},
                    device_id_type=mesh_id,
                )
            )
        return copies

    def lift(d, k):
        return pltpu.make_async_remote_copy(
            src_ref=lift_out.at[d * early + k],
            dst_ref=lift_in[d].at[skip[d] + k],
            send_sem=lift_sems.at[0, d * early + k],
            recv_sem=lift_sems.at[1, d * early + k],
            device_id={"row": above},
            device_id_type=mesh_id,
        )

    def give_back(d, k):
        return pltpu.make_async_remote_copy(
            src_ref=lower_new.at[d * early + k],
            dst_ref=(first_back, last_back)[d].at[k],
            send_sem=back_sems.at[0, d * soon + k],
            recv_sem=back_sems.at[1, d * soon + k],
            device_id={"row": below},
            device_id_type=mesh_id,
        )

    def repeat(count, body):
        def one(k, _):
            body(k)
            return 0

        lax.fori_loop(0, count, one, 0)

    mine = pl.ds(pl.multiple_of(me_col * height, height), height)

    def pick_panels(d):
        def one(g):
            for i in range(group):
                at = g * group + i
                panel[d * groups[0] * group + at, mine] = pieces[d, table[11 + d, at]]
            if strides:
                for copy in exchange(d * groups[0] + g, 0):
                    copy.start()

        repeat(groups[d], one)

    def forward(g):
        for stage in range(1, len(strides)):
            for copy in exchange(g, stage - 1):
                copy.wait_recv()
            for copy in exchange(g, stage):
                copy.start()

    def factor(d):
        count = by(d, groups)

        def one(at):
            g = d * groups[0] + at
            if strides:
                for copy in exchange(g, len(strides) - 1):
                    copy.wait_recv()

            @pl.when(at + 1 < count)
            def _():
                forward(g + 1)

            invert_and_store(panel, g * group, group, vh, vl, yh, yl)

        forward(d * groups[0])
        repeat(count, one)

    def send_lifts(d, value):
        def one(k):
            lift_out[d * early + k] = value(table[2 + d, k])

            @pl.when(k > 0)
            def _():
                lift(d, k - 1).start()

        repeat(lifts[d], one)
        lift(d, lifts[d] - 1).start()

    def reflect(d):
        def one(k):
            slot = d * early + k
            at = d * groups[0] * group + k

            @pl.when(d == 0)
            def _():
                lift(0, k).wait_recv()
                upper_now[...] = tiles[table[0, k]]
                lower_now[...] = lift_in[0][k]

            @pl.when(d == 1)
            def _():
                @pl.when(k >= skip[1])
                def _():
                    lift(1, k - skip[1]).wait_recv()

                kept = either(first_back, table[9, k], tiles[table[1, k]])
                again = table[8, k]
                upper_now[...] = either(upper_new, again, kept)
                arrived = either(lift_in[0], table[10, k], lift_in[1][k])
                lower_now[...] = either(lower_new, again, arrived)

            upper, lower = upper_now[...], lower_now[...]
            band = upper.shape[0]
            stacked = split(jnp.concatenate([upper, lower], axis=0))
            solved = split(dot3((yh[at], yl[at]), stacked))
            change = dot3((vh[at], vl[at]), solved)
            lower_now[...] = lower - change[band:]
            upper_new[slot] = upper - change[:band]

            @pl.when(d == 0)
            def _():
                lower_new[slot] = lower_now[...]

                @pl.when(k < soon)
                def _():
                    give_back(0, k).start()

            @pl.when(d == 1)
            def _():
                lower_new[slot] = either(lower_new, table[13, k], lower_now[...])
                give_back(1, k).start()

        repeat(by(d, slots), one)

    def receive(d):
        repeat(backs[d], lambda k: give_back(d, k).wait_recv())

    panels_copy.wait()
    pick_panels(0)
    tiles_copy.wait()
    send_lifts(0, lambda j: tiles[j])
    pick_panels(1)

    def diagonal(d):
        factor(d)

        @pl.when(d == 1)
        def _():
            receive(0)

        reflect(d)

        @pl.when(d == 0)
        def _():
            send_lifts(1, lambda j: either(upper_new, table[4, j], tiles[j]))

    repeat(2, diagonal)

    def merge(j):
        kept = either(first_back, table[6, j], tiles[j])
        merged[j] = either(upper_new, table[5, j], either(upper_new, table[4, j], kept))

    repeat(depth, merge)
    receive(1)

    def drain(g):
        for stage in range(len(strides)):
            for copy in exchange(g, stage):
                copy.wait_send()

    repeat(sum(groups), drain)
    for d in range(2):
        repeat(lifts[d], lambda k, d=d: lift(d, k).wait_send())
        repeat(backs[d], lambda k, d=d: give_back(d, k).wait_send())


def settle_kernel(table, merged, back, out, sems):
    depth = merged.shape[0]

    def one(j, _):
        slot = table[7, j]

        @pl.when(slot >= 0)
        def _():
            pltpu.make_async_copy(back.at[jnp.maximum(slot, 0)], out.at[j], sems.at[j]).start()

        @pl.when(slot < 0)
        def _():
            pltpu.make_async_copy(merged.at[j], out.at[j], sems.at[j]).start()

        return 0

    def drain(j, _):
        pltpu.make_async_copy(merged.at[j], out.at[j], sems.at[j]).wait()
        return 0

    lax.fori_loop(0, depth, one, 0)
    lax.fori_loop(0, depth, drain, 0)


def settle(table, merged, back):
    vmem_spec = pl.BlockSpec(memory_space=pltpu.VMEM)
    return pl.pallas_call(
        settle_kernel,
        in_specs=[pl.BlockSpec(memory_space=pltpu.SMEM), vmem_spec, vmem_spec],
        out_specs=pl.BlockSpec(memory_space=pl.ANY),
        out_shape=jax.ShapeDtypeStruct(merged.shape, merged.dtype),
        scratch_shapes=[pltpu.SemaphoreType.DMA((merged.shape[0],))],
        compiler_params=pltpu.CompilerParams(vmem_limit_bytes=8 * 2**20),
        name="settle",
    )(table, merged, back)


def whole(profile, index, table, tiles, panels):
    depth, band, columns = tiles.shape
    _, _, height, _ = panels.shape
    cols = lax.axis_size("col")
    long = height * cols
    early, soon, late, last = profile
    group = GROUPED
    groups = [-(-n // group) for n in (early, last)]
    padded = sum(groups) * group
    f32, bf16 = jnp.float32, jnp.bfloat16
    tile_slots = lambda n: pltpu.VMEM((n, band, columns), f32)
    dma = pltpu.SemaphoreType.DMA
    scratch = [
        pltpu.VMEM(tiles.shape, f32),
        pltpu.VMEM(panels.shape, f32),
        pltpu.VMEM((padded, long, band), f32),
        pltpu.VMEM((padded, long, band), bf16),
        pltpu.VMEM((padded, long, band), bf16),
        pltpu.VMEM((padded, band, long), bf16),
        pltpu.VMEM((padded, band, long), bf16),
        tile_slots(early + late),
        [tile_slots(early), tile_slots(last)],
        tile_slots(early + last),
        tile_slots(early + last),
        tile_slots(soon),
        pltpu.VMEM((band, columns), f32),
        pltpu.VMEM((band, columns), f32),
        dma((2,)),
        dma((2, sum(groups), max(cols - 1, 1))),
        dma((2, early + late)),
        dma((2, soon + last)),
    ]
    tile_bytes = band * columns * 4
    held = 2 * depth + soon + late + 4 * early + 4 * last
    limit = held * tile_bytes + panels.size * 4 + padded * long * band * 12 + SPARE
    any_spec = pl.BlockSpec(memory_space=pl.ANY)
    vmem_spec = pl.BlockSpec(memory_space=pltpu.VMEM)
    merged, back = pl.pallas_call(
        functools.partial(whole_kernel, profile, group),
        in_specs=[pl.BlockSpec(memory_space=pltpu.SMEM), any_spec, any_spec],
        out_specs=[vmem_spec] * 2,
        out_shape=[
            jax.ShapeDtypeStruct(tiles.shape, f32),
            jax.ShapeDtypeStruct((last, band, columns), f32),
        ],
        scratch_shapes=scratch,
        compiler_params=pltpu.CompilerParams(
            collective_id=1 + index, has_side_effects=True, vmem_limit_bytes=limit
        ),
    )(table, tiles, panels)
    return settle(table, merged, back)


def local(eigvec, reflectors, sweep_group):
    row_index = lax.axis_index("row")
    row_count = lax.axis_size("row")
    depth = eigvec.shape[0]
    profiles = [p for p in PROFILES if max(p) <= depth]
    small = depth <= max(PROFILES[-1])
    if small and (depth,) * 4 not in profiles:
        profiles.append((depth,) * 4)
    table, choice, flags = plan(profiles, sweep_group[:, :, 0])

    def general(table, flags, tiles, panels):
        half = flags.shape[1] // 2
        active = jnp.stack([flags[:, :depth], flags[:, half : half + depth]], axis=1) >= 0
        mine = lax.dynamic_index_in_dim(active, row_index, 0, keepdims=False)
        above = lax.dynamic_index_in_dim(
            active, (row_index + row_count - 1) % row_count, 0, keepdims=False
        )
        order, counts = ordering(jnp.stack([mine, above]))
        own = order[0]
        behind = jnp.where(row_index == 0, (order[1] + 1) % depth, order[1])
        return steps(depth, own, behind, counts, fresh(tiles), panels)

    def branch(index, profile):
        return lambda table, flags, tiles, panels: whole(profile, index, table, tiles, panels)

    branches = [branch(i, p) for i, p in enumerate(profiles)]
    if not small:
        branches.append(general)
    args = (table, flags, eigvec[:, 0], reflectors[:, :, 0])
    out = lax.switch(choice[0], branches, *args) if len(branches) > 1 else branches[0](*args)
    return out[:, None]


def solution(mesh):
    return jax.shard_map(
        local,
        mesh=mesh,
        in_specs=(
            P(None, "row", None, "col"),
            P(None, None, "row", "col", None),
            P(None, None, "row"),
        ),
        out_specs=P(None, "row", None, "col"),
        check_vma=False,
    )
```
